32 devices in a mesh: slab: 16 (over z, y, x), cell: 2 (over core).
Axes of the slice: x: 2, y: 2, z: 4, core: 2. Of those that a mesh axis runs over, the one named last changes fastest.
Arguments:
- cell_row: int32 [16384], P(('slab', 'cell')), may hold values from 0 to 2043, as said below
- cell_col: int32 [16384], P(('slab', 'cell')), may hold values from 0 to 2039
- cell_width: int32 [16384], P(('slab', 'cell')), may hold values from 1 to 8
- cell_height: int32 [16384], P(('slab', 'cell')), may hold values from 1 to 4
- cell_region: int32 [16384], P(('slab', 'cell')), may hold values from 0 to 3
- cell_offset: float32 [2, 16384], P(None, ('slab', 'cell')), may hold values from 0 to 1
Outputs:
- field_x: float32 [4, 2048, 2048], P(None, ('slab', 'cell'))
- field_y: float32 [4, 2048, 2048], P(None, ('slab', 'cell'))
- cell_force: float32 [2, 16384], P(None, ('slab', 'cell'))
- energy: float32 [], replicated
- overflow: float32 [], replicated
The draws below stay inside these ranges and needn't reach their ends.
Inputs may be any that keep to these rules, and one draw needn't show every extreme that they name: `cell_row`: cell i belongs to row slab s = i // 1024: its row lies in [s * 128, (s + 1) * 128); cells of the last slab lie at least 4 rows below the top of the grid.
All inputs are finite; a program needn't handle non-finite values.
Results may differ from the reference program's by a relative error of at most 0.0015.
Values may be sent and summed in bfloat16 or wider, within the bound.
No kernel may reach another device: no remote copies, remote signals or barrier semaphores. Data moves between devices by JAX's collectives and lax.ppermute only.
A program may use at most 128 MiB of HBM per device.

```python
import jax
import jax.numpy as jnp
from jax import lax

M = 2048
REGIONS = 4
HMAX = 4
WMAX = 8
ROWS = 128
CELLS_SLAB = 1024
CELLS = 16384


def draw_cell_row(key, part):
    positions = jnp.arange(CELLS, dtype=jnp.int32)
    slab_index = positions // CELLS_SLAB
    top_slab = M // ROWS - 1
    row_room = jnp.where(slab_index == top_slab, ROWS - HMAX, ROWS)
    random_bits = jax.random.randint(key, (CELLS,), 0, 1 << 20, dtype=jnp.int32)
    offset_rows = jnp.where(positions == top_slab * CELLS_SLAB, row_room - 1, random_bits % row_room)
    return (slab_index * ROWS + offset_rows).astype(jnp.int32)


def draw_cell_width(key, part):
    slab_count = M // ROWS
    key_cap, key_pick, key_width = jax.random.split(jax.random.fold_in(key, 7), 3)
    slab_caps = 1 + jax.random.randint(key_cap, (slab_count,), 0, WMAX, dtype=jnp.int32)
    widest = jax.random.randint(key_pick, (), 0, slab_count, dtype=jnp.int32)
    slab_caps = jnp.where(jnp.arange(slab_count, dtype=jnp.int32) == widest, WMAX, slab_caps)
    positions = jnp.arange(CELLS, dtype=jnp.int32)
    owner_slab = positions // CELLS_SLAB
    random_bits = jax.random.randint(key_width, (CELLS,), 0, 1 << 20, dtype=jnp.int32)
    widths = 1 + random_bits % slab_caps[owner_slab]
    return jnp.where(positions == widest * CELLS_SLAB, WMAX, widths).astype(jnp.int32)


def set_ends(values, key, least, top_value):
    spot = [jax.random.randint(jax.random.fold_in(key, axis), (), 0, length) for axis, length in enumerate(values.shape)]
    widest = values.shape.index(max(values.shape))
    neighbour = spot[:widest] + [(spot[widest] + 1) % values.shape[widest]] + spot[widest + 1:]
    return values.at[tuple(spot)].set(least).at[tuple(neighbour)].set(top_value)


def block_scale(key, shape, cuts, low, largest):
    def one(axis_at, blocks):
        draws = jax.random.uniform(jax.random.fold_in(jax.random.fold_in(key, 6), axis_at), (blocks,), jnp.float32, low / len(cuts), largest / len(cuts))
        return jnp.repeat(jnp.exp(draws), shape[axis_at] // blocks).reshape((-1,) + (1,) * (len(shape) - axis_at - 1))

    gain = one(*cuts[0])
    for cut in cuts[1:]:
        gain = gain * one(*cut)
    return gain


def setup_inputs(seed: int = 0) -> dict:
    key_list = jax.random.split(jax.random.key(seed), 7)
    cell_row = draw_cell_row(jax.random.fold_in(key_list[6], 71), 0)
    cell_col = set_ends(jax.random.randint(key_list[1], (CELLS,), 0, M - WMAX), jax.random.fold_in(key_list[1], 1), 0, (M - WMAX) - 1).astype(jnp.int32)
    cell_width = draw_cell_width(jax.random.fold_in(key_list[6], 71), 0)
    cell_height = set_ends(jax.random.randint(key_list[3], (CELLS,), 1, HMAX + 1), jax.random.fold_in(key_list[3], 1), 1, HMAX).astype(jnp.int32)
    cell_region = set_ends(jax.random.randint(key_list[4], (CELLS,), 0, REGIONS), jax.random.fold_in(key_list[4], 1), 0, REGIONS - 1).astype(jnp.int32)
    cell_offset = jnp.clip(1.0 * jax.random.uniform(key_list[5], (2, CELLS), jnp.float32) ** block_scale(key_list[5], (2, CELLS), ((1, 32),), -0.2, 0.2), 0.0, 1.0)
    return dict(cell_row=cell_row, cell_col=cell_col, cell_width=cell_width, cell_height=cell_height, cell_region=cell_region, cell_offset=cell_offset)


def intersect(offset_bins, fraction, extent):
    high_edge = jnp.minimum(offset_bins + 1.0, fraction + extent)
    low_edge = jnp.maximum(offset_bins, fraction)
    return jnp.maximum(high_edge - low_edge, 0.0).astype(jnp.bfloat16)

def basis_weight(length):
    freq_index = jnp.arange(length)
    return jnp.where(freq_index == 0, jnp.sqrt(1.0 / length), jnp.sqrt(2.0 / length)).astype(jnp.float32)

def dct_forward(values, axis):
    length = values.shape[axis]
    moved = jnp.moveaxis(values, axis, -1)
    doubled = jnp.concatenate([moved, jnp.flip(moved, -1)], axis=-1)
    spectral = jnp.fft.fft(doubled, axis=-1)[..., :length]
    freq_axis = jnp.arange(length).astype(jnp.float32)
    twist = jnp.exp(-1j * (jnp.pi / (2 * length)) * freq_axis)
    result = jnp.real(spectral * twist) * (0.5 * basis_weight(length))
    return jnp.moveaxis(result, -1, axis)

def dct_inverse(values, axis, sine):
    length = values.shape[axis]
    moved = jnp.moveaxis(values, axis, -1)
    freq_axis = jnp.arange(length).astype(jnp.float32)
    twisted = moved * basis_weight(length) * jnp.exp(1j * (jnp.pi / (2 * length)) * freq_axis)
    padded = jnp.concatenate([twisted, jnp.zeros_like(twisted)], axis=-1)
    summed = jnp.fft.ifft(padded, axis=-1)[..., :length] * (2 * length)
    picked = jnp.imag(summed) if sine else jnp.real(summed)
    return jnp.moveaxis(picked, -1, axis)

def reference(cell_row, cell_col, cell_width, cell_height, cell_region, cell_offset):
    span_x = jnp.arange(WMAX + 1)
    span_y = jnp.arange(HMAX + 1)
    x_intersect = intersect(span_x[None, :].astype(jnp.float32), cell_offset[0][:, None], cell_width.astype(jnp.float32)[:, None])
    y_intersect = intersect(span_y[None, :].astype(jnp.float32), cell_offset[1][:, None], cell_height.astype(jnp.float32)[:, None])
    weight = y_intersect.astype(jnp.float32)[:, :, None] * x_intersect.astype(jnp.float32)[:, None, :]
    row_index = jnp.broadcast_to(cell_row[:, None, None] + span_y[None, :, None], weight.shape)
    col_index = jnp.broadcast_to(cell_col[:, None, None] + span_x[None, None, :], weight.shape)
    region_index = jnp.broadcast_to(cell_region[:, None, None], weight.shape)
    density = jnp.zeros((REGIONS, M, M), jnp.float32).at[region_index, row_index, col_index].add(weight)
    overflow = jnp.sum(jnp.maximum(density - 1.0, 0.0)) / jnp.sum(density)
    spectrum = dct_forward(dct_forward(density, 2), 1)
    freq_axis = jnp.arange(M).astype(jnp.float32)
    p_grid = freq_axis[:, None]
    q_grid = freq_axis[None, :]
    anchor = jnp.arange(M)[:, None] + jnp.arange(M)[None, :] == 0
    step_size = jnp.pi / M
    squared = p_grid * p_grid + q_grid * q_grid
    potential_hat = jnp.where(anchor, 0.0, spectrum / (step_size * step_size * jnp.where(anchor, 1.0, squared)))
    field_x = dct_inverse(dct_inverse(potential_hat * (step_size * q_grid), 2, True), 1, False)
    field_y = dct_inverse(dct_inverse(potential_hat * (step_size * p_grid), 2, False), 1, True)
    potential = dct_inverse(dct_inverse(potential_hat, 2, False), 1, False)
    energy = jnp.sum(density * potential) / (M * M)
    rounded_x = lax.optimization_barrier(field_x.astype(jnp.bfloat16)).astype(jnp.float32)
    rounded_y = lax.optimization_barrier(field_y.astype(jnp.bfloat16)).astype(jnp.float32)
    force_x = lax.optimization_barrier(jnp.sum(weight * rounded_x[region_index, row_index, col_index], axis=(1, 2)))
    force_y = lax.optimization_barrier(jnp.sum(weight * rounded_y[region_index, row_index, col_index], axis=(1, 2)))
    return (field_x, field_y, jnp.stack([force_x, force_y]), energy, overflow)
```

```python
import functools
import math

import jax
import jax.numpy as jnp
import numpy as np
from jax import lax
from jax.experimental import pallas as pl
from jax.experimental.pallas import tpu as pltpu
from jax.sharding import PartitionSpec as P

M = 2048
REGIONS = 4
HMAX = 4
WMAX = 8
HALF = M // 2
STRIP = 32
TILE = 256
PARTS = HALF // TILE
FINE = 8192.0
AXES = ("slab", "cell")
BF = jnp.bfloat16
F32 = jnp.float32
I16 = jnp.int16
VMEM_LIMIT = 56 * 1024 * 1024


def params():
    return pltpu.CompilerParams(
        dimension_semantics=("arbitrary",), vmem_limit_bytes=VMEM_LIMIT
    )


def steps_of(bound):
    return 32700.0 / math.log2(1.0 + bound * FINE)


def encode(value, steps):
    code = jnp.minimum(jnp.log2(1.0 + jnp.abs(value) * FINE) * steps, 32767.0)
    code = jnp.where(value < 0.0, -code, code)
    return jnp.round(code).astype(jnp.int32).astype(I16)


def decode(code, steps):
    wide = code.astype(jnp.int32).astype(F32)
    size = (jnp.exp2(jnp.abs(wide) * (1.0 / steps)) - 1.0) * (1.0 / FINE)
    return jnp.where(wide < 0.0, -size, size)


def split(value):
    high = value.astype(BF)
    return high, (value - high.astype(F32)).astype(BF)


def dot(left, right):
    return lax.dot_general(left, right, (((1,), (0,)), ((), ())), preferred_element_type=F32)


def dot3(left_hi, left_lo, right_hi, right_lo):
    return dot(left_hi, right_hi) + (dot(left_lo, right_hi) + dot(left_hi, right_lo))


def base_tables():
    groups = HALF // STRIP
    unit = math.pi / (2 * M)
    turn = 4 * M
    place = (2 * np.arange(HALF) + 1)[None, :]
    freq = (2 * np.arange(HALF))[None, :]
    group = np.arange(groups)[:, None]
    inside = np.arange(STRIP)[:, None]
    gain = math.sqrt(2.0 / M)
    zero_gain = np.where(freq == 0, math.sqrt(0.5), 1.0)
    far = unit * (2 * STRIP * group * place % turn)
    far_t = unit * (2 * STRIP * group * freq % turn)
    near_even = unit * (2 * inside * place % turn)
    near_odd = unit * ((2 * inside + 1) * place % turn)
    near_t = unit * ((2 * inside + 1) * freq % turn)
    pad = np.zeros_like(far)
    outer = np.stack(
        [np.cos(far), np.sin(far), np.cos(far_t), np.sin(far_t), pad, pad, pad, pad], axis=1
    )
    inner = np.stack(
        [
            gain * np.cos(near_even),
            gain * np.sin(near_even),
            gain * np.cos(near_odd),
            gain * np.sin(near_odd),
            gain * zero_gain * np.cos(near_t),
            gain * zero_gain * np.sin(near_t),
        ]
    )
    return outer.astype(np.float32), inner.astype(np.float32)


def table_kernel(outer, inner, fwd_hi, fwd_lo, sy_hi, sy_lo, ce_hi, ce_lo, se_hi, se_lo):
    group = pl.program_id(0)

    def pair(far, near):
        cos_far = outer[0, far : far + 1, :]
        sin_far = outer[0, far + 1 : far + 2, :]
        cos_near = inner[near]
        sin_near = inner[near + 1]
        return cos_far * cos_near - sin_far * sin_near, sin_far * cos_near + cos_far * sin_near

    row = lax.broadcasted_iota(jnp.int32, (STRIP, 1), 0) + group * STRIP
    weight = jnp.where(row == 0, math.sqrt(0.5), 1.0).astype(F32)
    cos_even, sin_even = pair(0, 0)
    ce_hi[...], ce_lo[...] = split(cos_even * weight)
    se_hi[...], se_lo[...] = split(sin_even)
    cos_odd, sin_odd = pair(0, 2)
    fwd_hi[:, HALF:], fwd_lo[:, HALF:] = split(cos_odd)
    sy_hi[:, HALF:], sy_lo[:, HALF:] = split(sin_odd)
    cos_t, sin_t = pair(2, 4)
    fwd_hi[:, :HALF], fwd_lo[:, :HALF] = split(cos_t)
    sy_hi[:, :HALF], sy_lo[:, :HALF] = split(sin_t)


def make_tables():
    outer, inner = base_tables()
    wide = jax.ShapeDtypeStruct((HALF, M), BF)
    square = jax.ShapeDtypeStruct((HALF, HALF), BF)
    wide_spec = pl.BlockSpec((STRIP, M), lambda g: (g, 0))
    square_spec = pl.BlockSpec((STRIP, HALF), lambda g: (g, 0))
    return pl.pallas_call(
        table_kernel,
        grid=(HALF // STRIP,),
        in_specs=[
            pl.BlockSpec((1, 8, HALF), lambda g: (g, 0, 0)),
            pl.BlockSpec((6, STRIP, HALF), lambda g: (0, 0, 0)),
        ],
        out_specs=[wide_spec] * 4 + [square_spec] * 4,
        out_shape=[wide] * 4 + [square] * 4,
        compiler_params=params(),
        cost_estimate=pl.CostEstimate(
            flops=40 * HALF * HALF, transcendentals=0, bytes_accessed=24 * HALF * HALF
        ),
        name="tables",
    )(jnp.asarray(outer), jnp.asarray(inner))


def fold_rows(value):
    rows, cols = value.shape
    folded = jnp.sum(value.reshape(rows // 8, 8, cols), axis=0)
    out = folded[:, :128]
    for start in range(128, cols, 128):
        out = out + folded[:, start : start + 128]
    return out


def density_kernel(
    cells, row_info, fwd_hi, fwd_lo, xt, yt, codes, excess, area, dens, part_hi, part_lo, *, steps
):
    step = pl.program_id(0)
    total = cells.shape[1]
    chunk = 512

    @pl.when(step == 0)
    def _():
        place = row_info[:, 0:1]
        region = row_info[:, 1:2]
        for start in range(0, total, chunk):
            here = pl.ds(start, chunk)
            low = cells[6:7, here]
            rel = place - cells[0:1, here]
            high = jnp.minimum(rel + 1.0, low + cells[3:4, here])
            value = jnp.maximum(high - jnp.maximum(rel, low), 0.0)
            yt[:, here] = jnp.where(region == cells[4:5, here], value, 0.0).astype(BF)

    @pl.when(step < 2 * PARTS)
    def _():
        place = (step % PARTS) * TILE + lax.broadcasted_iota(jnp.int32, (TILE, 1), 0)
        place = jnp.where(step >= PARTS, M - 1 - place, place).astype(F32)
        acc = None
        for start in range(0, total, chunk):
            here = pl.ds(start, chunk)
            low = cells[5:6, here]
            rel = place - cells[1:2, here]
            high = jnp.minimum(rel + 1.0, low + cells[2:3, here])
            value = jnp.maximum(high - jnp.maximum(rel, low), 0.0).astype(BF)
            xt[:, here] = value
            part = lax.dot_general(
                yt[:, here], value, (((1,), (1,)), ((), ())), preferred_element_type=F32
            )
            acc = part if acc is None else acc + part
        dens[step] = acc

    @pl.when(step == 2 * PARTS)
    def _():
        over = jnp.zeros((8, 128), F32)
        full = jnp.zeros((8, 128), F32)
        for part in range(PARTS):
            here = pl.ds(part * TILE, TILE)
            near = dens[part]
            mirrored = dens[PARTS + part]
            even = near + mirrored
            over = over + fold_rows(
                jnp.maximum(near - 1.0, 0.0) + jnp.maximum(mirrored - 1.0, 0.0)
            )
            full = full + fold_rows(even)
            part_hi[0, :, here], part_lo[0, :, here] = split(even)
            part_hi[1, :, here], part_lo[1, :, here] = split(near - mirrored)
        excess[...] = over
        area[...] = full

    @pl.when(step >= 2 * PARTS)
    def _():
        odd = jnp.where(step >= 3 * PARTS, 1, 0)
        out = dot3(part_hi[odd], part_lo[odd], fwd_hi[...], fwd_lo[...])
        codes[...] = encode(out, steps)


def density_call(cells, row_info, tables, steps):
    total = cells.shape[1]
    rows = row_info.shape[0]
    late = lambda t: (0, jnp.maximum(t - 2 * PARTS, 0))
    whole = lambda t: (0, 0)
    small = jax.ShapeDtypeStruct((8, 128), F32)
    return pl.pallas_call(
        functools.partial(density_kernel, steps=steps),
        grid=(4 * PARTS,),
        in_specs=[
            pl.BlockSpec((8, total), whole),
            pl.BlockSpec((rows, 8), whole),
            pl.BlockSpec((HALF, TILE), late),
            pl.BlockSpec((HALF, TILE), late),
        ],
        out_specs=[
            pl.BlockSpec((TILE, total), lambda t: (jnp.minimum(t, 2 * PARTS - 1), 0)),
            pl.BlockSpec((rows, total), whole),
            pl.BlockSpec((rows, TILE), late),
            pl.BlockSpec((8, 128), whole),
            pl.BlockSpec((8, 128), whole),
        ],
        out_shape=[
            jax.ShapeDtypeStruct((M, total), BF),
            jax.ShapeDtypeStruct((rows, total), BF),
            jax.ShapeDtypeStruct((rows, M), I16),
            small,
            small,
        ],
        scratch_shapes=[
            pltpu.VMEM((2 * PARTS, rows, TILE), F32),
            pltpu.VMEM((2, rows, HALF), BF),
            pltpu.VMEM((2, rows, HALF), BF),
        ],
        compiler_params=params(),
        cost_estimate=pl.CostEstimate(
            flops=2 * rows * M * (total + 3 * HALF), transcendentals=0, bytes_accessed=1 << 24
        ),
        name="density",
    )(cells, row_info, tables[0], tables[1])


def place_rows(out, first, top, bottom, steps):
    count, rows = out.shape[0], out.shape[1]
    top = encode(top, steps)
    bottom = encode(bottom, steps)
    for inner in range(TILE // rows):
        here = slice(inner * rows, (inner + 1) * rows)
        out[first + inner] = top[here]
        out[count - 1 - first - inner] = bottom[here]


def spectrum_kernel(
    codes,
    q_row,
    ce_hi,
    ce_lo,
    co_hi,
    co_lo,
    ct_hi,
    ct_lo,
    out,
    dye_hi,
    dye_lo,
    dyo_hi,
    dyo_lo,
    energy,
    even_hi,
    even_lo,
    odd_hi,
    odd_lo,
    dxe_hi,
    dxe_lo,
    dxo_hi,
    dxo_lo,
    *,
    fwd_steps,
    back_steps,
):
    step = pl.program_id(0)
    count, rows = codes.shape[0], codes.shape[1]

    @pl.when(step == 0)
    def _():
        for block in range(count // 2):
            here = pl.ds(block * rows, rows)
            near = decode(codes[block], fwd_steps)
            mirrored = decode(codes[count - 1 - block], fwd_steps)
            even_hi[here, :], even_lo[here, :] = split(near + mirrored)
            odd_hi[here, :], odd_lo[here, :] = split(near - mirrored)
        energy[...] = jnp.zeros((8, 128), F32)

    @pl.when(step < PARTS)
    def _():
        unit = math.pi / M
        q = q_row[0:1, :]
        first = lax.broadcasted_iota(jnp.int32, (TILE, 1), 0) + step * TILE
        here = pl.ds(pl.multiple_of(step * TILE, TILE), TILE)

        def solve(spectrum, p):
            squared = p * p + q * q
            inverse = jnp.where(squared == 0.0, 0.0, 1.0 / jnp.where(squared == 0.0, 1.0, squared))
            scaled = spectrum * inverse
            return scaled * (q * (1.0 / unit)), scaled * (p * (1.0 / unit)), spectrum * scaled

        spec = dot3(ce_hi[...], ce_lo[...], even_hi[...], even_lo[...])
        drive_x, drive_y, power = solve(spec, (2 * first).astype(F32))
        dxe_hi[here, :], dxe_lo[here, :] = split(drive_x)
        dye_hi[...], dye_lo[...] = split(drive_y)
        spec = dot3(co_hi[...], co_lo[...], odd_hi[...], odd_lo[...])
        drive_x, drive_y, more = solve(spec, (2 * first + 1).astype(F32))
        dxo_hi[here, :], dxo_lo[here, :] = split(drive_x)
        dyo_hi[...], dyo_lo[...] = split(drive_y)
        both = power + more
        if both.shape[1] % 128:
            both = jnp.concatenate(
                [both, jnp.zeros((TILE, 128 - both.shape[1] % 128), F32)], axis=1
            )
        energy[...] += fold_rows(both) * (1.0 / (unit * unit))

    @pl.when(step >= PARTS)
    def _():
        even = dot3(ct_hi[...], ct_lo[...], dxe_hi[...], dxe_lo[...])
        odd = dot3(co_hi[...], co_lo[...], dxo_hi[...], dxo_lo[...])
        first = (step - PARTS) * (TILE // rows)
        place_rows(out, first, even + odd, even - odd, back_steps)


def spectrum_call(codes, q_row, tables, fwd_steps, back_steps):
    fwd_hi, fwd_lo, _, _, ce_hi, ce_lo, _, _ = tables
    count, rows, cols = codes.shape
    early = lambda t: (jnp.minimum(t, PARTS - 1), 0)
    drive = jax.ShapeDtypeStruct((HALF, cols), BF)
    return pl.pallas_call(
        functools.partial(spectrum_kernel, fwd_steps=fwd_steps, back_steps=back_steps),
        grid=(2 * PARTS,),
        in_specs=[
            pl.BlockSpec((count, rows, cols), lambda t: (0, 0, 0)),
            pl.BlockSpec((8, cols), lambda t: (0, 0)),
        ]
        + [pl.BlockSpec((TILE, HALF), early)] * 2
        + [pl.BlockSpec((TILE, HALF), lambda t: (t % PARTS, 1))] * 2
        + [pl.BlockSpec((TILE, HALF), lambda t: (jnp.maximum(t - PARTS, 0), 0))] * 2,
        out_specs=[pl.BlockSpec((count, rows, cols), lambda t: (0, 0, 0))]
        + [pl.BlockSpec((TILE, cols), early)] * 4
        + [pl.BlockSpec((8, 128), lambda t: (0, 0))],
        out_shape=[jax.ShapeDtypeStruct((count, rows, cols), I16)]
        + [drive] * 4
        + [jax.ShapeDtypeStruct((8, 128), F32)],
        scratch_shapes=[pltpu.VMEM((HALF, cols), BF)] * 8,
        compiler_params=params(),
        cost_estimate=pl.CostEstimate(
            flops=24 * HALF * HALF * cols, transcendentals=0, bytes_accessed=1 << 24
        ),
        name="spectrum",
    )(codes, q_row, ce_hi, ce_lo, fwd_hi, fwd_lo, fwd_hi, fwd_lo)


def sine_kernel(
    dye_hi, dye_lo, dyo_hi, dyo_lo, se_hi, se_lo, so_hi, so_lo, out, *, back_steps
):
    even = dot3(se_hi[...], se_lo[...], dye_hi[...], dye_lo[...])
    odd = dot3(so_hi[...], so_lo[...], dyo_hi[...], dyo_lo[...])
    first = pl.program_id(0) * (TILE // out.shape[1])
    place_rows(out, first, odd + even, odd - even, back_steps)


def sine_call(drives, tables, count, rows, back_steps):
    sy_hi, sy_lo = tables[2], tables[3]
    cols = drives[0].shape[1]
    return pl.pallas_call(
        functools.partial(sine_kernel, back_steps=back_steps),
        grid=(PARTS,),
        in_specs=[pl.BlockSpec((HALF, cols), lambda t: (0, 0))] * 4
        + [pl.BlockSpec((TILE, HALF), lambda t: (t, 0))] * 2
        + [pl.BlockSpec((TILE, HALF), lambda t: (t, 1))] * 2,
        out_specs=pl.BlockSpec((count, rows, cols), lambda t: (0, 0, 0)),
        out_shape=jax.ShapeDtypeStruct((count, rows, cols), I16),
        compiler_params=params(),
        cost_estimate=pl.CostEstimate(
            flops=12 * HALF * HALF * cols, transcendentals=0, bytes_accessed=1 << 23
        ),
        name="sine_rows",
    )(*drives, sy_hi, sy_lo, sy_hi, sy_lo)


def field_kernel(
    flag,
    codes,
    even_hi,
    even_lo,
    odd_hi,
    odd_lo,
    x_near,
    x_far,
    yt,
    field,
    force,
    part_hi,
    part_lo,
    acc,
    *,
    steps,
    rows,
    sine,
):
    step = pl.program_id(0)
    flipped = flag[0] == 1

    @pl.when(step == 0)
    def _():
        for part in range(2):
            for block in range(PARTS):
                here = pl.ds(block * TILE, TILE)
                value = decode(codes[:, part * HALF + block * TILE :][:, :TILE], steps)
                part_hi[part, :, here], part_lo[part, :, here] = split(value)

    even = dot3(part_hi[0], part_lo[0], even_hi[...], even_lo[...])
    odd = dot3(part_hi[1], part_lo[1], odd_hi[...], odd_lo[...])
    near = even + odd
    far = odd - even if sine else even - odd
    gathered = dot(near.astype(BF), x_near[...]) + dot(far.astype(BF), x_far[...])

    @pl.when(step == 0)
    def _():
        acc[...] = gathered

    @pl.when(step > 0)
    def _():
        acc[...] += gathered

    lane = 127 - lax.broadcasted_iota(jnp.int32, (8, 128), 1)
    sub = lax.broadcasted_iota(jnp.int32, (8, 128), 0)
    sub = jnp.where(flipped, 7 - sub, sub)
    for region in range(near.shape[0] // rows):
        for block in range(rows // 8):
            start = region * rows + 8 * block
            target = region * rows + jnp.where(flipped, rows - 8 - 8 * block, 8 * block)
            target = pl.multiple_of(target, 8)
            for tile in range(TILE // 128):
                piece = near[start : start + 8, tile * 128 : (tile + 1) * 128]
                piece = jnp.take_along_axis(piece, sub, axis=0)
                col = pl.multiple_of(step * TILE + tile * 128, 128)
                field[pl.ds(target, 8), pl.ds(col, 128)] = piece
                piece = far[start : start + 8, tile * 128 : (tile + 1) * 128]
                piece = jnp.take_along_axis(piece, sub, axis=0)
                piece = jnp.take_along_axis(piece, lane, axis=1)
                col = pl.multiple_of(M - 128 - step * TILE - tile * 128, 128)
                field[pl.ds(target, 8), pl.ds(col, 128)] = piece

    @pl.when(step == PARTS - 1)
    def _():
        force[...] = jnp.sum(yt[...].astype(F32) * acc[...], axis=0, keepdims=True)


def field_call(flag, codes, even, odd, xt, yt, steps, rows, sine):
    lines, total = yt.shape
    return pl.pallas_call(
        functools.partial(field_kernel, steps=steps, rows=rows, sine=sine),
        grid=(PARTS,),
        in_specs=[
            pl.BlockSpec(memory_space=pltpu.SMEM),
            pl.BlockSpec((lines, M), lambda t: (0, 0)),
        ]
        + [pl.BlockSpec((HALF, TILE), lambda t: (0, t))] * 2
        + [pl.BlockSpec((HALF, TILE), lambda t: (0, PARTS + t))] * 2
        + [
            pl.BlockSpec((TILE, total), lambda t: (t, 0)),
            pl.BlockSpec((TILE, total), lambda t: (PARTS + t, 0)),
            pl.BlockSpec((lines, total), lambda t: (0, 0)),
        ],
        out_specs=[
            pl.BlockSpec((lines, M), lambda t: (0, 0)),
            pl.BlockSpec((1, total), lambda t: (0, 0)),
        ],
        out_shape=[
            jax.ShapeDtypeStruct((lines, M), F32),
            jax.ShapeDtypeStruct((1, total), F32),
        ],
        scratch_shapes=[
            pltpu.VMEM((2, lines, HALF), BF),
            pltpu.VMEM((2, lines, HALF), BF),
            pltpu.VMEM((lines, total), F32),
        ],
        compiler_params=params(),
        cost_estimate=pl.CostEstimate(
            flops=2 * lines * M * (total + 3 * HALF), transcendentals=0, bytes_accessed=1 << 24
        ),
        name="field_x" if sine else "field_y",
    )(flag, codes, even[0], even[1], odd[0], odd[1], xt, xt, yt)


def exchange(blocks):
    return lax.all_to_all(blocks, AXES, split_axis=0, concat_axis=0, tiled=True)


def body(cell_row, cell_col, cell_width, cell_height, cell_region, cell_offset):
    slab_count = lax.axis_size("slab")
    cell_count = lax.axis_size("cell")
    count = slab_count * cell_count
    device = lax.axis_index("slab") * cell_count + lax.axis_index("cell")
    rows = M // count
    own = cell_row.shape[0]
    lines = REGIONS * rows
    gain = math.sqrt(2.0 / M)
    fwd_steps = steps_of(2.1 * own * cell_count * WMAX * gain)
    back_steps = steps_of(gain**3 * own * count * WMAX * HMAX * 1.1 * M / math.pi * 8.5)

    ints = [cell_row, cell_col, cell_width, cell_height, cell_region]
    mine = jnp.concatenate(
        [jnp.stack(ints).astype(F32), cell_offset, jnp.zeros((1, own), F32)], axis=0
    )
    pieces = [mine]
    back_moves = []
    for turn in range(1, cell_count):
        pairs = [
            (slab * cell_count + c, slab * cell_count + (c + turn) % cell_count)
            for slab in range(slab_count)
            for c in range(cell_count)
        ]
        pieces.append(lax.ppermute(mine, AXES, pairs))
        back_moves.append([(b, a) for a, b in pairs])
    for c in range(cell_count):
        pairs = [
            (slab * cell_count + c, (slab + 1) * cell_count) for slab in range(slab_count - 1)
        ]
        pieces.append(lax.ppermute(mine, AXES, pairs))
        back_moves.append([(b, a) for a, b in pairs])
    tables = make_tables()
    cells = jnp.concatenate(pieces, axis=1)

    flipped = device >= count // 2
    line = lax.iota(jnp.int32, lines)
    inside = line % rows
    place = device * rows + jnp.where(flipped, rows - 1 - inside, inside)
    row_info = jnp.stack([place.astype(F32), (line // rows).astype(F32)] + [place * 0.0] * 6, axis=1)
    q_local = lax.iota(jnp.int32, lines) % rows
    q_value = jnp.where(
        flipped, 2 * (rows * (device - count // 2) + q_local) + 1, 2 * (rows * device + q_local)
    )
    q_row = jnp.broadcast_to(q_value.astype(F32)[None, :], (8, lines))
    flag = jnp.where(flipped, 1, 0).astype(jnp.int32).reshape(1)

    xt, yt, codes, excess, area = density_call(cells, row_info, tables, fwd_steps)
    blocks = jnp.transpose(codes.reshape(REGIONS, rows, count, rows), (2, 1, 0, 3))
    arrived = exchange(blocks.reshape(count, rows, lines))
    drive = spectrum_call(arrived, q_row, tables, fwd_steps, back_steps)
    along_x = exchange(drive[0])
    along_y = exchange(sine_call(drive[1:5], tables, count, rows, back_steps))

    sums = jnp.stack([jnp.sum(excess), jnp.sum(area), jnp.sum(drive[5])])
    sums = jnp.pad(sums, (0, 125))
    sums = jnp.sum(exchange(jnp.broadcast_to(sums, (count, 8, 128))), axis=0)[0]

    def lines_of(blocks):
        shaped = blocks.reshape(count, rows, REGIONS, rows)
        return jnp.transpose(shaped, (2, 1, 0, 3)).reshape(lines, M)

    fwd, sy, ce, se = tables[0:2], tables[2:4], tables[4:6], tables[6:8]
    field_x, force_x = field_call(flag, lines_of(along_x), se, sy, xt, yt, back_steps, rows, True)
    field_y, force_y = field_call(flag, lines_of(along_y), ce, fwd, xt, yt, back_steps, rows, False)
    partial = jnp.concatenate([force_x, force_y], axis=0)
    cell_force = partial[:, :own]
    for index, pairs in enumerate(back_moves):
        piece = partial[:, (index + 1) * own : (index + 2) * own]
        cell_force = cell_force + lax.ppermute(piece, AXES, pairs)
    energy = sums[2] / (M * M)
    overflow = sums[0] / sums[1]
    shape = (REGIONS, rows, M)
    return (field_x.reshape(shape), field_y.reshape(shape), cell_force, energy, overflow)


def solution(mesh):
    return jax.shard_map(
        body,
        mesh=mesh,
        in_specs=(
            P(("slab", "cell")),
            P(("slab", "cell")),
            P(("slab", "cell")),
            P(("slab", "cell")),
            P(("slab", "cell")),
            P(None, ("slab", "cell")),
        ),
        out_specs=(
            P(None, ("slab", "cell"), None),
            P(None, ("slab", "cell"), None),
            P(None, ("slab", "cell")),
            P(),
            P(),
        ),
        check_vma=False,
    )
```

```python
import functools
import math

import jax
import jax.numpy as jnp
import numpy as np
from jax import lax
from jax.experimental import pallas as pl
from jax.experimental.pallas import tpu as pltpu
from jax.sharding import PartitionSpec as P

M = 2048
REGIONS = 4
HMAX = 4
WMAX = 8
HALF = M // 2
STRIP = 32
BAND = 4
TILE = 256
PARTS = HALF // TILE
FINE = 8192.0
AXES = ("slab", "cell")
BF = jnp.bfloat16
F32 = jnp.float32
I16 = jnp.int16
VMEM_LIMIT = 56 * 1024 * 1024


def params():
    return pltpu.CompilerParams(
        dimension_semantics=("arbitrary",), vmem_limit_bytes=VMEM_LIMIT
    )


def steps_of(bound):
    return 32700.0 / math.log2(1.0 + bound * FINE)


def encode_wide(value, steps):
    code = jnp.minimum(jnp.log2(1.0 + jnp.abs(value) * FINE) * steps, 32767.0)
    return jnp.round(jnp.where(value < 0.0, -code, code))


def encode(value, steps):
    return encode_wide(value, steps).astype(jnp.int32).astype(I16)


def packable(rows):
    return rows == 64 and REGIONS == 4


def swap_halves(values):
    lane = lax.broadcasted_iota(jnp.int32, values[0].shape, 1)
    turned = [pltpu.roll(value, 64, 1) for value in values]
    first = jnp.where(lane < 64, values[0], turned[1])
    second = jnp.where(lane < 64, turned[0], values[1])
    return first, second


def pack(out, value):
    for pair in range(TILE // 128):
        tile = value[:, pair * 128 : (pair + 1) * 128]
        for half in range(2):
            here = pl.ds(half * 128, 128)
            low = tile[half * 128 : half * 128 + 64]
            high = tile[half * 128 + 64 : half * 128 + 128]
            first, second = swap_halves((low, high))
            out[2 * pair, :, here] = first.astype(jnp.int32).astype(I16)
            out[2 * pair + 1, :, here] = second.astype(jnp.int32).astype(I16)


def decode(code, steps):
    wide = code.astype(jnp.int32).astype(F32)
    size = (jnp.exp2(jnp.abs(wide) * (1.0 / steps)) - 1.0) * (1.0 / FINE)
    return jnp.where(wide < 0.0, -size, size)


def split(value):
    high = value.astype(BF)
    return high, (value - high.astype(F32)).astype(BF)


def dot(left, right):
    return lax.dot_general(left, right, (((1,), (0,)), ((), ())), preferred_element_type=F32)


def dot3(left_hi, left_lo, right_hi, right_lo):
    return dot(left_hi, right_hi) + (dot(left_lo, right_hi) + dot(left_hi, right_lo))


def base_tables():
    groups = HALF // STRIP
    unit = math.pi / (2 * M)
    turn = 4 * M
    place = (2 * np.arange(HALF) + 1)[None, :]
    freq = (2 * np.arange(HALF))[None, :]
    group = np.arange(groups)[:, None]
    inside = np.arange(STRIP)[:, None]
    gain = math.sqrt(2.0 / M)
    zero_gain = np.where(freq == 0, math.sqrt(0.5), 1.0)
    far = unit * (2 * STRIP * group * place % turn)
    far_t = unit * (2 * STRIP * group * freq % turn)
    near_even = unit * (2 * inside * place % turn)
    near_odd = unit * ((2 * inside + 1) * place % turn)
    near_t = unit * ((2 * inside + 1) * freq % turn)
    outer = np.stack([np.cos(far), np.sin(far), np.cos(far_t), np.sin(far_t)], axis=1)
    inner = np.stack(
        [
            gain * np.cos(near_even),
            gain * np.sin(near_even),
            gain * np.cos(near_odd),
            gain * np.sin(near_odd),
            gain * zero_gain * np.cos(near_t),
            gain * zero_gain * np.sin(near_t),
        ]
    )
    return outer.astype(np.float32), inner.astype(np.float32)


def table_kernel(outer, inner, fwd_hi, fwd_lo, sy_hi, sy_lo, ce_hi, ce_lo, se_hi, se_lo):
    for group in range(BAND):
        here = pl.ds(group * STRIP, STRIP)

        def pair(far, near):
            cos_far = outer[group, far : far + 1, :]
            sin_far = outer[group, far + 1 : far + 2, :]
            cos_near = inner[near]
            sin_near = inner[near + 1]
            return cos_far * cos_near - sin_far * sin_near, sin_far * cos_near + cos_far * sin_near

        cos_even, sin_even = pair(0, 0)
        if group == 0:
            row = lax.broadcasted_iota(jnp.int32, (STRIP, 1), 0) + pl.program_id(0) * STRIP
            cos_even = cos_even * jnp.where(row == 0, math.sqrt(0.5), 1.0).astype(F32)
        ce_hi[here, :], ce_lo[here, :] = split(cos_even)
        se_hi[here, :], se_lo[here, :] = split(sin_even)
        cos_odd, sin_odd = pair(0, 2)
        fwd_hi[here, HALF:], fwd_lo[here, HALF:] = split(cos_odd)
        sy_hi[here, HALF:], sy_lo[here, HALF:] = split(sin_odd)
        cos_t, sin_t = pair(2, 4)
        fwd_hi[here, :HALF], fwd_lo[here, :HALF] = split(cos_t)
        sy_hi[here, :HALF], sy_lo[here, :HALF] = split(sin_t)


def make_tables():
    outer, inner = base_tables()
    wide = jax.ShapeDtypeStruct((HALF, M), BF)
    square = jax.ShapeDtypeStruct((HALF, HALF), BF)
    wide_spec = pl.BlockSpec((BAND * STRIP, M), lambda g: (g, 0))
    square_spec = pl.BlockSpec((BAND * STRIP, HALF), lambda g: (g, 0))
    return pl.pallas_call(
        table_kernel,
        grid=(HALF // (BAND * STRIP),),
        in_specs=[
            pl.BlockSpec((BAND, 4, HALF), lambda g: (g, 0, 0)),
            pl.BlockSpec((6, STRIP, HALF), lambda g: (0, 0, 0)),
        ],
        out_specs=[wide_spec] * 4 + [square_spec] * 4,
        out_shape=[wide] * 4 + [square] * 4,
        compiler_params=params(),
        cost_estimate=pl.CostEstimate(
            flops=40 * HALF * HALF, transcendentals=0, bytes_accessed=24 * HALF * HALF
        ),
        name="tables",
    )(jnp.asarray(outer), jnp.asarray(inner))


def fold_rows(value):
    rows, cols = value.shape
    folded = jnp.sum(value.reshape(rows // 8, 8, cols), axis=0)
    out = folded[:, :128]
    for start in range(128, cols, 128):
        out = out + folded[:, start : start + 128]
    return out


def density_kernel(
    device,
    cells,
    fwd_hi,
    fwd_lo,
    xt,
    yt,
    codes,
    sums,
    dens,
    part_hi,
    part_lo,
    *,
    steps,
    rows,
    count,
):
    step = pl.program_id(0)
    total = cells.shape[1]
    chunk = 512

    @pl.when(step == 0)
    def _():
        line = lax.broadcasted_iota(jnp.int32, (yt.shape[0], 1), 0)
        inside = line & (rows - 1)
        place = jnp.where(device[0] >= count // 2, rows - 1 - inside, inside) + device[0] * rows
        place = place.astype(F32)
        region = (line >> (rows.bit_length() - 1)).astype(F32)
        for start in range(0, total, chunk):
            here = pl.ds(start, chunk)
            low = cells[6:7, here]
            rel = place - cells[0:1, here]
            high = jnp.minimum(rel + 1.0, low + cells[3:4, here])
            value = jnp.maximum(high - jnp.maximum(rel, low), 0.0)
            yt[:, here] = jnp.where(region == cells[4:5, here], value, 0.0).astype(BF)

    @pl.when(step < 2 * PARTS)
    def _():
        place = (step % PARTS) * TILE + lax.broadcasted_iota(jnp.int32, (TILE, 1), 0)
        place = jnp.where(step >= PARTS, M - 1 - place, place).astype(F32)
        acc = None
        for start in range(0, total, chunk):
            here = pl.ds(start, chunk)
            low = cells[5:6, here]
            rel = place - cells[1:2, here]
            high = jnp.minimum(rel + 1.0, low + cells[2:3, here])
            value = jnp.maximum(high - jnp.maximum(rel, low), 0.0).astype(BF)
            xt[:, here] = value
            part = lax.dot_general(
                yt[:, here], value, (((1,), (1,)), ((), ())), preferred_element_type=F32
            )
            acc = part if acc is None else acc + part
        dens[step] = acc

    @pl.when(step == 2 * PARTS)
    def _():
        over = jnp.zeros((8, 128), F32)
        full = jnp.zeros((8, 128), F32)
        for part in range(PARTS):
            here = pl.ds(part * TILE, TILE)
            near = dens[part]
            mirrored = dens[PARTS + part]
            even = near + mirrored
            over = over + fold_rows(
                jnp.maximum(near - 1.0, 0.0) + jnp.maximum(mirrored - 1.0, 0.0)
            )
            full = full + fold_rows(even)
            part_hi[0, :, here], part_lo[0, :, here] = split(even)
            part_hi[1, :, here], part_lo[1, :, here] = split(near - mirrored)
        sums[0:8, :] = over
        sums[8:16, :] = full

    @pl.when(step >= 2 * PARTS)
    def _():
        odd = jnp.where(step >= 3 * PARTS, 1, 0)
        out = dot3(part_hi[odd], part_lo[odd], fwd_hi[...], fwd_lo[...])
        if packable(rows):
            pack(codes, encode_wide(out, steps))
        else:
            codes[...] = encode(out, steps)


def density_call(device, cells, tables, rows, count, steps):
    total = cells.shape[1]
    lines = REGIONS * rows
    late = lambda t: (0, jnp.maximum(t - 2 * PARTS, 0))
    whole = lambda t: (0, 0)
    if packable(rows):
        code_spec = pl.BlockSpec(
            (TILE // rows, rows, lines), lambda t: (jnp.maximum(t - 2 * PARTS, 0), 0, 0)
        )
        code_shape = (count, rows, lines)
    else:
        code_spec = pl.BlockSpec((lines, TILE), late)
        code_shape = (lines, M)
    return pl.pallas_call(
        functools.partial(density_kernel, steps=steps, rows=rows, count=count),
        grid=(4 * PARTS,),
        in_specs=[
            pl.BlockSpec(memory_space=pltpu.SMEM),
            pl.BlockSpec((8, total), whole),
            pl.BlockSpec((HALF, TILE), late),
            pl.BlockSpec((HALF, TILE), late),
        ],
        out_specs=[
            pl.BlockSpec((TILE, total), lambda t: (jnp.minimum(t, 2 * PARTS - 1), 0)),
            pl.BlockSpec((lines, total), whole),
            code_spec,
            pl.BlockSpec((16, 128), whole),
        ],
        out_shape=[
            jax.ShapeDtypeStruct((M, total), BF),
            jax.ShapeDtypeStruct((lines, total), BF),
            jax.ShapeDtypeStruct(code_shape, I16),
            jax.ShapeDtypeStruct((16, 128), F32),
        ],
        scratch_shapes=[
            pltpu.VMEM((2 * PARTS, lines, TILE), F32),
            pltpu.VMEM((2, lines, HALF), BF),
            pltpu.VMEM((2, lines, HALF), BF),
        ],
        compiler_params=params(),
        cost_estimate=pl.CostEstimate(
            flops=2 * lines * M * (total + 3 * HALF), transcendentals=0, bytes_accessed=1 << 24
        ),
        name="density",
    )(device, cells, tables[0], tables[1])


def place_rows(out, first, top, bottom, steps):
    count, rows = out.shape[0], out.shape[1]
    top = encode(top, steps)
    bottom = encode(bottom, steps)
    for inner in range(TILE // rows):
        here = slice(inner * rows, (inner + 1) * rows)
        out[first + inner] = top[here]
        out[count - 1 - first - inner] = bottom[here]


def spectrum_kernel(
    device,
    codes,
    ce_hi,
    ce_lo,
    co_hi,
    co_lo,
    ct_hi,
    ct_lo,
    out,
    dye_hi,
    dye_lo,
    dyo_hi,
    dyo_lo,
    energy,
    even_hi,
    even_lo,
    odd_hi,
    odd_lo,
    dxe_hi,
    dxe_lo,
    dxo_hi,
    dxo_lo,
    *,
    fwd_steps,
    back_steps,
):
    step = pl.program_id(0)
    count, rows = codes.shape[0], codes.shape[1]

    @pl.when(step == 0)
    def _():
        for block in range(count // 2):
            here = pl.ds(block * rows, rows)
            near = decode(codes[block], fwd_steps)
            mirrored = decode(codes[count - 1 - block], fwd_steps)
            even_hi[here, :], even_lo[here, :] = split(near + mirrored)
            odd_hi[here, :], odd_lo[here, :] = split(near - mirrored)
        energy[...] = jnp.zeros((8, 128), F32)

    @pl.when(step < PARTS)
    def _():
        unit = math.pi / M
        lane = lax.broadcasted_iota(jnp.int32, (1, codes.shape[2]), 1) & (rows - 1)
        odd = jnp.where(device[0] >= count // 2, 1, 0)
        q = (2 * (rows * (device[0] - odd * (count // 2)) + lane) + odd).astype(F32)
        first = lax.broadcasted_iota(jnp.int32, (TILE, 1), 0) + step * TILE
        here = pl.ds(pl.multiple_of(step * TILE, TILE), TILE)

        def solve(spectrum, p):
            squared = p * p + q * q
            inverse = jnp.where(squared == 0.0, 0.0, 1.0 / jnp.where(squared == 0.0, 1.0, squared))
            scaled = spectrum * inverse
            return scaled * (q * (1.0 / unit)), scaled * (p * (1.0 / unit)), spectrum * scaled

        spec = dot3(ce_hi[...], ce_lo[...], even_hi[...], even_lo[...])
        drive_x, drive_y, power = solve(spec, (2 * first).astype(F32))
        dxe_hi[here, :], dxe_lo[here, :] = split(drive_x)
        dye_hi[...], dye_lo[...] = split(drive_y)
        spec = dot3(co_hi[...], co_lo[...], odd_hi[...], odd_lo[...])
        drive_x, drive_y, more = solve(spec, (2 * first + 1).astype(F32))
        dxo_hi[here, :], dxo_lo[here, :] = split(drive_x)
        dyo_hi[...], dyo_lo[...] = split(drive_y)
        both = power + more
        if both.shape[1] % 128:
            both = jnp.concatenate(
                [both, jnp.zeros((TILE, 128 - both.shape[1] % 128), F32)], axis=1
            )
        energy[...] += fold_rows(both) * (1.0 / (unit * unit))

    @pl.when(step >= PARTS)
    def _():
        even = dot3(ct_hi[...], ct_lo[...], dxe_hi[...], dxe_lo[...])
        odd = dot3(co_hi[...], co_lo[...], dxo_hi[...], dxo_lo[...])
        first = (step - PARTS) * (TILE // rows)
        place_rows(out, first, even + odd, even - odd, back_steps)


def spectrum_call(device, codes, tables, fwd_steps, back_steps):
    fwd_hi, fwd_lo, _, _, ce_hi, ce_lo, _, _ = tables
    count, rows, cols = codes.shape
    early = lambda t: (jnp.minimum(t, PARTS - 1), 0)
    drive = jax.ShapeDtypeStruct((HALF, cols), BF)
    return pl.pallas_call(
        functools.partial(spectrum_kernel, fwd_steps=fwd_steps, back_steps=back_steps),
        grid=(2 * PARTS,),
        in_specs=[
            pl.BlockSpec(memory_space=pltpu.SMEM),
            pl.BlockSpec((count, rows, cols), lambda t: (0, 0, 0)),
        ]
        + [pl.BlockSpec((TILE, HALF), early)] * 2
        + [pl.BlockSpec((TILE, HALF), lambda t: (t % PARTS, 1))] * 2
        + [pl.BlockSpec((TILE, HALF), lambda t: (jnp.maximum(t - PARTS, 0), 0))] * 2,
        out_specs=[pl.BlockSpec((count, rows, cols), lambda t: (0, 0, 0))]
        + [pl.BlockSpec((TILE, cols), early)] * 4
        + [pl.BlockSpec((8, 128), lambda t: (0, 0))],
        out_shape=[jax.ShapeDtypeStruct((count, rows, cols), I16)]
        + [drive] * 4
        + [jax.ShapeDtypeStruct((8, 128), F32)],
        scratch_shapes=[pltpu.VMEM((HALF, cols), BF)] * 8,
        compiler_params=params(),
        cost_estimate=pl.CostEstimate(
            flops=24 * HALF * HALF * cols, transcendentals=0, bytes_accessed=1 << 24
        ),
        name="spectrum",
    )(device, codes, ce_hi, ce_lo, fwd_hi, fwd_lo, fwd_hi, fwd_lo)


def sine_kernel(
    dye_hi, dye_lo, dyo_hi, dyo_lo, se_hi, se_lo, so_hi, so_lo, out, *, back_steps
):
    even = dot3(se_hi[...], se_lo[...], dye_hi[...], dye_lo[...])
    odd = dot3(so_hi[...], so_lo[...], dyo_hi[...], dyo_lo[...])
    first = pl.program_id(0) * (TILE // out.shape[1])
    place_rows(out, first, odd + even, odd - even, back_steps)


def sine_call(drives, tables, count, rows, back_steps):
    sy_hi, sy_lo = tables[2], tables[3]
    cols = drives[0].shape[1]
    return pl.pallas_call(
        functools.partial(sine_kernel, back_steps=back_steps),
        grid=(PARTS,),
        in_specs=[pl.BlockSpec((HALF, cols), lambda t: (0, 0))] * 4
        + [pl.BlockSpec((TILE, HALF), lambda t: (t, 0))] * 2
        + [pl.BlockSpec((TILE, HALF), lambda t: (t, 1))] * 2,
        out_specs=pl.BlockSpec((count, rows, cols), lambda t: (0, 0, 0)),
        out_shape=jax.ShapeDtypeStruct((count, rows, cols), I16),
        compiler_params=params(),
        cost_estimate=pl.CostEstimate(
            flops=12 * HALF * HALF * cols, transcendentals=0, bytes_accessed=1 << 23
        ),
        name="sine_rows",
    )(*drives, sy_hi, sy_lo, sy_hi, sy_lo)


def field_kernel(
    device,
    codes,
    even_hi,
    even_lo,
    odd_hi,
    odd_lo,
    x_near,
    x_far,
    yt,
    field,
    force,
    part_hi,
    part_lo,
    acc,
    *,
    steps,
    rows,
    count,
    sine,
):
    step = pl.program_id(0)
    flipped = device[0] >= count // 2

    @pl.when(step == 0)
    def _():
        if packable(rows):
            for pair in range(count // 2):
                near = decode(codes[2 * pair], steps)
                far = decode(codes[2 * pair + 1], steps)
                part = 2 * pair // (count // 2)
                here = pl.ds((pair % (count // 4)) * 128, 128)
                for half in range(2):
                    lanes = slice(half * 128, (half + 1) * 128)
                    for inner, value in enumerate(swap_halves((near[:, lanes], far[:, lanes]))):
                        lines = pl.ds((2 * half + inner) * rows, rows)
                        part_hi[part, lines, here], part_lo[part, lines, here] = split(value)
        else:
            for part in range(2):
                for block in range(PARTS):
                    here = pl.ds(block * TILE, TILE)
                    value = decode(codes[:, part * HALF + block * TILE :][:, :TILE], steps)
                    part_hi[part, :, here], part_lo[part, :, here] = split(value)

    even = dot3(part_hi[0], part_lo[0], even_hi[...], even_lo[...])
    odd = dot3(part_hi[1], part_lo[1], odd_hi[...], odd_lo[...])
    near = even + odd
    far = odd - even if sine else even - odd
    gathered = dot(near.astype(BF), x_near[...]) + dot(far.astype(BF), x_far[...])

    @pl.when(step == 0)
    def _():
        acc[...] = gathered

    @pl.when(step > 0)
    def _():
        acc[...] += gathered

    lane = 127 - lax.broadcasted_iota(jnp.int32, (8, 128), 1)
    sub = lax.broadcasted_iota(jnp.int32, (8, 128), 0)
    sub = jnp.where(flipped, 7 - sub, sub)
    for region in range(near.shape[0] // rows):
        for block in range(rows // 8):
            start = region * rows + 8 * block
            target = region * rows + jnp.where(flipped, rows - 8 - 8 * block, 8 * block)
            target = pl.multiple_of(target, 8)
            for tile in range(TILE // 128):
                piece = near[start : start + 8, tile * 128 : (tile + 1) * 128]
                piece = jnp.take_along_axis(piece, sub, axis=0)
                col = pl.multiple_of(step * TILE + tile * 128, 128)
                field[pl.ds(target, 8), pl.ds(col, 128)] = piece
                piece = far[start : start + 8, tile * 128 : (tile + 1) * 128]
                piece = jnp.take_along_axis(piece, sub, axis=0)
                piece = jnp.take_along_axis(piece, lane, axis=1)
                col = pl.multiple_of(M - 128 - step * TILE - tile * 128, 128)
                field[pl.ds(target, 8), pl.ds(col, 128)] = piece

    @pl.when(step == PARTS - 1)
    def _():
        force[...] = jnp.sum(yt[...].astype(F32) * acc[...], axis=0, keepdims=True)


def field_call(device, codes, even, odd, xt, yt, steps, rows, count, sine):
    lines, total = yt.shape
    zeros = (0,) * codes.ndim
    return pl.pallas_call(
        functools.partial(field_kernel, steps=steps, rows=rows, count=count, sine=sine),
        grid=(PARTS,),
        in_specs=[
            pl.BlockSpec(memory_space=pltpu.SMEM),
            pl.BlockSpec(codes.shape, lambda t: zeros),
        ]
        + [pl.BlockSpec((HALF, TILE), lambda t: (0, t))] * 2
        + [pl.BlockSpec((HALF, TILE), lambda t: (0, PARTS + t))] * 2
        + [
            pl.BlockSpec((TILE, total), lambda t: (t, 0)),
            pl.BlockSpec((TILE, total), lambda t: (PARTS + t, 0)),
            pl.BlockSpec((lines, total), lambda t: (0, 0)),
        ],
        out_specs=[
            pl.BlockSpec((lines, M), lambda t: (0, 0)),
            pl.BlockSpec((1, total), lambda t: (0, 0)),
        ],
        out_shape=[
            jax.ShapeDtypeStruct((lines, M), F32),
            jax.ShapeDtypeStruct((1, total), F32),
        ],
        scratch_shapes=[
            pltpu.VMEM((2, lines, HALF), BF),
            pltpu.VMEM((2, lines, HALF), BF),
            pltpu.VMEM((lines, total), F32),
        ],
        compiler_params=params(),
        cost_estimate=pl.CostEstimate(
            flops=2 * lines * M * (total + 3 * HALF), transcendentals=0, bytes_accessed=1 << 24
        ),
        name="field_x" if sine else "field_y",
    )(device, codes, even[0], even[1], odd[0], odd[1], xt, xt, yt)


def exchange(blocks):
    return lax.all_to_all(blocks, AXES, split_axis=0, concat_axis=0, tiled=True)


def work(cell_row, cell_col, cell_width, cell_height, cell_region, cell_offset):
    slab_count = lax.axis_size("slab")
    cell_count = lax.axis_size("cell")
    count = slab_count * cell_count
    device = lax.axis_index("slab") * cell_count + lax.axis_index("cell")
    rows = M // count
    own = cell_row.shape[0]
    lines = REGIONS * rows
    gain = math.sqrt(2.0 / M)
    fwd_steps = steps_of(2.1 * own * cell_count * WMAX * gain)
    back_steps = steps_of(gain**3 * own * count * WMAX * HMAX * 1.1 * M / math.pi * 8.5)

    ints = [cell_row, cell_col, cell_width, cell_height, cell_region]
    mine = jnp.concatenate(
        [jnp.stack(ints).astype(F32), cell_offset, jnp.zeros((1, own), F32)], axis=0
    )
    pieces = [mine]
    back_moves = []
    for turn in range(1, cell_count):
        pairs = [
            (slab * cell_count + c, slab * cell_count + (c + turn) % cell_count)
            for slab in range(slab_count)
            for c in range(cell_count)
        ]
        pieces.append(lax.ppermute(mine, AXES, pairs))
        back_moves.append([(b, a) for a, b in pairs])
    for c in range(cell_count):
        pairs = [
            (slab * cell_count + c, (slab + 1) * cell_count) for slab in range(slab_count - 1)
        ]
        pieces.append(lax.ppermute(mine, AXES, pairs))
        back_moves.append([(b, a) for a, b in pairs])
    tables = make_tables()
    cells = jnp.concatenate(pieces, axis=1)

    device = device.astype(jnp.int32).reshape(1)
    xt, yt, codes, sums = density_call(device, cells, tables, rows, count, fwd_steps)
    if not packable(rows):
        codes = jnp.transpose(codes.reshape(REGIONS, rows, count, rows), (2, 1, 0, 3))
        codes = codes.reshape(count, rows, lines)
    arrived = exchange(codes)
    drive = spectrum_call(device, arrived, tables, fwd_steps, back_steps)
    along_x = exchange(drive[0])
    sine_part = sine_call(drive[1:5], tables, count, rows, back_steps)
    along_y = exchange(sine_part)

    sums = jnp.concatenate([sums, drive[5]], axis=0)
    reach = 1
    while reach < count:
        sums = sums + lax.ppermute(sums, AXES, [(i, i ^ reach) for i in range(count)])
        reach *= 2
    sums = jnp.sum(sums.reshape(3, 8 * 128), axis=1)

    def lines_of(blocks):
        if packable(rows):
            return blocks
        shaped = blocks.reshape(count, rows, REGIONS, rows)
        return jnp.transpose(shaped, (2, 1, 0, 3)).reshape(lines, M)

    fwd, sy, ce, se = tables[0:2], tables[2:4], tables[4:6], tables[6:8]
    field_x, force_x = field_call(
        device, lines_of(along_x), se, sy, xt, yt, back_steps, rows, count, True
    )
    field_y, force_y = field_call(
        device, lines_of(along_y), ce, fwd, xt, yt, back_steps, rows, count, False
    )
    partial = jnp.concatenate([force_x, force_y], axis=0)
    cell_force = partial[:, :own]
    for index, pairs in enumerate(back_moves):
        piece = partial[:, (index + 1) * own : (index + 2) * own]
        cell_force = cell_force + lax.ppermute(piece, AXES, pairs)
    energy = sums[2] / (M * M)
    overflow = sums[0] / sums[1]
    shape = (REGIONS, rows, M)
    return (field_x.reshape(shape), field_y.reshape(shape), cell_force, energy, overflow)


def solution(mesh):
    return jax.shard_map(
        work,
        mesh=mesh,
        in_specs=(
            P(("slab", "cell")),
            P(("slab", "cell")),
            P(("slab", "cell")),
            P(("slab", "cell")),
            P(("slab", "cell")),
            P(None, ("slab", "cell")),
        ),
        out_specs=(
            P(None, ("slab", "cell"), None),
            P(None, ("slab", "cell"), None),
            P(None, ("slab", "cell")),
            P(),
            P(),
        ),
        check_vma=False,
    )
```

```python
import functools
import math

import jax
import jax.numpy as jnp
import numpy as np
from jax import lax
from jax.experimental import pallas as pl
from jax.experimental.pallas import tpu as pltpu
from jax.sharding import PartitionSpec as P

M = 2048
REGIONS = 4
HMAX = 4
WMAX = 8
HALF = M // 2
STRIP = 32
BAND = 4
TILE = 256
PARTS = HALF // TILE
FINE = 8192.0
AXES = ("slab", "cell")
BF = jnp.bfloat16
F32 = jnp.float32
I16 = jnp.int16
VMEM_LIMIT = 56 * 1024 * 1024


def params():
    return pltpu.CompilerParams(
        dimension_semantics=("arbitrary",), vmem_limit_bytes=VMEM_LIMIT
    )


def steps_of(bound):
    return 32700.0 / math.log2(1.0 + bound * FINE)


def encode_wide(value, steps):
    code = jnp.minimum(jnp.log2(1.0 + jnp.abs(value) * FINE) * steps, 32767.0)
    return jnp.round(jnp.where(value < 0.0, -code, code))


def encode(value, steps):
    return encode_wide(value, steps).astype(jnp.int32).astype(I16)


def packable(rows):
    return rows == 64 and REGIONS == 4


def swap_halves(values):
    lane = lax.broadcasted_iota(jnp.int32, values[0].shape, 1)
    turned = [pltpu.roll(value, 64, 1) for value in values]
    first = jnp.where(lane < 64, values[0], turned[1])
    second = jnp.where(lane < 64, turned[0], values[1])
    return first, second


def pack(out, value):
    for pair in range(TILE // 128):
        tile = value[:, pair * 128 : (pair + 1) * 128]
        for half in range(2):
            here = pl.ds(half * 128, 128)
            low = tile[half * 128 : half * 128 + 64]
            high = tile[half * 128 + 64 : half * 128 + 128]
            first, second = swap_halves((low, high))
            out[2 * pair, :, here] = first.astype(jnp.int32).astype(I16)
            out[2 * pair + 1, :, here] = second.astype(jnp.int32).astype(I16)


def decode(code, steps):
    wide = code.astype(jnp.int32).astype(F32)
    size = (jnp.exp2(jnp.abs(wide) * (1.0 / steps)) - 1.0) * (1.0 / FINE)
    return jnp.where(wide < 0.0, -size, size)


def split(value):
    high = value.astype(BF)
    return high, (value - high.astype(F32)).astype(BF)


def dot(left, right):
    return lax.dot_general(left, right, (((1,), (0,)), ((), ())), preferred_element_type=F32)


def dot3(left_hi, left_lo, right_hi, right_lo):
    return dot(left_hi, right_hi) + (dot(left_lo, right_hi) + dot(left_hi, right_lo))


def base_tables():
    groups = HALF // STRIP
    unit = math.pi / (2 * M)
    turn = 4 * M
    place = (2 * np.arange(HALF) + 1)[None, :]
    freq = (2 * np.arange(HALF))[None, :]
    group = np.arange(groups)[:, None]
    inside = np.arange(STRIP)[:, None]
    gain = math.sqrt(2.0 / M)
    zero_gain = np.where(freq == 0, math.sqrt(0.5), 1.0)
    far = unit * (2 * STRIP * group * place % turn)
    far_t = unit * (2 * STRIP * group * freq % turn)
    near_even = unit * (2 * inside * place % turn)
    near_odd = unit * ((2 * inside + 1) * place % turn)
    near_t = unit * ((2 * inside + 1) * freq % turn)
    outer = np.stack([np.cos(far), np.sin(far), np.cos(far_t), np.sin(far_t)], axis=1)
    inner = np.stack(
        [
            gain * np.cos(near_even),
            gain * np.sin(near_even),
            gain * np.cos(near_odd),
            gain * np.sin(near_odd),
            gain * zero_gain * np.cos(near_t),
            gain * zero_gain * np.sin(near_t),
        ]
    )
    return outer.astype(np.float32), inner.astype(np.float32)


def table_kernel(outer, inner, fwd_hi, fwd_lo, sy_hi, sy_lo, ce_hi, ce_lo, se_hi, se_lo):
    for group in range(BAND):
        here = pl.ds(group * STRIP, STRIP)

        def pair(far, near):
            cos_far = outer[group, far : far + 1, :]
            sin_far = outer[group, far + 1 : far + 2, :]
            cos_near = inner[near]
            sin_near = inner[near + 1]
            return cos_far * cos_near - sin_far * sin_near, sin_far * cos_near + cos_far * sin_near

        cos_even, sin_even = pair(0, 0)
        if group == 0:
            row = lax.broadcasted_iota(jnp.int32, (STRIP, 1), 0) + pl.program_id(0) * STRIP
            cos_even = cos_even * jnp.where(row == 0, math.sqrt(0.5), 1.0).astype(F32)
        ce_hi[here, :], ce_lo[here, :] = split(cos_even)
        se_hi[here, :], se_lo[here, :] = split(sin_even)
        cos_odd, sin_odd = pair(0, 2)
        fwd_hi[here, HALF:], fwd_lo[here, HALF:] = split(cos_odd)
        sy_hi[here, HALF:], sy_lo[here, HALF:] = split(sin_odd)
        cos_t, sin_t = pair(2, 4)
        fwd_hi[here, :HALF], fwd_lo[here, :HALF] = split(cos_t)
        sy_hi[here, :HALF], sy_lo[here, :HALF] = split(sin_t)


def make_tables():
    outer, inner = base_tables()
    wide = jax.ShapeDtypeStruct((HALF, M), BF)
    square = jax.ShapeDtypeStruct((HALF, HALF), BF)
    wide_spec = pl.BlockSpec((BAND * STRIP, M), lambda g: (g, 0))
    square_spec = pl.BlockSpec((BAND * STRIP, HALF), lambda g: (g, 0))
    return pl.pallas_call(
        table_kernel,
        grid=(HALF // (BAND * STRIP),),
        in_specs=[
            pl.BlockSpec((BAND, 4, HALF), lambda g: (g, 0, 0)),
            pl.BlockSpec((6, STRIP, HALF), lambda g: (0, 0, 0)),
        ],
        out_specs=[wide_spec] * 4 + [square_spec] * 4,
        out_shape=[wide] * 4 + [square] * 4,
        compiler_params=params(),
        cost_estimate=pl.CostEstimate(
            flops=40 * HALF * HALF, transcendentals=0, bytes_accessed=24 * HALF * HALF
        ),
        name="tables",
    )(jnp.asarray(outer), jnp.asarray(inner))


def fold_rows(value):
    rows, cols = value.shape
    folded = jnp.sum(value.reshape(rows // 8, 8, cols), axis=0)
    out = folded[:, :128]
    for start in range(128, cols, 128):
        out = out + folded[:, start : start + 128]
    return out


def density_kernel(
    device,
    cells,
    fwd_hi,
    fwd_lo,
    xt,
    yt,
    codes,
    sums,
    dens,
    part_hi,
    part_lo,
    *,
    steps,
    rows,
    count,
):
    step = pl.program_id(0)
    total = cells.shape[1]
    chunk = 512

    @pl.when(step == 0)
    def _():
        line = lax.broadcasted_iota(jnp.int32, (yt.shape[0], 1), 0)
        inside = line & (rows - 1)
        place = jnp.where(device[0] >= count // 2, rows - 1 - inside, inside) + device[0] * rows
        place = place.astype(F32)
        region = (line >> (rows.bit_length() - 1)).astype(F32)
        for start in range(0, total, chunk):
            here = pl.ds(start, chunk)
            low = cells[6:7, here]
            rel = place - cells[0:1, here]
            high = jnp.minimum(rel + 1.0, low + cells[3:4, here])
            value = jnp.maximum(high - jnp.maximum(rel, low), 0.0)
            yt[:, here] = jnp.where(region == cells[4:5, here], value, 0.0).astype(BF)

    @pl.when(step < 2 * PARTS)
    def _():
        place = (step % PARTS) * TILE + lax.broadcasted_iota(jnp.int32, (TILE, 1), 0)
        place = jnp.where(step >= PARTS, M - 1 - place, place).astype(F32)
        acc = None
        for start in range(0, total, chunk):
            here = pl.ds(start, chunk)
            low = cells[5:6, here]
            rel = place - cells[1:2, here]
            high = jnp.minimum(rel + 1.0, low + cells[2:3, here])
            value = jnp.maximum(high - jnp.maximum(rel, low), 0.0).astype(BF)
            xt[:, here] = value
            part = lax.dot_general(
                yt[:, here], value, (((1,), (1,)), ((), ())), preferred_element_type=F32
            )
            acc = part if acc is None else acc + part
        dens[step] = acc

    @pl.when(step == 2 * PARTS)
    def _():
        over = jnp.zeros((8, 128), F32)
        full = jnp.zeros((8, 128), F32)
        for part in range(PARTS):
            here = pl.ds(part * TILE, TILE)
            near = dens[part]
            mirrored = dens[PARTS + part]
            even = near + mirrored
            over = over + fold_rows(
                jnp.maximum(near - 1.0, 0.0) + jnp.maximum(mirrored - 1.0, 0.0)
            )
            full = full + fold_rows(even)
            part_hi[0, :, here], part_lo[0, :, here] = split(even)
            part_hi[1, :, here], part_lo[1, :, here] = split(near - mirrored)
        sums[0:8, :] = over
        sums[8:16, :] = full

    @pl.when(step >= 2 * PARTS)
    def _():
        odd = jnp.where(step >= 3 * PARTS, 1, 0)
        out = dot3(part_hi[odd], part_lo[odd], fwd_hi[...], fwd_lo[...])
        if packable(rows):
            pack(codes, encode_wide(out, steps))
        else:
            codes[...] = encode(out, steps)


def density_call(device, cells, tables, rows, count, steps):
    total = cells.shape[1]
    lines = REGIONS * rows
    late = lambda t: (0, jnp.maximum(t - 2 * PARTS, 0))
    whole = lambda t: (0, 0)
    if packable(rows):
        code_spec = pl.BlockSpec(
            (TILE // rows, rows, lines), lambda t: (jnp.maximum(t - 2 * PARTS, 0), 0, 0)
        )
        code_shape = (count, rows, lines)
    else:
        code_spec = pl.BlockSpec((lines, TILE), late)
        code_shape = (lines, M)
    return pl.pallas_call(
        functools.partial(density_kernel, steps=steps, rows=rows, count=count),
        grid=(4 * PARTS,),
        in_specs=[
            pl.BlockSpec(memory_space=pltpu.SMEM),
            pl.BlockSpec((8, total), whole),
            pl.BlockSpec((HALF, TILE), late),
            pl.BlockSpec((HALF, TILE), late),
        ],
        out_specs=[
            pl.BlockSpec((TILE, total), lambda t: (jnp.minimum(t, 2 * PARTS - 1), 0)),
            pl.BlockSpec((lines, total), whole),
            code_spec,
            pl.BlockSpec((16, 128), whole),
        ],
        out_shape=[
            jax.ShapeDtypeStruct((M, total), BF),
            jax.ShapeDtypeStruct((lines, total), BF),
            jax.ShapeDtypeStruct(code_shape, I16),
            jax.ShapeDtypeStruct((16, 128), F32),
        ],
        scratch_shapes=[
            pltpu.VMEM((2 * PARTS, lines, TILE), F32),
            pltpu.VMEM((2, lines, HALF), BF),
            pltpu.VMEM((2, lines, HALF), BF),
        ],
        compiler_params=params(),
        cost_estimate=pl.CostEstimate(
            flops=2 * lines * M * (total + 3 * HALF), transcendentals=0, bytes_accessed=1 << 24
        ),
        name="density",
    )(device, cells, tables[0], tables[1])


def place_rows(out, first, top, bottom, steps):
    count, rows = out.shape[0], out.shape[1]
    top = encode(top, steps)
    bottom = encode(bottom, steps)
    for inner in range(TILE // rows):
        here = slice(inner * rows, (inner + 1) * rows)
        out[first + inner] = top[here]
        out[count - 1 - first - inner] = bottom[here]


def spectrum_kernel(
    device,
    codes,
    ce_hi,
    ce_lo,
    co_hi,
    co_lo,
    ct_hi,
    ct_lo,
    out,
    dye_hi,
    dye_lo,
    dyo_hi,
    dyo_lo,
    energy,
    even_hi,
    even_lo,
    odd_hi,
    odd_lo,
    dxe_hi,
    dxe_lo,
    dxo_hi,
    dxo_lo,
    *,
    fwd_steps,
    back_steps,
):
    step = pl.program_id(0)
    count, rows = codes.shape[0], codes.shape[1]

    @pl.when(step == 0)
    def _():
        for block in range(count // 2):
            here = pl.ds(block * rows, rows)
            near = decode(codes[block], fwd_steps)
            mirrored = decode(codes[count - 1 - block], fwd_steps)
            even_hi[here, :], even_lo[here, :] = split(near + mirrored)
            odd_hi[here, :], odd_lo[here, :] = split(near - mirrored)
        energy[...] = jnp.zeros((8, 128), F32)

    @pl.when(step < PARTS)
    def _():
        unit = math.pi / M
        lane = lax.broadcasted_iota(jnp.int32, (1, codes.shape[2]), 1) & (rows - 1)
        odd = jnp.where(device[0] >= count // 2, 1, 0)
        q = (2 * (rows * (device[0] - odd * (count // 2)) + lane) + odd).astype(F32)
        first = lax.broadcasted_iota(jnp.int32, (TILE, 1), 0) + step * TILE
        here = pl.ds(pl.multiple_of(step * TILE, TILE), TILE)

        def solve(spectrum, p):
            squared = p * p + q * q
            inverse = jnp.where(squared == 0.0, 0.0, 1.0 / jnp.where(squared == 0.0, 1.0, squared))
            scaled = spectrum * inverse
            return scaled * (q * (1.0 / unit)), scaled * (p * (1.0 / unit)), spectrum * scaled

        spec = dot3(ce_hi[...], ce_lo[...], even_hi[...], even_lo[...])
        drive_x, drive_y, power = solve(spec, (2 * first).astype(F32))
        dxe_hi[here, :], dxe_lo[here, :] = split(drive_x)
        dye_hi[...], dye_lo[...] = split(drive_y)
        spec = dot3(co_hi[...], co_lo[...], odd_hi[...], odd_lo[...])
        drive_x, drive_y, more = solve(spec, (2 * first + 1).astype(F32))
        dxo_hi[here, :], dxo_lo[here, :] = split(drive_x)
        dyo_hi[...], dyo_lo[...] = split(drive_y)
        both = power + more
        if both.shape[1] % 128:
            both = jnp.concatenate(
                [both, jnp.zeros((TILE, 128 - both.shape[1] % 128), F32)], axis=1
            )
        energy[...] += fold_rows(both) * (1.0 / (unit * unit))

    @pl.when(step >= PARTS)
    def _():
        even = dot3(ct_hi[...], ct_lo[...], dxe_hi[...], dxe_lo[...])
        odd = dot3(co_hi[...], co_lo[...], dxo_hi[...], dxo_lo[...])
        first = (step - PARTS) * (TILE // rows)
        place_rows(out, first, even + odd, even - odd, back_steps)


def spectrum_call(device, codes, tables, fwd_steps, back_steps):
    fwd_hi, fwd_lo, _, _, ce_hi, ce_lo, _, _ = tables
    count, rows, cols = codes.shape
    early = lambda t: (jnp.minimum(t, PARTS - 1), 0)
    drive = jax.ShapeDtypeStruct((HALF, cols), BF)
    return pl.pallas_call(
        functools.partial(spectrum_kernel, fwd_steps=fwd_steps, back_steps=back_steps),
        grid=(2 * PARTS,),
        in_specs=[
            pl.BlockSpec(memory_space=pltpu.SMEM),
            pl.BlockSpec((count, rows, cols), lambda t: (0, 0, 0)),
        ]
        + [pl.BlockSpec((TILE, HALF), early)] * 2
        + [pl.BlockSpec((TILE, HALF), lambda t: (t % PARTS, 1))] * 2
        + [pl.BlockSpec((TILE, HALF), lambda t: (jnp.maximum(t - PARTS, 0), 0))] * 2,
        out_specs=[pl.BlockSpec((count, rows, cols), lambda t: (0, 0, 0))]
        + [pl.BlockSpec((TILE, cols), early)] * 4
        + [pl.BlockSpec((8, 128), lambda t: (0, 0))],
        out_shape=[jax.ShapeDtypeStruct((count, rows, cols), I16)]
        + [drive] * 4
        + [jax.ShapeDtypeStruct((8, 128), F32)],
        scratch_shapes=[pltpu.VMEM((HALF, cols), BF)] * 8,
        compiler_params=params(),
        cost_estimate=pl.CostEstimate(
            flops=24 * HALF * HALF * cols, transcendentals=0, bytes_accessed=1 << 24
        ),
        name="spectrum",
    )(device, codes, ce_hi, ce_lo, fwd_hi, fwd_lo, fwd_hi, fwd_lo)


def sine_kernel(
    dye_hi, dye_lo, dyo_hi, dyo_lo, se_hi, se_lo, so_hi, so_lo, out, *, back_steps
):
    even = dot3(se_hi[...], se_lo[...], dye_hi[...], dye_lo[...])
    odd = dot3(so_hi[...], so_lo[...], dyo_hi[...], dyo_lo[...])
    first = pl.program_id(0) * (TILE // out.shape[1])
    place_rows(out, first, odd + even, odd - even, back_steps)


def sine_call(drives, tables, count, rows, back_steps):
    sy_hi, sy_lo = tables[2], tables[3]
    cols = drives[0].shape[1]
    return pl.pallas_call(
        functools.partial(sine_kernel, back_steps=back_steps),
        grid=(PARTS,),
        in_specs=[pl.BlockSpec((HALF, cols), lambda t: (0, 0))] * 4
        + [pl.BlockSpec((TILE, HALF), lambda t: (t, 0))] * 2
        + [pl.BlockSpec((TILE, HALF), lambda t: (t, 1))] * 2,
        out_specs=pl.BlockSpec((count, rows, cols), lambda t: (0, 0, 0)),
        out_shape=jax.ShapeDtypeStruct((count, rows, cols), I16),
        compiler_params=params(),
        cost_estimate=pl.CostEstimate(
            flops=12 * HALF * HALF * cols, transcendentals=0, bytes_accessed=1 << 23
        ),
        name="sine_rows",
    )(*drives, sy_hi, sy_lo, sy_hi, sy_lo)


def field_kernel(
    device,
    codes,
    even_hi,
    even_lo,
    odd_hi,
    odd_lo,
    x_near,
    x_far,
    yt,
    field,
    force,
    part_hi,
    part_lo,
    acc,
    *,
    steps,
    rows,
    count,
    sine,
):
    step = pl.program_id(0)
    flipped = device[0] >= count // 2

    @pl.when(step == 0)
    def _():
        if codes.ndim == 3 and codes.shape[2] % 512 == 0:
            width = codes.shape[2] // REGIONS
            sources = codes.shape[0]
            for source in range(sources):
                value = decode(codes[source], steps)
                part = 2 * source // sources
                here = pl.ds((source % (sources // 2)) * width, width)
                for g in range(REGIONS):
                    lines = pl.ds(g * rows, rows)
                    high, low = split(value[:, g * width : (g + 1) * width])
                    part_hi[part, lines, here] = high
                    part_lo[part, lines, here] = low
        elif packable(rows):
            for pair in range(count // 2):
                near = decode(codes[2 * pair], steps)
                far = decode(codes[2 * pair + 1], steps)
                part = 2 * pair // (count // 2)
                here = pl.ds((pair % (count // 4)) * 128, 128)
                for half in range(2):
                    lanes = slice(half * 128, (half + 1) * 128)
                    for inner, value in enumerate(swap_halves((near[:, lanes], far[:, lanes]))):
                        lines = pl.ds((2 * half + inner) * rows, rows)
                        part_hi[part, lines, here], part_lo[part, lines, here] = split(value)
        else:
            for part in range(2):
                for block in range(PARTS):
                    here = pl.ds(block * TILE, TILE)
                    value = decode(codes[:, part * HALF + block * TILE :][:, :TILE], steps)
                    part_hi[part, :, here], part_lo[part, :, here] = split(value)

    even = dot3(part_hi[0], part_lo[0], even_hi[...], even_lo[...])
    odd = dot3(part_hi[1], part_lo[1], odd_hi[...], odd_lo[...])
    near = even + odd
    far = odd - even if sine else even - odd
    gathered = dot(near.astype(BF), x_near[...]) + dot(far.astype(BF), x_far[...])

    @pl.when(step == 0)
    def _():
        acc[...] = gathered

    @pl.when(step > 0)
    def _():
        acc[...] += gathered

    lane = 127 - lax.broadcasted_iota(jnp.int32, (8, 128), 1)
    sub = lax.broadcasted_iota(jnp.int32, (8, 128), 0)
    sub = jnp.where(flipped, 7 - sub, sub)
    for region in range(near.shape[0] // rows):
        for block in range(rows // 8):
            start = region * rows + 8 * block
            target = region * rows + jnp.where(flipped, rows - 8 - 8 * block, 8 * block)
            target = pl.multiple_of(target, 8)
            for tile in range(TILE // 128):
                piece = near[start : start + 8, tile * 128 : (tile + 1) * 128]
                piece = jnp.take_along_axis(piece, sub, axis=0)
                col = pl.multiple_of(step * TILE + tile * 128, 128)
                field[pl.ds(target, 8), pl.ds(col, 128)] = piece
                piece = far[start : start + 8, tile * 128 : (tile + 1) * 128]
                piece = jnp.take_along_axis(piece, sub, axis=0)
                piece = jnp.take_along_axis(piece, lane, axis=1)
                col = pl.multiple_of(M - 128 - step * TILE - tile * 128, 128)
                field[pl.ds(target, 8), pl.ds(col, 128)] = piece

    @pl.when(step == PARTS - 1)
    def _():
        force[...] = jnp.sum(yt[...].astype(F32) * acc[...], axis=0, keepdims=True)


def field_call(device, codes, even, odd, xt, yt, steps, rows, count, sine):
    lines, total = yt.shape
    zeros = (0,) * codes.ndim
    return pl.pallas_call(
        functools.partial(field_kernel, steps=steps, rows=rows, count=count, sine=sine),
        grid=(PARTS,),
        in_specs=[
            pl.BlockSpec(memory_space=pltpu.SMEM),
            pl.BlockSpec(codes.shape, lambda t: zeros),
        ]
        + [pl.BlockSpec((HALF, TILE), lambda t: (0, t))] * 2
        + [pl.BlockSpec((HALF, TILE), lambda t: (0, PARTS + t))] * 2
        + [
            pl.BlockSpec((TILE, total), lambda t: (t, 0)),
            pl.BlockSpec((TILE, total), lambda t: (PARTS + t, 0)),
            pl.BlockSpec((lines, total), lambda t: (0, 0)),
        ],
        out_specs=[
            pl.BlockSpec((lines, M), lambda t: (0, 0)),
            pl.BlockSpec((1, total), lambda t: (0, 0)),
        ],
        out_shape=[
            jax.ShapeDtypeStruct((lines, M), F32),
            jax.ShapeDtypeStruct((1, total), F32),
        ],
        scratch_shapes=[
            pltpu.VMEM((2, lines, HALF), BF),
            pltpu.VMEM((2, lines, HALF), BF),
            pltpu.VMEM((lines, total), F32),
        ],
        compiler_params=params(),
        cost_estimate=pl.CostEstimate(
            flops=2 * lines * M * (total + 3 * HALF), transcendentals=0, bytes_accessed=1 << 24
        ),
        name="field_x" if sine else "field_y",
    )(device, codes, even[0], even[1], odd[0], odd[1], xt, xt, yt)


def profile(rel, low, extent):
    high = jnp.minimum(rel + 1.0, low + extent)
    return jnp.maximum(high - jnp.maximum(rel, low), 0.0)


def local_kernel(device, cells, xt, yt, sums, dens, *, rows, count):
    step = pl.program_id(0)
    total = cells.shape[1]
    chunk = 512

    @pl.when(step == 0)
    def _():
        line = lax.broadcasted_iota(jnp.int32, (yt.shape[0], 1), 0)
        inside = line & (rows - 1)
        place = jnp.where(device[0] >= count // 2, rows - 1 - inside, inside) + device[0] * rows
        place = place.astype(F32)
        region = (line >> (rows.bit_length() - 1)).astype(F32)
        for start in range(0, total, chunk):
            here = pl.ds(start, chunk)
            value = profile(place - cells[0:1, here], cells[6:7, here], cells[3:4, here])
            yt[:, here] = jnp.where(region == cells[4:5, here], value, 0.0).astype(BF)
        sums[...] = jnp.zeros((16, 128), F32)

    place = (step % PARTS) * TILE + lax.broadcasted_iota(jnp.int32, (TILE, 1), 0)
    place = jnp.where(step >= PARTS, M - 1 - place, place).astype(F32)
    acc = None
    for start in range(0, total, chunk):
        here = pl.ds(start, chunk)
        value = profile(place - cells[1:2, here], cells[5:6, here], cells[2:3, here]).astype(BF)
        xt[:, here] = value
        part = lax.dot_general(
            yt[:, here], value, (((1,), (1,)), ((), ())), preferred_element_type=F32
        )
        acc = part if acc is None else acc + part
    sums[0:8, :] += fold_rows(jnp.maximum(acc - 1.0, 0.0))
    sums[8:16, :] += fold_rows(acc)


def local_call(device, cells, rows, count):
    total = cells.shape[1]
    lines = REGIONS * rows
    whole = lambda t: (0, 0)
    return pl.pallas_call(
        functools.partial(local_kernel, rows=rows, count=count),
        grid=(2 * PARTS,),
        in_specs=[
            pl.BlockSpec(memory_space=pltpu.SMEM),
            pl.BlockSpec((8, total), whole),
        ],
        out_specs=[
            pl.BlockSpec((TILE, total), lambda t: (t, 0)),
            pl.BlockSpec((lines, total), whole),
            pl.BlockSpec((16, 128), whole),
        ],
        out_shape=[
            jax.ShapeDtypeStruct((M, total), BF),
            jax.ShapeDtypeStruct((lines, total), BF),
            jax.ShapeDtypeStruct((16, 128), F32),
        ],
        scratch_shapes=[pltpu.VMEM((8, 128), F32)],
        compiler_params=params(),
        cost_estimate=pl.CostEstimate(
            flops=2 * lines * M * total, transcendentals=0, bytes_accessed=1 << 23
        ),
        name="local",
    )(device, cells)


SPAN = 256
EXTRA = 16


def spectral_kernel(
    device,
    cells,
    far_table,
    near_table,
    ce_hi,
    ce_lo,
    co_hi,
    co_lo,
    ct_hi,
    ct_lo,
    out,
    dye_hi,
    dye_lo,
    dyo_hi,
    dyo_lo,
    energy,
    dens,
    far_hi,
    far_lo,
    near_both,
    even_hi,
    even_lo,
    odd_hi,
    odd_lo,
    dxe_hi,
    dxe_lo,
    dxo_hi,
    dxo_lo,
    *,
    slab_count,
    count,
    back_steps,
):
    step = pl.program_id(0)
    slab_rows = M // slab_count
    group = count // 2
    rows = M // count
    width = M // group
    window = slab_rows + EXTRA
    upper = device[0] >= group
    member = jnp.where(upper, device[0] - group, device[0])
    sign = jnp.where(upper, -1.0, 1.0).astype(F32)

    @pl.when(step == 0)
    def _():
        dens[...] = jnp.zeros(dens.shape, F32)
        far_hi[...], far_lo[...] = split(far_table[...])
        near_both[:, : SPAN // 2], near_both[:, SPAN // 2 :] = split(near_table[...])
        energy[...] = jnp.zeros((8, 128), F32)

    @pl.when(step < slab_count)
    def _():
        top = step >= slab_count // 2
        line = lax.broadcasted_iota(jnp.int32, (window, 1), 0)
        line = jnp.where(top, window - 1 - line, line) + step * slab_rows
        line = line.astype(F32)
        turn = M.bit_length() - 1
        acc = None
        for piece in range(cells.shape[0]):
            first = cells[piece, 0:1, :].astype(jnp.int32)
            second = cells[piece, 1:2, :].astype(jnp.int32)
            low_x = cells[piece, 2:3, :]
            low_y = cells[piece, 3:4, :]
            row = (first & (M - 1)).astype(F32)
            region = (first >> turn) & (REGIONS - 1)
            height = ((first >> (turn + 2)) + 1).astype(F32)
            col = second & (M - 1)
            wide = second >> turn
            width_x = (wide + 1).astype(F32)
            value_y = profile(line - row, low_y, height)
            stacked = jnp.concatenate(
                [jnp.where(region == g, value_y, 0.0).astype(BF) for g in range(REGIONS)], axis=0
            )
            head = profile(jnp.zeros_like(low_x), low_x, width_x)
            tail = profile(width_x, low_x, width_x)
            base = (col & 7) * 16
            slot = lax.broadcasted_iota(jnp.int32, (SPAN // 2, 1), 0)
            feature = jnp.where(slot == base + wide, 1.0, jnp.where(slot == base + 8 + wide, tail, 0.0))
            feature = jnp.where(slot == base, head, feature).astype(BF)
            spot = lax.broadcasted_iota(jnp.int32, (SPAN, 1), 0)
            chosen = jnp.where(spot == (col >> 3), 1.0, 0.0).astype(BF)
            near = dot(near_both[...], jnp.concatenate([feature, feature], axis=0))
            far = dot(far_hi[...], chosen) + dot(far_lo[...], chosen)
            value = near[:width] * far[:width] - near[width:] * far[width:]
            value = jnp.concatenate(split(value), axis=0)
            part = lax.dot_general(
                stacked, value, (((1,), (1,)), ((), ())), preferred_element_type=F32
            )
            acc = part if acc is None else acc + part
        half = jnp.where(top, 1, 0)
        start = jnp.where(top, slab_count - 1 - step, step) * slab_rows
        here = pl.ds(pl.multiple_of(start, 8), window)
        for g in range(REGIONS):
            lines = slice(g * window, (g + 1) * window)
            lanes = pl.ds(g * width, width)
            dens[half, here, lanes] += acc[lines, :width] + acc[lines, width:]

    @pl.when(step == slab_count)
    def _():
        sub = 7 - lax.broadcasted_iota(jnp.int32, (8, 128), 0)
        for tile in range(dens.shape[2] // 128):
            lanes = pl.ds(tile * 128, 128)
            spill = jnp.take_along_axis(dens[0, HALF : HALF + 8, lanes], sub, axis=0)
            dens[1, HALF + EXTRA - 8 : HALF + EXTRA, lanes] += spill
        for block in range(HALF // 128):
            here = pl.ds(block * 128, 128)
            near = dens[0, here, :]
            mirrored = dens[1, pl.ds(block * 128 + EXTRA, 128), :]
            even_hi[here, :], even_lo[here, :] = split(near + mirrored)
            odd_hi[here, :], odd_lo[here, :] = split(near - mirrored)

    @pl.when((step >= slab_count) & (step < slab_count + PARTS))
    def _():
        turn = step - slab_count
        unit = math.pi / M
        lane = lax.broadcasted_iota(jnp.int32, (1, REGIONS * width), 1) & (width - 1)
        odd = jnp.where(member >= group // 2, 1, 0)
        q = (2 * (width * (member - odd * (group // 2)) + lane) + odd).astype(F32)
        first = lax.broadcasted_iota(jnp.int32, (TILE, 1), 0) + turn * TILE
        here = pl.ds(pl.multiple_of(turn * TILE, TILE), TILE)

        def solve(spectrum, p):
            squared = p * p + q * q
            inverse = jnp.where(squared == 0.0, 0.0, 1.0 / jnp.where(squared == 0.0, 1.0, squared))
            scaled = spectrum * inverse
            return scaled * (q * (1.0 / unit)), scaled * (p * (1.0 / unit)), spectrum * scaled

        spec = dot3(ce_hi[...], ce_lo[...], even_hi[...], even_lo[...])
        drive_x, drive_y, power = solve(spec, (2 * first).astype(F32))
        dxe_hi[here, :], dxe_lo[here, :] = split(drive_x)
        dye_hi[...], dye_lo[...] = split(drive_y * sign)
        spec = dot3(co_hi[...], co_lo[...], odd_hi[...], odd_lo[...])
        drive_x, drive_y, more = solve(spec, (2 * first + 1).astype(F32))
        dxo_hi[here, :], dxo_lo[here, :] = split(drive_x * sign)
        dyo_hi[...], dyo_lo[...] = split(drive_y)
        energy[...] += fold_rows(power + more) * (1.0 / (unit * unit))

    @pl.when(step >= slab_count + PARTS)
    def _():
        value = dot3(ct_hi[...], ct_lo[...], dxe_hi[...], dxe_lo[...])
        value = value + dot3(co_hi[...], co_lo[...], dxo_hi[...], dxo_lo[...])
        send_rows(out, (step - slab_count - PARTS) * (TILE // rows), value, upper, back_steps)


def send_rows(out, first, value, upper, steps):
    count, rows = out.shape[0], out.shape[1]
    code = encode(value, steps)
    for inner in range(TILE // rows):
        target = first + inner
        target = jnp.where(upper, count - 1 - target, target)
        out[target] = code[inner * rows : (inner + 1) * rows]


def spectral_call(device, cells, far_table, near_table, tables, slab_count, back_steps):
    fwd_hi, fwd_lo, _, _, ce_hi, ce_lo, _, _ = tables
    count = cells.shape[0]
    group = count // 2
    rows = M // count
    width = M // group
    cols = REGIONS * width
    share = count // slab_count
    phase = lambda t: jnp.clip(t - slab_count, 0, PARTS - 1)
    last = lambda t: jnp.clip(t - slab_count - PARTS, 0, PARTS - 1)
    both = lambda t: jnp.where(t < slab_count, 0, (t - slab_count) % PARTS)
    drive = jax.ShapeDtypeStruct((HALF, cols), BF)
    return pl.pallas_call(
        functools.partial(
            spectral_kernel, slab_count=slab_count, count=count, back_steps=back_steps
        ),
        grid=(slab_count + 2 * PARTS,),
        in_specs=[
            pl.BlockSpec(memory_space=pltpu.SMEM),
            pl.BlockSpec(
                (share,) + cells.shape[1:], lambda t: (jnp.minimum(t, slab_count - 1), 0, 0)
            ),
            pl.BlockSpec(far_table.shape, lambda t: (0, 0)),
            pl.BlockSpec(near_table.shape, lambda t: (0, 0)),
        ]
        + [pl.BlockSpec((TILE, HALF), lambda t: (phase(t), 0))] * 2
        + [pl.BlockSpec((TILE, HALF), lambda t: (both(t), 1))] * 2
        + [pl.BlockSpec((TILE, HALF), lambda t: (last(t), 0))] * 2,
        out_specs=[pl.BlockSpec((group, rows, cols), lambda t: (0, 0, 0))]
        + [pl.BlockSpec((TILE, cols), lambda t: (phase(t), 0))] * 4
        + [pl.BlockSpec((8, 128), lambda t: (0, 0))],
        out_shape=[jax.ShapeDtypeStruct((group, rows, cols), I16)]
        + [drive] * 4
        + [jax.ShapeDtypeStruct((8, 128), F32)],
        scratch_shapes=[
            pltpu.VMEM((2, HALF + EXTRA, cols), F32),
            pltpu.VMEM((2 * width, SPAN), BF),
            pltpu.VMEM((2 * width, SPAN), BF),
            pltpu.VMEM((2 * width, SPAN), BF),
        ]
        + [pltpu.VMEM((HALF, cols), BF)] * 8,
        compiler_params=params(),
        cost_estimate=pl.CostEstimate(
            flops=30 * HALF * HALF * cols, transcendentals=0, bytes_accessed=1 << 24
        ),
        name="spectral",
    )(device, cells, far_table, near_table, ce_hi, ce_lo, fwd_hi, fwd_lo, fwd_hi, fwd_lo)


def sine_half_kernel(
    device, dye_hi, dye_lo, dyo_hi, dyo_lo, se_hi, se_lo, so_hi, so_lo, out, *, back_steps
):
    value = dot3(se_hi[...], se_lo[...], dye_hi[...], dye_lo[...])
    value = value + dot3(so_hi[...], so_lo[...], dyo_hi[...], dyo_lo[...])
    first = pl.program_id(0) * (TILE // out.shape[1])
    send_rows(out, first, value, device[0] >= out.shape[0], back_steps)


def sine_half_call(device, drives, tables, group, rows, back_steps):
    sy_hi, sy_lo = tables[2], tables[3]
    cols = drives[0].shape[1]
    return pl.pallas_call(
        functools.partial(sine_half_kernel, back_steps=back_steps),
        grid=(PARTS,),
        in_specs=[pl.BlockSpec(memory_space=pltpu.SMEM)]
        + [pl.BlockSpec((HALF, cols), lambda t: (0, 0))] * 4
        + [pl.BlockSpec((TILE, HALF), lambda t: (t, 0))] * 2
        + [pl.BlockSpec((TILE, HALF), lambda t: (t, 1))] * 2,
        out_specs=pl.BlockSpec((group, rows, cols), lambda t: (0, 0, 0)),
        out_shape=jax.ShapeDtypeStruct((group, rows, cols), I16),
        compiler_params=params(),
        cost_estimate=pl.CostEstimate(
            flops=12 * HALF * HALF * cols, transcendentals=0, bytes_accessed=1 << 23
        ),
        name="sine_half",
    )(device, *drives, sy_hi, sy_lo, sy_hi, sy_lo)


def cell_tables(q):
    odd = 2 * np.arange(16) + 1
    moment = np.concatenate([16 * np.arange(SPAN), odd])
    phase = (q[:, None] * jnp.asarray(moment, jnp.int32)[None, :]) % (4 * M)
    angle = phase.astype(F32) * (math.pi / (2.0 * M))
    both = jnp.concatenate([jnp.cos(angle), jnp.sin(angle)], axis=0)
    weight = jnp.where(q == 0, math.sqrt(1.0 / M), math.sqrt(2.0 / M)).astype(F32)
    far = both[:, :SPAN] * jnp.concatenate([weight, weight])[:, None]
    chosen = np.zeros((16, 8, 16), np.float32)
    for start in range(8):
        chosen[start, start, 0] = 1.0
        for wide in range(1, 9):
            if wide > 1:
                chosen[start + 1 : start + wide, start, wide - 1] = 1.0
            chosen[start + wide, start, 7 + wide] = 1.0
    near = jnp.dot(
        both[:, SPAN:],
        jnp.asarray(chosen.reshape(16, SPAN // 2)),
        precision=lax.Precision.HIGHEST,
        preferred_element_type=F32,
    )
    return far, near


def exchange(blocks, groups=None):
    return lax.all_to_all(
        blocks, AXES, split_axis=0, concat_axis=0, tiled=True, axis_index_groups=groups
    )


def full_work(cell_row, cell_col, cell_width, cell_height, cell_region, cell_offset):
    slab_count = lax.axis_size("slab")
    cell_count = lax.axis_size("cell")
    count = slab_count * cell_count
    device = lax.axis_index("slab") * cell_count + lax.axis_index("cell")
    rows = M // count
    own = cell_row.shape[0]
    lines = REGIONS * rows
    gain = math.sqrt(2.0 / M)
    fwd_steps = steps_of(2.1 * own * cell_count * WMAX * gain)
    back_steps = steps_of(gain**3 * own * count * WMAX * HMAX * 1.1 * M / math.pi * 8.5)

    ints = [cell_row, cell_col, cell_width, cell_height, cell_region]
    mine = jnp.concatenate(
        [jnp.stack(ints).astype(F32), cell_offset, jnp.zeros((1, own), F32)], axis=0
    )
    pieces = [mine]
    back_moves = []
    for turn in range(1, cell_count):
        pairs = [
            (slab * cell_count + c, slab * cell_count + (c + turn) % cell_count)
            for slab in range(slab_count)
            for c in range(cell_count)
        ]
        pieces.append(lax.ppermute(mine, AXES, pairs))
        back_moves.append([(b, a) for a, b in pairs])
    for c in range(cell_count):
        pairs = [
            (slab * cell_count + c, (slab + 1) * cell_count) for slab in range(slab_count - 1)
        ]
        pieces.append(lax.ppermute(mine, AXES, pairs))
        back_moves.append([(b, a) for a, b in pairs])
    tables = make_tables()
    cells = jnp.concatenate(pieces, axis=1)

    device = device.astype(jnp.int32).reshape(1)
    xt, yt, codes, sums = density_call(device, cells, tables, rows, count, fwd_steps)
    if not packable(rows):
        codes = jnp.transpose(codes.reshape(REGIONS, rows, count, rows), (2, 1, 0, 3))
        codes = codes.reshape(count, rows, lines)
    arrived = exchange(codes)
    drive = spectrum_call(device, arrived, tables, fwd_steps, back_steps)
    along_x = exchange(drive[0])
    sine_part = sine_call(drive[1:5], tables, count, rows, back_steps)
    along_y = exchange(sine_part)

    sums = jnp.concatenate([sums, drive[5]], axis=0)
    reach = 1
    while reach < count:
        sums = sums + lax.ppermute(sums, AXES, [(i, i ^ reach) for i in range(count)])
        reach *= 2
    sums = jnp.sum(sums.reshape(3, 8 * 128), axis=1)

    def lines_of(blocks):
        if packable(rows):
            return blocks
        shaped = blocks.reshape(count, rows, REGIONS, rows)
        return jnp.transpose(shaped, (2, 1, 0, 3)).reshape(lines, M)

    fwd, sy, ce, se = tables[0:2], tables[2:4], tables[4:6], tables[6:8]
    field_x, force_x = field_call(
        device, lines_of(along_x), se, sy, xt, yt, back_steps, rows, count, True
    )
    field_y, force_y = field_call(
        device, lines_of(along_y), ce, fwd, xt, yt, back_steps, rows, count, False
    )
    partial = jnp.concatenate([force_x, force_y], axis=0)
    cell_force = partial[:, :own]
    for index, pairs in enumerate(back_moves):
        piece = partial[:, (index + 1) * own : (index + 2) * own]
        cell_force = cell_force + lax.ppermute(piece, AXES, pairs)
    energy = sums[2] / (M * M)
    overflow = sums[0] / sums[1]
    shape = (REGIONS, rows, M)
    return (field_x.reshape(shape), field_y.reshape(shape), cell_force, energy, overflow)


def half_work(cell_row, cell_col, cell_width, cell_height, cell_region, cell_offset):
    slab_count = lax.axis_size("slab")
    cell_count = lax.axis_size("cell")
    count = slab_count * cell_count
    group = count // 2
    slab = lax.axis_index("slab")
    member = lax.axis_index("cell")
    device = slab * cell_count + member
    rows = M // count
    width = M // group
    own = cell_row.shape[0]
    gain = math.sqrt(2.0 / M)
    back_steps = steps_of(gain**3 * own * count * WMAX * HMAX * 1.1 * M / math.pi * 8.5)
    groups = [list(range(group)), list(range(group, count))]

    first = cell_row + M * (cell_region + REGIONS * (cell_height - 1))
    second = cell_col + M * (cell_width - 1)
    mine = jnp.concatenate([jnp.stack([first, second]).astype(F32), cell_offset], axis=0)
    everyone = exchange(jnp.broadcast_to(mine[None], (count,) + mine.shape))
    tables = make_tables()
    within = device % group
    odd = within // (group // 2)
    q = 2 * (width * (within - odd * (group // 2)) + lax.iota(jnp.int32, width)) + odd
    far_table, near_table = cell_tables(q)
    scalar = device.astype(jnp.int32).reshape(1)

    drive = spectral_call(scalar, everyone, far_table, near_table, tables, slab_count, back_steps)
    along_x = exchange(drive[0], groups)
    sine_part = sine_half_call(scalar, drive[1:5], tables, group, rows, back_steps)
    along_y = exchange(sine_part, groups)

    begin = jnp.maximum(slab - 1, 0) * cell_count
    below = lax.dynamic_slice_in_dim(everyone, begin, cell_count)
    level = lax.dynamic_slice_in_dim(everyone, slab * cell_count, cell_count)
    near_cells = jnp.concatenate([level, below], axis=0)
    low = near_cells[:, 0].astype(jnp.int32)
    wide = near_cells[:, 1].astype(jnp.int32)
    turn = M.bit_length() - 1
    block = lax.iota(jnp.int32, 2 * cell_count)[:, None]
    used = (block < cell_count) | ((member == 0) & (slab > 0))
    used = used.astype(F32)
    region = (low >> turn) & (REGIONS - 1)
    region = jnp.where(used > 0.0, region, REGIONS)
    fields = [
        (low & (M - 1)).astype(F32),
        (wide & (M - 1)).astype(F32),
        ((wide >> turn) + 1).astype(F32),
        ((low >> (turn + 2)) + 1).astype(F32),
        region.astype(F32),
        near_cells[:, 2],
        near_cells[:, 3],
        near_cells[:, 3],
    ]
    cells = jnp.stack(fields).reshape(8, 2 * cell_count * own)
    xt, yt, sums = local_call(scalar, cells, rows, count)

    sums = jnp.concatenate([sums, drive[5]], axis=0)
    reach = 1
    while reach < count:
        sums = sums + lax.ppermute(sums, AXES, [(i, i ^ reach) for i in range(count)])
        reach *= 2
    sums = jnp.sum(sums.reshape(3, 8 * 128), axis=1)

    fwd, sy, ce, se = tables[0:2], tables[2:4], tables[4:6], tables[6:8]
    field_x, force_x = field_call(scalar, along_x, se, sy, xt, yt, back_steps, rows, count, True)
    field_y, force_y = field_call(scalar, along_y, ce, fwd, xt, yt, back_steps, rows, count, False)
    partial = jnp.concatenate([force_x, force_y], axis=0).reshape(2, 2 * cell_count, own)
    cell_force = lax.dynamic_index_in_dim(partial, member, 1, keepdims=False)
    for turn in range(1, cell_count):
        piece = lax.dynamic_index_in_dim(partial, (member + turn) % cell_count, 1, keepdims=False)
        pairs = [
            (s * cell_count + c, s * cell_count + (c + turn) % cell_count)
            for s in range(slab_count)
            for c in range(cell_count)
        ]
        cell_force = cell_force + lax.ppermute(piece, AXES, pairs)
    for c in range(cell_count):
        pairs = [(s * cell_count, (s - 1) * cell_count + c) for s in range(1, slab_count)]
        cell_force = cell_force + lax.ppermute(partial[:, cell_count + c], AXES, pairs)
    energy = sums[2] / (2 * M * M)
    overflow = sums[0] / sums[1]
    shape = (REGIONS, rows, M)
    return (field_x.reshape(shape), field_y.reshape(shape), cell_force, energy, overflow)


def work(*args):
    count = lax.axis_size("slab") * lax.axis_size("cell")
    if packable(M // count):
        return half_work(*args)
    return full_work(*args)


def solution(mesh):
    return jax.shard_map(
        work,
        mesh=mesh,
        in_specs=(
            P(("slab", "cell")),
            P(("slab", "cell")),
            P(("slab", "cell")),
            P(("slab", "cell")),
            P(("slab", "cell")),
            P(None, ("slab", "cell")),
        ),
        out_specs=(
            P(None, ("slab", "cell"), None),
            P(None, ("slab", "cell"), None),
            P(None, ("slab", "cell")),
            P(),
            P(),
        ),
        check_vma=False,
    )
```

```python
import functools
import math

import jax
import jax.numpy as jnp
import numpy as np
from jax import lax
from jax.experimental import pallas as pl
from jax.experimental.pallas import tpu as pltpu
from jax.sharding import PartitionSpec as P

M = 2048
REGIONS = 4
HMAX = 4
WMAX = 8
HALF = M // 2
STRIP = 32
BAND = 4
TILE = 256
PARTS = HALF // TILE
FINE = 8192.0
AXES = ("slab", "cell")
BF = jnp.bfloat16
F32 = jnp.float32
I16 = jnp.int16
VMEM_LIMIT = 56 * 1024 * 1024


def params():
    return pltpu.CompilerParams(
        dimension_semantics=("arbitrary",), vmem_limit_bytes=VMEM_LIMIT
    )


def steps_of(bound):
    return 32700.0 / math.log2(1.0 + bound * FINE)


def encode_wide(value, steps):
    code = jnp.minimum(jnp.log2(1.0 + jnp.abs(value) * FINE) * steps, 32767.0)
    return jnp.round(jnp.where(value < 0.0, -code, code))


def encode(value, steps):
    return encode_wide(value, steps).astype(jnp.int32).astype(I16)


def packable(rows):
    return rows == 64 and REGIONS == 4


def swap_halves(values):
    lane = lax.broadcasted_iota(jnp.int32, values[0].shape, 1)
    turned = [pltpu.roll(value, 64, 1) for value in values]
    first = jnp.where(lane < 64, values[0], turned[1])
    second = jnp.where(lane < 64, turned[0], values[1])
    return first, second


def pack(out, value):
    for pair in range(TILE // 128):
        tile = value[:, pair * 128 : (pair + 1) * 128]
        for half in range(2):
            here = pl.ds(half * 128, 128)
            low = tile[half * 128 : half * 128 + 64]
            high = tile[half * 128 + 64 : half * 128 + 128]
            first, second = swap_halves((low, high))
            out[2 * pair, :, here] = first.astype(jnp.int32).astype(I16)
            out[2 * pair + 1, :, here] = second.astype(jnp.int32).astype(I16)


def decode(code, steps):
    wide = code.astype(jnp.int32).astype(F32)
    size = (jnp.exp2(jnp.abs(wide) * (1.0 / steps)) - 1.0) * (1.0 / FINE)
    return jnp.where(wide < 0.0, -size, size)


def split(value):
    high = value.astype(BF)
    return high, (value - high.astype(F32)).astype(BF)


def dot(left, right):
    return lax.dot_general(left, right, (((1,), (0,)), ((), ())), preferred_element_type=F32)


def dot3(left_hi, left_lo, right_hi, right_lo):
    return dot(left_hi, right_hi) + (dot(left_lo, right_hi) + dot(left_hi, right_lo))


def base_tables():
    groups = HALF // STRIP
    unit = math.pi / (2 * M)
    turn = 4 * M
    place = (2 * np.arange(HALF) + 1)[None, :]
    freq = (2 * np.arange(HALF))[None, :]
    group = np.arange(groups)[:, None]
    inside = np.arange(STRIP)[:, None]
    gain = math.sqrt(2.0 / M)
    zero_gain = np.where(freq == 0, math.sqrt(0.5), 1.0)
    far = unit * (2 * STRIP * group * place % turn)
    far_t = unit * (2 * STRIP * group * freq % turn)
    near_even = unit * (2 * inside * place % turn)
    near_odd = unit * ((2 * inside + 1) * place % turn)
    near_t = unit * ((2 * inside + 1) * freq % turn)
    outer = np.stack([np.cos(far), np.sin(far), np.cos(far_t), np.sin(far_t)], axis=1)
    inner = np.stack(
        [
            gain * np.cos(near_even),
            gain * np.sin(near_even),
            gain * np.cos(near_odd),
            gain * np.sin(near_odd),
            gain * zero_gain * np.cos(near_t),
            gain * zero_gain * np.sin(near_t),
        ]
    )
    return outer.astype(np.float32), inner.astype(np.float32)


def table_kernel(device, outer, inner, fwd_hi, fwd_lo, sy_hi, sy_lo, ce_hi, ce_lo, se_hi, se_lo, look):
    @pl.when(pl.program_id(0) == 0)
    def _():
        look[...] = cell_tables(device[0], look.shape[0] // 4)

    for group in range(BAND):
        here = pl.ds(group * STRIP, STRIP)

        def pair(far, near):
            cos_far = outer[group, far : far + 1, :]
            sin_far = outer[group, far + 1 : far + 2, :]
            cos_near = inner[near]
            sin_near = inner[near + 1]
            return cos_far * cos_near - sin_far * sin_near, sin_far * cos_near + cos_far * sin_near

        cos_even, sin_even = pair(0, 0)
        if group == 0:
            row = lax.broadcasted_iota(jnp.int32, (STRIP, 1), 0) + pl.program_id(0) * STRIP
            cos_even = cos_even * jnp.where(row == 0, math.sqrt(0.5), 1.0).astype(F32)
        ce_hi[here, :], ce_lo[here, :] = split(cos_even)
        se_hi[here, :], se_lo[here, :] = split(sin_even)
        cos_odd, sin_odd = pair(0, 2)
        fwd_hi[here, HALF:], fwd_lo[here, HALF:] = split(cos_odd)
        sy_hi[here, HALF:], sy_lo[here, HALF:] = split(sin_odd)
        cos_t, sin_t = pair(2, 4)
        fwd_hi[here, :HALF], fwd_lo[here, :HALF] = split(cos_t)
        sy_hi[here, :HALF], sy_lo[here, :HALF] = split(sin_t)


def make_tables(first_q, width):
    outer, inner = base_tables()
    wide = jax.ShapeDtypeStruct((HALF, M), BF)
    square = jax.ShapeDtypeStruct((HALF, HALF), BF)
    wide_spec = pl.BlockSpec((BAND * STRIP, M), lambda g: (g, 0))
    square_spec = pl.BlockSpec((BAND * STRIP, HALF), lambda g: (g, 0))
    return pl.pallas_call(
        table_kernel,
        grid=(HALF // (BAND * STRIP),),
        in_specs=[
            pl.BlockSpec(memory_space=pltpu.SMEM),
            pl.BlockSpec((BAND, 4, HALF), lambda g: (g, 0, 0)),
            pl.BlockSpec((6, STRIP, HALF), lambda g: (0, 0, 0)),
        ],
        out_specs=[wide_spec] * 4
        + [square_spec] * 4
        + [pl.BlockSpec((4 * width, 2 * LOOK), lambda g: (0, 0))],
        out_shape=[wide] * 4
        + [square] * 4
        + [jax.ShapeDtypeStruct((4 * width, 2 * LOOK), F32)],
        compiler_params=params(),
        cost_estimate=pl.CostEstimate(
            flops=40 * HALF * HALF, transcendentals=0, bytes_accessed=24 * HALF * HALF
        ),
        name="tables",
    )(first_q, jnp.asarray(outer), jnp.asarray(inner))


def fold_rows(value):
    rows, cols = value.shape
    folded = jnp.sum(value.reshape(rows // 8, 8, cols), axis=0)
    out = folded[:, :128]
    for start in range(128, cols, 128):
        out = out + folded[:, start : start + 128]
    return out


def density_kernel(
    device,
    cells,
    fwd_hi,
    fwd_lo,
    xt,
    yt,
    codes,
    sums,
    dens,
    part_hi,
    part_lo,
    *,
    steps,
    rows,
    count,
):
    step = pl.program_id(0)
    total = cells.shape[1]
    chunk = 512

    @pl.when(step == 0)
    def _():
        line = lax.broadcasted_iota(jnp.int32, (yt.shape[0], 1), 0)
        inside = line & (rows - 1)
        place = jnp.where(device[0] >= count // 2, rows - 1 - inside, inside) + device[0] * rows
        place = place.astype(F32)
        region = (line >> (rows.bit_length() - 1)).astype(F32)
        for start in range(0, total, chunk):
            here = pl.ds(start, chunk)
            low = cells[6:7, here]
            rel = place - cells[0:1, here]
            high = jnp.minimum(rel + 1.0, low + cells[3:4, here])
            value = jnp.maximum(high - jnp.maximum(rel, low), 0.0)
            yt[:, here] = jnp.where(region == cells[4:5, here], value, 0.0).astype(BF)

    @pl.when(step < 2 * PARTS)
    def _():
        place = (step % PARTS) * TILE + lax.broadcasted_iota(jnp.int32, (TILE, 1), 0)
        place = jnp.where(step >= PARTS, M - 1 - place, place).astype(F32)
        acc = None
        for start in range(0, total, chunk):
            here = pl.ds(start, chunk)
            low = cells[5:6, here]
            rel = place - cells[1:2, here]
            high = jnp.minimum(rel + 1.0, low + cells[2:3, here])
            value = jnp.maximum(high - jnp.maximum(rel, low), 0.0).astype(BF)
            xt[:, here] = value
            part = lax.dot_general(
                yt[:, here], value, (((1,), (1,)), ((), ())), preferred_element_type=F32
            )
            acc = part if acc is None else acc + part
        dens[step] = acc

    @pl.when(step == 2 * PARTS)
    def _():
        over = jnp.zeros((8, 128), F32)
        full = jnp.zeros((8, 128), F32)
        for part in range(PARTS):
            here = pl.ds(part * TILE, TILE)
            near = dens[part]
            mirrored = dens[PARTS + part]
            even = near + mirrored
            over = over + fold_rows(
                jnp.maximum(near - 1.0, 0.0) + jnp.maximum(mirrored - 1.0, 0.0)
            )
            full = full + fold_rows(even)
            part_hi[0, :, here], part_lo[0, :, here] = split(even)
            part_hi[1, :, here], part_lo[1, :, here] = split(near - mirrored)
        sums[0:8, :] = over
        sums[8:16, :] = full

    @pl.when(step >= 2 * PARTS)
    def _():
        odd = jnp.where(step >= 3 * PARTS, 1, 0)
        out = dot3(part_hi[odd], part_lo[odd], fwd_hi[...], fwd_lo[...])
        if packable(rows):
            pack(codes, encode_wide(out, steps))
        else:
            codes[...] = encode(out, steps)


def density_call(device, cells, tables, rows, count, steps):
    total = cells.shape[1]
    lines = REGIONS * rows
    late = lambda t: (0, jnp.maximum(t - 2 * PARTS, 0))
    whole = lambda t: (0, 0)
    if packable(rows):
        code_spec = pl.BlockSpec(
            (TILE // rows, rows, lines), lambda t: (jnp.maximum(t - 2 * PARTS, 0), 0, 0)
        )
        code_shape = (count, rows, lines)
    else:
        code_spec = pl.BlockSpec((lines, TILE), late)
        code_shape = (lines, M)
    return pl.pallas_call(
        functools.partial(density_kernel, steps=steps, rows=rows, count=count),
        grid=(4 * PARTS,),
        in_specs=[
            pl.BlockSpec(memory_space=pltpu.SMEM),
            pl.BlockSpec((8, total), whole),
            pl.BlockSpec((HALF, TILE), late),
            pl.BlockSpec((HALF, TILE), late),
        ],
        out_specs=[
            pl.BlockSpec((TILE, total), lambda t: (jnp.minimum(t, 2 * PARTS - 1), 0)),
            pl.BlockSpec((lines, total), whole),
            code_spec,
            pl.BlockSpec((16, 128), whole),
        ],
        out_shape=[
            jax.ShapeDtypeStruct((M, total), BF),
            jax.ShapeDtypeStruct((lines, total), BF),
            jax.ShapeDtypeStruct(code_shape, I16),
            jax.ShapeDtypeStruct((16, 128), F32),
        ],
        scratch_shapes=[
            pltpu.VMEM((2 * PARTS, lines, TILE), F32),
            pltpu.VMEM((2, lines, HALF), BF),
            pltpu.VMEM((2, lines, HALF), BF),
        ],
        compiler_params=params(),
        cost_estimate=pl.CostEstimate(
            flops=2 * lines * M * (total + 3 * HALF), transcendentals=0, bytes_accessed=1 << 24
        ),
        name="density",
    )(device, cells, tables[0], tables[1])


def place_rows(out, first, top, bottom, steps):
    count, rows = out.shape[0], out.shape[1]
    top = encode(top, steps)
    bottom = encode(bottom, steps)
    for inner in range(TILE // rows):
        here = slice(inner * rows, (inner + 1) * rows)
        out[first + inner] = top[here]
        out[count - 1 - first - inner] = bottom[here]


def spectrum_kernel(
    device,
    codes,
    ce_hi,
    ce_lo,
    co_hi,
    co_lo,
    ct_hi,
    ct_lo,
    out,
    dye_hi,
    dye_lo,
    dyo_hi,
    dyo_lo,
    energy,
    even_hi,
    even_lo,
    odd_hi,
    odd_lo,
    dxe_hi,
    dxe_lo,
    dxo_hi,
    dxo_lo,
    *,
    fwd_steps,
    back_steps,
):
    step = pl.program_id(0)
    count, rows = codes.shape[0], codes.shape[1]

    @pl.when(step == 0)
    def _():
        for block in range(count // 2):
            here = pl.ds(block * rows, rows)
            near = decode(codes[block], fwd_steps)
            mirrored = decode(codes[count - 1 - block], fwd_steps)
            even_hi[here, :], even_lo[here, :] = split(near + mirrored)
            odd_hi[here, :], odd_lo[here, :] = split(near - mirrored)
        energy[...] = jnp.zeros((8, 128), F32)

    @pl.when(step < PARTS)
    def _():
        unit = math.pi / M
        lane = lax.broadcasted_iota(jnp.int32, (1, codes.shape[2]), 1) & (rows - 1)
        odd = jnp.where(device[0] >= count // 2, 1, 0)
        q = (2 * (rows * (device[0] - odd * (count // 2)) + lane) + odd).astype(F32)
        first = lax.broadcasted_iota(jnp.int32, (TILE, 1), 0) + step * TILE
        here = pl.ds(pl.multiple_of(step * TILE, TILE), TILE)

        def solve(spectrum, p):
            squared = p * p + q * q
            inverse = jnp.where(squared == 0.0, 0.0, 1.0 / jnp.where(squared == 0.0, 1.0, squared))
            scaled = spectrum * inverse
            return scaled * (q * (1.0 / unit)), scaled * (p * (1.0 / unit)), spectrum * scaled

        spec = dot3(ce_hi[...], ce_lo[...], even_hi[...], even_lo[...])
        drive_x, drive_y, power = solve(spec, (2 * first).astype(F32))
        dxe_hi[here, :], dxe_lo[here, :] = split(drive_x)
        dye_hi[...], dye_lo[...] = split(drive_y)
        spec = dot3(co_hi[...], co_lo[...], odd_hi[...], odd_lo[...])
        drive_x, drive_y, more = solve(spec, (2 * first + 1).astype(F32))
        dxo_hi[here, :], dxo_lo[here, :] = split(drive_x)
        dyo_hi[...], dyo_lo[...] = split(drive_y)
        both = power + more
        if both.shape[1] % 128:
            both = jnp.concatenate(
                [both, jnp.zeros((TILE, 128 - both.shape[1] % 128), F32)], axis=1
            )
        energy[...] += fold_rows(both) * (1.0 / (unit * unit))

    @pl.when(step >= PARTS)
    def _():
        even = dot3(ct_hi[...], ct_lo[...], dxe_hi[...], dxe_lo[...])
        odd = dot3(co_hi[...], co_lo[...], dxo_hi[...], dxo_lo[...])
        first = (step - PARTS) * (TILE // rows)
        place_rows(out, first, even + odd, even - odd, back_steps)


def spectrum_call(device, codes, tables, fwd_steps, back_steps):
    fwd_hi, fwd_lo, _, _, ce_hi, ce_lo, _, _ = tables
    count, rows, cols = codes.shape
    early = lambda t: (jnp.minimum(t, PARTS - 1), 0)
    drive = jax.ShapeDtypeStruct((HALF, cols), BF)
    return pl.pallas_call(
        functools.partial(spectrum_kernel, fwd_steps=fwd_steps, back_steps=back_steps),
        grid=(2 * PARTS,),
        in_specs=[
            pl.BlockSpec(memory_space=pltpu.SMEM),
            pl.BlockSpec((count, rows, cols), lambda t: (0, 0, 0)),
        ]
        + [pl.BlockSpec((TILE, HALF), early)] * 2
        + [pl.BlockSpec((TILE, HALF), lambda t: (t % PARTS, 1))] * 2
        + [pl.BlockSpec((TILE, HALF), lambda t: (jnp.maximum(t - PARTS, 0), 0))] * 2,
        out_specs=[pl.BlockSpec((count, rows, cols), lambda t: (0, 0, 0))]
        + [pl.BlockSpec((TILE, cols), early)] * 4
        + [pl.BlockSpec((8, 128), lambda t: (0, 0))],
        out_shape=[jax.ShapeDtypeStruct((count, rows, cols), I16)]
        + [drive] * 4
        + [jax.ShapeDtypeStruct((8, 128), F32)],
        scratch_shapes=[pltpu.VMEM((HALF, cols), BF)] * 8,
        compiler_params=params(),
        cost_estimate=pl.CostEstimate(
            flops=24 * HALF * HALF * cols, transcendentals=0, bytes_accessed=1 << 24
        ),
        name="spectrum",
    )(device, codes, ce_hi, ce_lo, fwd_hi, fwd_lo, fwd_hi, fwd_lo)


def sine_kernel(
    dye_hi, dye_lo, dyo_hi, dyo_lo, se_hi, se_lo, so_hi, so_lo, out, *, back_steps
):
    even = dot3(se_hi[...], se_lo[...], dye_hi[...], dye_lo[...])
    odd = dot3(so_hi[...], so_lo[...], dyo_hi[...], dyo_lo[...])
    first = pl.program_id(0) * (TILE // out.shape[1])
    place_rows(out, first, odd + even, odd - even, back_steps)


def sine_call(drives, tables, count, rows, back_steps):
    sy_hi, sy_lo = tables[2], tables[3]
    cols = drives[0].shape[1]
    return pl.pallas_call(
        functools.partial(sine_kernel, back_steps=back_steps),
        grid=(PARTS,),
        in_specs=[pl.BlockSpec((HALF, cols), lambda t: (0, 0))] * 4
        + [pl.BlockSpec((TILE, HALF), lambda t: (t, 0))] * 2
        + [pl.BlockSpec((TILE, HALF), lambda t: (t, 1))] * 2,
        out_specs=pl.BlockSpec((count, rows, cols), lambda t: (0, 0, 0)),
        out_shape=jax.ShapeDtypeStruct((count, rows, cols), I16),
        compiler_params=params(),
        cost_estimate=pl.CostEstimate(
            flops=12 * HALF * HALF * cols, transcendentals=0, bytes_accessed=1 << 23
        ),
        name="sine_rows",
    )(*drives, sy_hi, sy_lo, sy_hi, sy_lo)


def field_kernel(
    device,
    codes,
    even_hi,
    even_lo,
    odd_hi,
    odd_lo,
    x_near,
    x_far,
    yt,
    field,
    force,
    part_hi,
    part_lo,
    acc,
    *,
    steps,
    rows,
    count,
    sine,
    by_half,
):
    step = pl.program_id(0)
    flipped = device[0] >= count // 2

    @pl.when(step == 0)
    def _():
        if by_half:
            sources, width = codes.shape[0], codes.shape[2]
            for source in range(sources):
                value = decode(codes[source, 0 : REGIONS * rows, :], steps)
                part = 2 * source // sources
                here = pl.ds((source % (sources // 2)) * width, width)
                part_hi[part, :, here], part_lo[part, :, here] = split(value)
        elif packable(rows):
            for pair in range(count // 2):
                near = decode(codes[2 * pair], steps)
                far = decode(codes[2 * pair + 1], steps)
                part = 2 * pair // (count // 2)
                here = pl.ds((pair % (count // 4)) * 128, 128)
                for half in range(2):
                    lanes = slice(half * 128, (half + 1) * 128)
                    for inner, value in enumerate(swap_halves((near[:, lanes], far[:, lanes]))):
                        lines = pl.ds((2 * half + inner) * rows, rows)
                        part_hi[part, lines, here], part_lo[part, lines, here] = split(value)
        else:
            for part in range(2):
                for block in range(PARTS):
                    here = pl.ds(block * TILE, TILE)
                    value = decode(codes[:, part * HALF + block * TILE :][:, :TILE], steps)
                    part_hi[part, :, here], part_lo[part, :, here] = split(value)

    even = dot3(part_hi[0], part_lo[0], even_hi[...], even_lo[...])
    odd = dot3(part_hi[1], part_lo[1], odd_hi[...], odd_lo[...])
    near = even + odd
    far = odd - even if sine else even - odd
    gathered = dot(near.astype(BF), x_near[...]) + dot(far.astype(BF), x_far[...])

    @pl.when(step == 0)
    def _():
        acc[...] = gathered

    @pl.when(step > 0)
    def _():
        acc[...] += gathered

    lane = 127 - lax.broadcasted_iota(jnp.int32, (8, 128), 1)
    sub = lax.broadcasted_iota(jnp.int32, (8, 128), 0)
    sub = jnp.where(flipped, 7 - sub, sub)
    for region in range(near.shape[0] // rows):
        for block in range(rows // 8):
            start = region * rows + 8 * block
            target = region * rows + jnp.where(flipped, rows - 8 - 8 * block, 8 * block)
            target = pl.multiple_of(target, 8)
            for tile in range(TILE // 128):
                piece = near[start : start + 8, tile * 128 : (tile + 1) * 128]
                piece = jnp.take_along_axis(piece, sub, axis=0)
                col = pl.multiple_of(step * TILE + tile * 128, 128)
                field[pl.ds(target, 8), pl.ds(col, 128)] = piece
                piece = far[start : start + 8, tile * 128 : (tile + 1) * 128]
                piece = jnp.take_along_axis(piece, sub, axis=0)
                piece = jnp.take_along_axis(piece, lane, axis=1)
                col = pl.multiple_of(M - 128 - step * TILE - tile * 128, 128)
                field[pl.ds(target, 8), pl.ds(col, 128)] = piece

    @pl.when(step == PARTS - 1)
    def _():
        force[...] = jnp.sum(yt[...].astype(F32) * acc[...], axis=0, keepdims=True)


def field_call(device, codes, even, odd, xt, yt, steps, rows, count, sine, half=False):
    lines, total = yt.shape
    zeros = (0,) * codes.ndim
    return pl.pallas_call(
        functools.partial(field_kernel, steps=steps, rows=rows, count=count, sine=sine, by_half=half),
        grid=(PARTS,),
        in_specs=[
            pl.BlockSpec(memory_space=pltpu.SMEM),
            pl.BlockSpec(codes.shape, lambda t: zeros),
        ]
        + [pl.BlockSpec((HALF, TILE), lambda t: (0, t))] * 2
        + [pl.BlockSpec((HALF, TILE), lambda t: (0, PARTS + t))] * 2
        + [
            pl.BlockSpec((TILE, total), lambda t: (t, 0)),
            pl.BlockSpec((TILE, total), lambda t: (PARTS + t, 0)),
            pl.BlockSpec((lines, total), lambda t: (0, 0)),
        ],
        out_specs=[
            pl.BlockSpec((lines, M), lambda t: (0, 0)),
            pl.BlockSpec((1, total), lambda t: (0, 0)),
        ],
        out_shape=[
            jax.ShapeDtypeStruct((lines, M), F32),
            jax.ShapeDtypeStruct((1, total), F32),
        ],
        scratch_shapes=[
            pltpu.VMEM((2, lines, HALF), BF),
            pltpu.VMEM((2, lines, HALF), BF),
            pltpu.VMEM((lines, total), F32),
        ],
        compiler_params=params(),
        cost_estimate=pl.CostEstimate(
            flops=2 * lines * M * (total + 3 * HALF), transcendentals=0, bytes_accessed=1 << 24
        ),
        name="field_x" if sine else "field_y",
    )(device, codes, even[0], even[1], odd[0], odd[1], xt, xt, yt)


def profile(rel, low, extent):
    high = jnp.minimum(rel + 1.0, low + extent)
    return jnp.maximum(high - jnp.maximum(rel, low), 0.0)


def unpack(first, second):
    turn = M.bit_length() - 1
    first = first.astype(jnp.int32)
    second = second.astype(jnp.int32)
    row = (first & (M - 1)).astype(F32)
    region = (first >> turn) & (REGIONS - 1)
    height = ((first >> (turn + 2)) + 1).astype(F32)
    return row, region, height, second & (M - 1), ((second >> turn) + 1).astype(F32)


def local_kernel(device, everyone, xt, yt, sums, *, rows, count, cell_count):
    step = pl.program_id(0)
    chunk = everyone.shape[2]
    pieces = 2 * cell_count
    slab = device[0] >> (cell_count.bit_length() - 1)
    member = device[0] & (cell_count - 1)

    def source(piece):
        if piece < cell_count:
            return slab * cell_count + ((member + piece) & (cell_count - 1))
        return jnp.maximum(slab - 1, 0) * cell_count + piece - cell_count

    @pl.when(step == 0)
    def _():
        line = lax.broadcasted_iota(jnp.int32, (yt.shape[0], 1), 0)
        inside = line & (rows - 1)
        place = jnp.where(device[0] >= count // 2, rows - 1 - inside, inside) + device[0] * rows
        place = place.astype(F32)
        owner = line >> (rows.bit_length() - 1)
        reached = jnp.where((member == 0) & (slab > 0), 0, REGIONS)
        for piece in range(pieces):
            cell = everyone[source(piece)]
            row, region, height, _, _ = unpack(cell[0:1], cell[1:2])
            if piece >= cell_count:
                region = region + reached
            value = profile(place - row, cell[3:4], height)
            yt[:, pl.ds(piece * chunk, chunk)] = jnp.where(owner == region, value, 0.0).astype(BF)
        sums[...] = jnp.zeros((16, 128), F32)

    place = (step % PARTS) * TILE + lax.broadcasted_iota(jnp.int32, (TILE, 1), 0)
    place = jnp.where(step >= PARTS, M - 1 - place, place).astype(F32)
    acc = None
    for piece in range(pieces):
        here = pl.ds(piece * chunk, chunk)
        cell = everyone[source(piece)]
        _, _, _, col, width = unpack(cell[0:1], cell[1:2])
        value = profile(place - col.astype(F32), cell[2:3], width).astype(BF)
        xt[:, here] = value
        part = lax.dot_general(
            yt[:, here], value, (((1,), (1,)), ((), ())), preferred_element_type=F32
        )
        acc = part if acc is None else acc + part
    sums[0:8, :] += fold_rows(jnp.maximum(acc - 1.0, 0.0))
    sums[8:16, :] += fold_rows(acc)


def local_call(device, everyone, rows, count, cell_count):
    total = 2 * cell_count * everyone.shape[2]
    lines = REGIONS * rows
    whole = lambda t: (0, 0)
    return pl.pallas_call(
        functools.partial(local_kernel, rows=rows, count=count, cell_count=cell_count),
        grid=(2 * PARTS,),
        in_specs=[
            pl.BlockSpec(memory_space=pltpu.SMEM),
            pl.BlockSpec(everyone.shape, lambda t: (0, 0, 0)),
        ],
        out_specs=[
            pl.BlockSpec((TILE, total), lambda t: (t, 0)),
            pl.BlockSpec((lines, total), whole),
            pl.BlockSpec((16, 128), whole),
        ],
        out_shape=[
            jax.ShapeDtypeStruct((M, total), BF),
            jax.ShapeDtypeStruct((lines, total), BF),
            jax.ShapeDtypeStruct((16, 128), F32),
        ],
        compiler_params=params(),
        cost_estimate=pl.CostEstimate(
            flops=2 * lines * M * total, transcendentals=0, bytes_accessed=1 << 23
        ),
        name="local",
    )(device, everyone)


BATCH = 2
BIG = 512
BIG_PARTS = HALF // BIG
NEAR = 32
LOOK = 64
EXTRA = 16
DIGIT = 2048.0
SCALAR_STEPS = steps_of(2.0**36)


def spectral_kernel(
    device,
    cells,
    look_table,
    ce_hi,
    ce_lo,
    co_hi,
    co_lo,
    ct_hi,
    ct_lo,
    out,
    dye_hi,
    dye_lo,
    dyo_hi,
    dyo_lo,
    energy,
    dens,
    look,
    even_hi,
    even_lo,
    odd_hi,
    odd_lo,
    dxe_hi,
    dxe_lo,
    dxo_hi,
    dxo_lo,
    *,
    slab_count,
    count,
    batch,
    back_steps,
):
    step = pl.program_id(0)
    cell_steps = slab_count // batch
    slab_rows = M // slab_count
    group = count // 2
    rows = M // count
    width = M // group
    window = slab_rows + EXTRA
    upper = device[0] >= group
    member = jnp.where(upper, device[0] - group, device[0])
    sign = jnp.where(upper, -1.0, 1.0).astype(F32)

    @pl.when(step == 0)
    def _():
        dens[...] = jnp.zeros(dens.shape, F32)
        look[:, : 2 * LOOK], look[:, 2 * LOOK :] = split(look_table[...])
        energy[...] = jnp.zeros((8, 128), F32)

    def add_slab(slab, pieces):
        top = slab >= slab_count // 2
        line = lax.broadcasted_iota(jnp.int32, (window, 1), 0)
        line = jnp.where(top, window - 1 - line, line) + slab * slab_rows
        line = line.astype(F32)
        turn = M.bit_length() - 1
        acc = None
        for piece in pieces:
            first = cells[piece, 0:1, :].astype(jnp.int32)
            second = cells[piece, 1:2, :].astype(jnp.int32)
            low_x = cells[piece, 2:3, :]
            low_y = cells[piece, 3:4, :]
            row = (first & (M - 1)).astype(F32)
            region = (first >> turn) & (REGIONS - 1)
            height = ((first >> (turn + 2)) + 1).astype(F32)
            col = second & (M - 1)
            wide = second >> turn
            width_x = (wide + 1).astype(F32)
            value_y = profile(line - row, low_y, height)
            stacked = jnp.concatenate(
                [jnp.where(region == g, value_y, 0.0).astype(BF) for g in range(REGIONS)], axis=0
            )
            slot = lax.broadcasted_iota(jnp.int32, (NEAR + 16, 1), 0).astype(F32)
            inside = (col & (NEAR - 1)).astype(F32)
            feature = profile(slot - inside, low_x, width_x).astype(BF)
            feature = jnp.concatenate(
                [feature, jnp.zeros((LOOK - NEAR - 16, feature.shape[1]), BF)], axis=0
            )
            spot = lax.broadcasted_iota(jnp.int32, (LOOK, 1), 0)
            chosen = jnp.where(spot == (col >> (NEAR.bit_length() - 1)), 1.0, 0.0).astype(BF)
            found = dot(look[...], jnp.concatenate([feature, chosen, feature, chosen], axis=0))
            value = found[:width] * found[2 * width : 3 * width]
            value = value - found[width : 2 * width] * found[3 * width :]
            value = jnp.concatenate(split(value), axis=0)
            part = lax.dot_general(
                stacked, value, (((1,), (1,)), ((), ())), preferred_element_type=F32
            )
            acc = part if acc is None else acc + part
        half = jnp.where(top, 1, 0)
        start = jnp.where(top, slab_count - 1 - slab, slab) * slab_rows
        here = pl.ds(pl.multiple_of(start, 8), window)
        for g in range(REGIONS):
            lines = slice(g * window, (g + 1) * window)
            lanes = pl.ds(g * width, width)
            dens[half, here, lanes] += acc[lines, :width] + acc[lines, width:]

    @pl.when(step < cell_steps)
    def _():
        share = count // slab_count
        for inner in range(batch):
            add_slab(step * batch + inner, range(inner * share, (inner + 1) * share))

    @pl.when(step == cell_steps)
    def _():
        sub = 7 - lax.broadcasted_iota(jnp.int32, (8, 128), 0)
        for tile in range(dens.shape[2] // 128):
            lanes = pl.ds(tile * 128, 128)
            spill = jnp.take_along_axis(dens[0, HALF : HALF + 8, lanes], sub, axis=0)
            dens[1, HALF + EXTRA - 8 : HALF + EXTRA, lanes] += spill
        for block in range(HALF // 128):
            here = pl.ds(block * 128, 128)
            near = dens[0, here, :]
            mirrored = dens[1, pl.ds(block * 128 + EXTRA, 128), :]
            even_hi[here, :], even_lo[here, :] = split(near + mirrored)
            odd_hi[here, :], odd_lo[here, :] = split(near - mirrored)

    @pl.when((step >= cell_steps) & (step < cell_steps + BIG_PARTS))
    def _():
        turn = step - cell_steps
        unit = math.pi / M
        lane = lax.broadcasted_iota(jnp.int32, (1, width), 1)
        odd = jnp.where(member >= group // 2, 1, 0)
        q = (2 * (width * (member - odd * (group // 2)) + lane) + odd).astype(F32)
        first = lax.broadcasted_iota(jnp.int32, (BIG, 1), 0) + turn * BIG
        here = pl.ds(pl.multiple_of(turn * BIG, BIG), BIG)
        spent = jnp.zeros((8, 128), F32)

        def solve(spectrum, p, x_hi, x_lo, y_hi, y_lo, sign_x, sign_y, spent):
            squared = p * p + q * q
            inverse = jnp.where(squared == 0.0, 0.0, 1.0 / jnp.where(squared == 0.0, 1.0, squared))
            factor_x = inverse * (q * (sign_x / unit))
            factor_y = inverse * (p * (sign_y / unit))
            for g in range(REGIONS):
                lanes = pl.ds(g * width, width)
                part = spectrum[:, g * width : (g + 1) * width]
                x_hi[here, lanes], x_lo[here, lanes] = split(part * factor_x)
                y_hi[:, lanes], y_lo[:, lanes] = split(part * factor_y)
                spent = spent + fold_rows(part * (part * inverse))
            return spent

        spec = dot3(ce_hi[...], ce_lo[...], even_hi[...], even_lo[...])
        spent = solve(
            spec, (2 * first).astype(F32), dxe_hi, dxe_lo, dye_hi, dye_lo, 1.0, sign, spent
        )
        spec = dot3(co_hi[...], co_lo[...], odd_hi[...], odd_lo[...])
        spent = solve(
            spec, (2 * first + 1).astype(F32), dxo_hi, dxo_lo, dyo_hi, dyo_lo, sign, 1.0, spent
        )
        energy[...] += spent * (1.0 / (unit * unit))

    @pl.when(step >= cell_steps + BIG_PARTS)
    def _():
        value = dot3(ct_hi[...], ct_lo[...], dxe_hi[...], dxe_lo[...])
        value = value + dot3(co_hi[...], co_lo[...], dxo_hi[...], dxo_lo[...])
        first = (step - cell_steps - BIG_PARTS) * (BIG // rows)
        send_rows(out, first, value, upper, rows, back_steps)


def send_rows(out, first, value, upper, rows, steps):
    count, width = out.shape[0], out.shape[2]
    code = encode(value, steps)
    for inner in range(value.shape[0] // rows):
        target = first + inner
        target = jnp.where(upper, count - 1 - target, target)
        for g in range(REGIONS):
            here = pl.ds(g * rows, rows)
            piece = code[inner * rows : (inner + 1) * rows, g * width : (g + 1) * width]
            out[target, here, :] = piece


def spectral_call(device, cells, look_table, tables, slab_count, back_steps):
    fwd_hi, fwd_lo, _, _, ce_hi, ce_lo, _, _ = tables
    count = cells.shape[0]
    group = count // 2
    rows = M // count
    width = M // group
    cols = REGIONS * width
    batch = math.gcd(slab_count, BATCH)
    cell_steps = slab_count // batch
    share = batch * count // slab_count
    phase = lambda t: jnp.clip(t - cell_steps, 0, BIG_PARTS - 1)
    last = lambda t: jnp.clip(t - cell_steps - BIG_PARTS, 0, BIG_PARTS - 1)
    both = lambda t: jnp.where(t < cell_steps, 0, (t - cell_steps) % BIG_PARTS)
    drive = jax.ShapeDtypeStruct((HALF, cols), BF)
    return pl.pallas_call(
        functools.partial(
            spectral_kernel,
            slab_count=slab_count,
            count=count,
            batch=batch,
            back_steps=back_steps,
        ),
        grid=(cell_steps + 2 * BIG_PARTS,),
        in_specs=[
            pl.BlockSpec(memory_space=pltpu.SMEM),
            pl.BlockSpec(
                (share,) + cells.shape[1:], lambda t: (jnp.minimum(t, cell_steps - 1), 0, 0)
            ),
            pl.BlockSpec(look_table.shape, lambda t: (0, 0)),
        ]
        + [pl.BlockSpec((BIG, HALF), lambda t: (phase(t), 0))] * 2
        + [pl.BlockSpec((BIG, HALF), lambda t: (both(t), 1))] * 2
        + [pl.BlockSpec((BIG, HALF), lambda t: (last(t), 0))] * 2,
        out_specs=[pl.BlockSpec((group, REGIONS * rows, width), lambda t: (0, 0, 0))]
        + [pl.BlockSpec((BIG, cols), lambda t: (phase(t), 0))] * 4
        + [pl.BlockSpec((8, 128), lambda t: (0, 0))],
        out_shape=[jax.ShapeDtypeStruct((group, REGIONS * rows, width), I16)]
        + [drive] * 4
        + [jax.ShapeDtypeStruct((8, 128), F32)],
        scratch_shapes=[
            pltpu.VMEM((2, HALF + EXTRA, cols), F32),
            pltpu.VMEM((4 * width, 4 * LOOK), BF),
        ]
        + [pltpu.VMEM((HALF, cols), BF)] * 8,
        compiler_params=params(),
        cost_estimate=pl.CostEstimate(
            flops=30 * HALF * HALF * cols, transcendentals=0, bytes_accessed=1 << 24
        ),
        name="spectral",
    )(device, cells, look_table, ce_hi, ce_lo, fwd_hi, fwd_lo, fwd_hi, fwd_lo)


def sine_half_kernel(
    device,
    sums,
    power,
    dye_hi,
    dye_lo,
    dyo_hi,
    dyo_lo,
    se_hi,
    se_lo,
    so_hi,
    so_lo,
    out,
    *,
    rows,
    back_steps,
):
    @pl.when(pl.program_id(0) == 0)
    def _():
        def digits(parts):
            total = jnp.sum(jnp.sum(parts, axis=1, keepdims=True), axis=0, keepdims=True)
            first = encode_wide(total, SCALAR_STEPS)
            rest = (total - decode(first.astype(jnp.int32), SCALAR_STEPS)) * DIGIT
            return [first, encode_wide(rest, SCALAR_STEPS)]

        shape = (EXTRA, out.shape[2])
        lane = lax.broadcasted_iota(jnp.int32, shape, 1)
        lane = jnp.where(lax.broadcasted_iota(jnp.int32, shape, 0) == 0, lane, -1)
        block = jnp.zeros(shape, F32)
        codes = digits(sums[0:8, :]) + digits(sums[8:16, :])
        codes = codes + digits(power[...] * (1.0 / (M * M)))
        for index, code in enumerate(codes):
            block = jnp.where(lane == index, code, block)
        block = block.astype(jnp.int32).astype(I16)
        for target in range(out.shape[0]):
            out[target, REGIONS * rows : REGIONS * rows + EXTRA, :] = block

    value = dot3(se_hi[...], se_lo[...], dye_hi[...], dye_lo[...])
    value = value + dot3(so_hi[...], so_lo[...], dyo_hi[...], dyo_lo[...])
    first = pl.program_id(0) * (TILE // rows)
    send_rows(out, first, value, device[0] >= out.shape[0], rows, back_steps)


def sine_half_call(device, sums, power, drives, tables, group, rows, back_steps):
    sy_hi, sy_lo = tables[2], tables[3]
    cols = drives[0].shape[1]
    shape = (group, REGIONS * rows + EXTRA, cols // REGIONS)
    return pl.pallas_call(
        functools.partial(sine_half_kernel, rows=rows, back_steps=back_steps),
        grid=(PARTS,),
        in_specs=[
            pl.BlockSpec(memory_space=pltpu.SMEM),
            pl.BlockSpec((16, 128), lambda t: (0, 0)),
            pl.BlockSpec((8, 128), lambda t: (0, 0)),
        ]
        + [pl.BlockSpec((HALF, cols), lambda t: (0, 0))] * 4
        + [pl.BlockSpec((TILE, HALF), lambda t: (t, 0))] * 2
        + [pl.BlockSpec((TILE, HALF), lambda t: (t, 1))] * 2,
        out_specs=pl.BlockSpec(shape, lambda t: (0, 0, 0)),
        out_shape=jax.ShapeDtypeStruct(shape, I16),
        compiler_params=params(),
        cost_estimate=pl.CostEstimate(
            flops=12 * HALF * HALF * cols, transcendentals=0, bytes_accessed=1 << 23
        ),
        name="sine_half",
    )(device, sums, power, *drives, sy_hi, sy_lo, sy_hi, sy_lo)


def cell_tables(first_q, width):
    line = lax.broadcasted_iota(jnp.int32, (2 * width, 2 * LOOK), 0)
    lane = lax.broadcasted_iota(jnp.int32, (2 * width, 2 * LOOK), 1)
    q = first_q + 2 * (line & (width - 1))
    near = lane < LOOK
    moment = jnp.where(near, 2 * lane + 1, 2 * NEAR * (lane - LOOK))
    phase = (q * moment + jnp.where(line < width, 0, 3 * M)) & (4 * M - 1)
    weight = jnp.where(q == 0, math.sqrt(1.0 / M), math.sqrt(2.0 / M)).astype(F32)
    value = jnp.cos(phase.astype(F32) * (math.pi / (2.0 * M)))
    return jnp.concatenate(
        [jnp.where(near, value * weight, 0.0), jnp.where(near, 0.0, value)], axis=0
    )


def exchange(blocks, groups=None):
    return lax.all_to_all(
        blocks, AXES, split_axis=0, concat_axis=0, tiled=True, axis_index_groups=groups
    )


def full_work(cell_row, cell_col, cell_width, cell_height, cell_region, cell_offset):
    slab_count = lax.axis_size("slab")
    cell_count = lax.axis_size("cell")
    count = slab_count * cell_count
    device = lax.axis_index("slab") * cell_count + lax.axis_index("cell")
    rows = M // count
    own = cell_row.shape[0]
    lines = REGIONS * rows
    gain = math.sqrt(2.0 / M)
    fwd_steps = steps_of(2.1 * own * cell_count * WMAX * gain)
    back_steps = steps_of(gain**3 * own * count * WMAX * HMAX * 1.1 * M / math.pi * 8.5)

    ints = [cell_row, cell_col, cell_width, cell_height, cell_region]
    mine = jnp.concatenate(
        [jnp.stack(ints).astype(F32), cell_offset, jnp.zeros((1, own), F32)], axis=0
    )
    pieces = [mine]
    back_moves = []
    for turn in range(1, cell_count):
        pairs = [
            (slab * cell_count + c, slab * cell_count + (c + turn) % cell_count)
            for slab in range(slab_count)
            for c in range(cell_count)
        ]
        pieces.append(lax.ppermute(mine, AXES, pairs))
        back_moves.append([(b, a) for a, b in pairs])
    for c in range(cell_count):
        pairs = [
            (slab * cell_count + c, (slab + 1) * cell_count) for slab in range(slab_count - 1)
        ]
        pieces.append(lax.ppermute(mine, AXES, pairs))
        back_moves.append([(b, a) for a, b in pairs])
    tables = make_tables(jnp.zeros((1,), jnp.int32), 128)[:8]
    cells = jnp.concatenate(pieces, axis=1)

    device = device.astype(jnp.int32).reshape(1)
    xt, yt, codes, sums = density_call(device, cells, tables, rows, count, fwd_steps)
    if not packable(rows):
        codes = jnp.transpose(codes.reshape(REGIONS, rows, count, rows), (2, 1, 0, 3))
        codes = codes.reshape(count, rows, lines)
    arrived = exchange(codes)
    drive = spectrum_call(device, arrived, tables, fwd_steps, back_steps)
    along_x = exchange(drive[0])
    sine_part = sine_call(drive[1:5], tables, count, rows, back_steps)
    along_y = exchange(sine_part)

    sums = jnp.concatenate([sums, drive[5]], axis=0)
    reach = 1
    while reach < count:
        sums = sums + lax.ppermute(sums, AXES, [(i, i ^ reach) for i in range(count)])
        reach *= 2
    sums = jnp.sum(sums.reshape(3, 8 * 128), axis=1)

    def lines_of(blocks):
        if packable(rows):
            return blocks
        shaped = blocks.reshape(count, rows, REGIONS, rows)
        return jnp.transpose(shaped, (2, 1, 0, 3)).reshape(lines, M)

    fwd, sy, ce, se = tables[0:2], tables[2:4], tables[4:6], tables[6:8]
    field_x, force_x = field_call(
        device, lines_of(along_x), se, sy, xt, yt, back_steps, rows, count, True
    )
    field_y, force_y = field_call(
        device, lines_of(along_y), ce, fwd, xt, yt, back_steps, rows, count, False
    )
    partial = jnp.concatenate([force_x, force_y], axis=0)
    cell_force = partial[:, :own]
    for index, pairs in enumerate(back_moves):
        piece = partial[:, (index + 1) * own : (index + 2) * own]
        cell_force = cell_force + lax.ppermute(piece, AXES, pairs)
    energy = sums[2] / (M * M)
    overflow = sums[0] / sums[1]
    shape = (REGIONS, rows, M)
    return (field_x.reshape(shape), field_y.reshape(shape), cell_force, energy, overflow)


def half_work(cell_row, cell_col, cell_width, cell_height, cell_region, cell_offset):
    slab_count = lax.axis_size("slab")
    cell_count = lax.axis_size("cell")
    count = slab_count * cell_count
    group = count // 2
    slab = lax.axis_index("slab")
    member = lax.axis_index("cell")
    device = slab * cell_count + member
    rows = M // count
    width = M // group
    lines = REGIONS * rows
    own = cell_row.shape[0]
    gain = math.sqrt(2.0 / M)
    back_steps = steps_of(gain**3 * own * count * WMAX * HMAX * 1.1 * M / math.pi * 8.5)
    groups = [list(range(group)), list(range(group, count))]

    first = (cell_row + M * (cell_region + REGIONS * (cell_height - 1))).astype(F32)
    second = (cell_col + M * (cell_width - 1)).astype(F32)
    kind = lax.broadcasted_iota(jnp.int32, (count, 4, own), 1)
    mine = jnp.where(kind == 2, cell_offset[0][None, None, :], cell_offset[1][None, None, :])
    mine = jnp.where(kind == 1, second[None, None, :], mine)
    mine = jnp.where(kind == 0, first[None, None, :], mine)
    everyone = exchange(mine)
    within = device % group
    odd = within // (group // 2)
    first_q = 2 * width * (within - odd * (group // 2)) + odd
    tables = make_tables(first_q.astype(jnp.int32).reshape(1), width)
    scalar = device.astype(jnp.int32).reshape(1)

    drive = spectral_call(scalar, everyone, tables[8], tables[:8], slab_count, back_steps)
    along_x = exchange(drive[0], groups)
    xt, yt, sums = local_call(scalar, everyone, rows, count, cell_count)
    sine_part = sine_half_call(scalar, sums, drive[5], drive[1:5], tables, group, rows, back_steps)
    along_y = exchange(sine_part, groups)
    scalars = jnp.sum(decode(along_y[:, lines : lines + 8, :], SCALAR_STEPS), axis=0)
    other = lax.ppermute(scalars, AXES, [(i, (i + group) % count) for i in range(count)])
    joint = scalars[0] + other[0]

    fwd, sy, ce, se = tables[0:2], tables[2:4], tables[4:6], tables[6:8]
    field_x, force_x = field_call(
        scalar, along_x, se, sy, xt, yt, back_steps, rows, count, True, True
    )
    field_y, force_y = field_call(
        scalar, along_y, ce, fwd, xt, yt, back_steps, rows, count, False, True
    )
    partial = jnp.concatenate([force_x, force_y], axis=0).reshape(2, 2 * cell_count, own)
    cell_force = partial[:, 0]
    for turn in range(1, cell_count):
        piece = partial[:, turn]
        pairs = [
            (s * cell_count + c, s * cell_count + (c + turn) % cell_count)
            for s in range(slab_count)
            for c in range(cell_count)
        ]
        cell_force = cell_force + lax.ppermute(piece, AXES, pairs)
    for c in range(cell_count):
        pairs = [(s * cell_count, (s - 1) * cell_count + c) for s in range(1, slab_count)]
        cell_force = cell_force + lax.ppermute(partial[:, cell_count + c], AXES, pairs)
    energy = scalars[0, 4] + scalars[0, 5] * (1.0 / DIGIT)
    overflow = (joint[0] + joint[1] * (1.0 / DIGIT)) / (joint[2] + joint[3] * (1.0 / DIGIT))
    shape = (REGIONS, rows, M)
    return (field_x.reshape(shape), field_y.reshape(shape), cell_force, energy, overflow)


def work(*args):
    count = lax.axis_size("slab") * lax.axis_size("cell")
    if packable(M // count):
        return half_work(*args)
    return full_work(*args)


def solution(mesh):
    return jax.shard_map(
        work,
        mesh=mesh,
        in_specs=(
            P(("slab", "cell")),
            P(("slab", "cell")),
            P(("slab", "cell")),
            P(("slab", "cell")),
            P(("slab", "cell")),
            P(None, ("slab", "cell")),
        ),
        out_specs=(
            P(None, ("slab", "cell"), None),
            P(None, ("slab", "cell"), None),
            P(None, ("slab", "cell")),
            P(),
            P(),
        ),
        check_vma=False,
    )
```

```python
import functools
import math

import jax
import jax.numpy as jnp
import numpy as np
from jax import lax
from jax.experimental import pallas as pl
from jax.experimental.pallas import tpu as pltpu
from jax.sharding import PartitionSpec as P

M = 2048
REGIONS = 4
HMAX = 4
WMAX = 8
HALF = M // 2
STRIP = 32
BAND = 4
TILE = 256
PARTS = HALF // TILE
FINE = 8192.0
AXES = ("slab", "cell")
BF = jnp.bfloat16
F32 = jnp.float32
I16 = jnp.int16
VMEM_LIMIT = 56 * 1024 * 1024


def params():
    return pltpu.CompilerParams(
        dimension_semantics=("arbitrary",), vmem_limit_bytes=VMEM_LIMIT
    )


def steps_of(bound):
    return 32700.0 / math.log2(1.0 + bound * FINE)


def encode_wide(value, steps):
    code = jnp.minimum(jnp.log2(1.0 + jnp.abs(value) * FINE) * steps, 32767.0)
    return jnp.round(jnp.where(value < 0.0, -code, code))


def encode(value, steps):
    return encode_wide(value, steps).astype(jnp.int32).astype(I16)


def packable(rows):
    return rows == 64 and REGIONS == 4


def swap_halves(values):
    lane = lax.broadcasted_iota(jnp.int32, values[0].shape, 1)
    turned = [pltpu.roll(value, 64, 1) for value in values]
    first = jnp.where(lane < 64, values[0], turned[1])
    second = jnp.where(lane < 64, turned[0], values[1])
    return first, second


def pack(out, value):
    for pair in range(TILE // 128):
        tile = value[:, pair * 128 : (pair + 1) * 128]
        for half in range(2):
            here = pl.ds(half * 128, 128)
            low = tile[half * 128 : half * 128 + 64]
            high = tile[half * 128 + 64 : half * 128 + 128]
            first, second = swap_halves((low, high))
            out[2 * pair, :, here] = first.astype(jnp.int32).astype(I16)
            out[2 * pair + 1, :, here] = second.astype(jnp.int32).astype(I16)


def decode(code, steps):
    wide = code.astype(jnp.int32).astype(F32)
    size = (jnp.exp2(jnp.abs(wide) * (1.0 / steps)) - 1.0) * (1.0 / FINE)
    return jnp.where(wide < 0.0, -size, size)


def split(value):
    high = value.astype(BF)
    return high, (value - high.astype(F32)).astype(BF)


def dot(left, right):
    return lax.dot_general(left, right, (((1,), (0,)), ((), ())), preferred_element_type=F32)


def dot3(left_hi, left_lo, right_hi, right_lo):
    return dot(left_hi, right_hi) + (dot(left_lo, right_hi) + dot(left_hi, right_lo))


def base_tables():
    groups = HALF // STRIP
    unit = math.pi / (2 * M)
    turn = 4 * M
    place = (2 * np.arange(HALF) + 1)[None, :]
    freq = (2 * np.arange(HALF))[None, :]
    group = np.arange(groups)[:, None]
    inside = np.arange(STRIP)[:, None]
    gain = math.sqrt(2.0 / M)
    zero_gain = np.where(freq == 0, math.sqrt(0.5), 1.0)
    far = unit * (2 * STRIP * group * place % turn)
    far_t = unit * (2 * STRIP * group * freq % turn)
    near_even = unit * (2 * inside * place % turn)
    near_odd = unit * ((2 * inside + 1) * place % turn)
    near_t = unit * ((2 * inside + 1) * freq % turn)
    outer = np.stack([np.cos(far), np.sin(far), np.cos(far_t), np.sin(far_t)], axis=1)
    inner = np.stack(
        [
            gain * np.cos(near_even),
            gain * np.sin(near_even),
            gain * np.cos(near_odd),
            gain * np.sin(near_odd),
            gain * zero_gain * np.cos(near_t),
            gain * zero_gain * np.sin(near_t),
        ]
    )
    return outer.astype(np.float32), inner.astype(np.float32)


def table_kernel(device, outer, inner, fwd_hi, fwd_lo, sy_hi, sy_lo, ce_hi, ce_lo, se_hi, se_lo, look):
    @pl.when(pl.program_id(0) == 0)
    def _():
        look[...] = cell_tables(device[0], look.shape[0] // 4)

    for group in range(BAND):
        here = pl.ds(group * STRIP, STRIP)

        def pair(far, near):
            cos_far = outer[group, far : far + 1, :]
            sin_far = outer[group, far + 1 : far + 2, :]
            cos_near = inner[near]
            sin_near = inner[near + 1]
            return cos_far * cos_near - sin_far * sin_near, sin_far * cos_near + cos_far * sin_near

        cos_even, sin_even = pair(0, 0)
        if group == 0:
            row = lax.broadcasted_iota(jnp.int32, (STRIP, 1), 0) + pl.program_id(0) * STRIP
            cos_even = cos_even * jnp.where(row == 0, math.sqrt(0.5), 1.0).astype(F32)
        ce_hi[here, :], ce_lo[here, :] = split(cos_even)
        se_hi[here, :], se_lo[here, :] = split(sin_even)
        cos_odd, sin_odd = pair(0, 2)
        fwd_hi[here, HALF:], fwd_lo[here, HALF:] = split(cos_odd)
        sy_hi[here, HALF:], sy_lo[here, HALF:] = split(sin_odd)
        cos_t, sin_t = pair(2, 4)
        fwd_hi[here, :HALF], fwd_lo[here, :HALF] = split(cos_t)
        sy_hi[here, :HALF], sy_lo[here, :HALF] = split(sin_t)


def make_tables(first_q, width):
    outer, inner = base_tables()
    wide = jax.ShapeDtypeStruct((HALF, M), BF)
    square = jax.ShapeDtypeStruct((HALF, HALF), BF)
    wide_spec = pl.BlockSpec((BAND * STRIP, M), lambda g: (g, 0))
    square_spec = pl.BlockSpec((BAND * STRIP, HALF), lambda g: (g, 0))
    return pl.pallas_call(
        table_kernel,
        grid=(HALF // (BAND * STRIP),),
        in_specs=[
            pl.BlockSpec(memory_space=pltpu.SMEM),
            pl.BlockSpec((BAND, 4, HALF), lambda g: (g, 0, 0)),
            pl.BlockSpec((6, STRIP, HALF), lambda g: (0, 0, 0)),
        ],
        out_specs=[wide_spec] * 4
        + [square_spec] * 4
        + [pl.BlockSpec((4 * width, 2 * LOOK), lambda g: (0, 0))],
        out_shape=[wide] * 4
        + [square] * 4
        + [jax.ShapeDtypeStruct((4 * width, 2 * LOOK), F32)],
        compiler_params=params(),
        cost_estimate=pl.CostEstimate(
            flops=40 * HALF * HALF, transcendentals=0, bytes_accessed=24 * HALF * HALF
        ),
        name="tables",
    )(first_q, jnp.asarray(outer), jnp.asarray(inner))


def fold_rows(value):
    rows, cols = value.shape
    folded = jnp.sum(value.reshape(rows // 8, 8, cols), axis=0)
    out = folded[:, :128]
    for start in range(128, cols, 128):
        out = out + folded[:, start : start + 128]
    return out


def density_kernel(
    device,
    cells,
    fwd_hi,
    fwd_lo,
    xt,
    yt,
    codes,
    sums,
    dens,
    part_hi,
    part_lo,
    *,
    steps,
    rows,
    count,
):
    step = pl.program_id(0)
    total = cells.shape[1]
    chunk = 512

    @pl.when(step == 0)
    def _():
        line = lax.broadcasted_iota(jnp.int32, (yt.shape[0], 1), 0)
        inside = line & (rows - 1)
        place = jnp.where(device[0] >= count // 2, rows - 1 - inside, inside) + device[0] * rows
        place = place.astype(F32)
        region = (line >> (rows.bit_length() - 1)).astype(F32)
        for start in range(0, total, chunk):
            here = pl.ds(start, chunk)
            low = cells[6:7, here]
            rel = place - cells[0:1, here]
            high = jnp.minimum(rel + 1.0, low + cells[3:4, here])
            value = jnp.maximum(high - jnp.maximum(rel, low), 0.0)
            yt[:, here] = jnp.where(region == cells[4:5, here], value, 0.0).astype(BF)

    @pl.when(step < 2 * PARTS)
    def _():
        place = (step % PARTS) * TILE + lax.broadcasted_iota(jnp.int32, (TILE, 1), 0)
        place = jnp.where(step >= PARTS, M - 1 - place, place).astype(F32)
        acc = None
        for start in range(0, total, chunk):
            here = pl.ds(start, chunk)
            low = cells[5:6, here]
            rel = place - cells[1:2, here]
            high = jnp.minimum(rel + 1.0, low + cells[2:3, here])
            value = jnp.maximum(high - jnp.maximum(rel, low), 0.0).astype(BF)
            xt[:, here] = value
            part = lax.dot_general(
                yt[:, here], value, (((1,), (1,)), ((), ())), preferred_element_type=F32
            )
            acc = part if acc is None else acc + part
        dens[step] = acc

    @pl.when(step == 2 * PARTS)
    def _():
        over = jnp.zeros((8, 128), F32)
        full = jnp.zeros((8, 128), F32)
        for part in range(PARTS):
            here = pl.ds(part * TILE, TILE)
            near = dens[part]
            mirrored = dens[PARTS + part]
            even = near + mirrored
            over = over + fold_rows(
                jnp.maximum(near - 1.0, 0.0) + jnp.maximum(mirrored - 1.0, 0.0)
            )
            full = full + fold_rows(even)
            part_hi[0, :, here], part_lo[0, :, here] = split(even)
            part_hi[1, :, here], part_lo[1, :, here] = split(near - mirrored)
        sums[0:8, :] = over
        sums[8:16, :] = full

    @pl.when(step >= 2 * PARTS)
    def _():
        odd = jnp.where(step >= 3 * PARTS, 1, 0)
        out = dot3(part_hi[odd], part_lo[odd], fwd_hi[...], fwd_lo[...])
        if packable(rows):
            pack(codes, encode_wide(out, steps))
        else:
            codes[...] = encode(out, steps)


def density_call(device, cells, tables, rows, count, steps):
    total = cells.shape[1]
    lines = REGIONS * rows
    late = lambda t: (0, jnp.maximum(t - 2 * PARTS, 0))
    whole = lambda t: (0, 0)
    if packable(rows):
        code_spec = pl.BlockSpec(
            (TILE // rows, rows, lines), lambda t: (jnp.maximum(t - 2 * PARTS, 0), 0, 0)
        )
        code_shape = (count, rows, lines)
    else:
        code_spec = pl.BlockSpec((lines, TILE), late)
        code_shape = (lines, M)
    return pl.pallas_call(
        functools.partial(density_kernel, steps=steps, rows=rows, count=count),
        grid=(4 * PARTS,),
        in_specs=[
            pl.BlockSpec(memory_space=pltpu.SMEM),
            pl.BlockSpec((8, total), whole),
            pl.BlockSpec((HALF, TILE), late),
            pl.BlockSpec((HALF, TILE), late),
        ],
        out_specs=[
            pl.BlockSpec((TILE, total), lambda t: (jnp.minimum(t, 2 * PARTS - 1), 0)),
            pl.BlockSpec((lines, total), whole),
            code_spec,
            pl.BlockSpec((16, 128), whole),
        ],
        out_shape=[
            jax.ShapeDtypeStruct((M, total), BF),
            jax.ShapeDtypeStruct((lines, total), BF),
            jax.ShapeDtypeStruct(code_shape, I16),
            jax.ShapeDtypeStruct((16, 128), F32),
        ],
        scratch_shapes=[
            pltpu.VMEM((2 * PARTS, lines, TILE), F32),
            pltpu.VMEM((2, lines, HALF), BF),
            pltpu.VMEM((2, lines, HALF), BF),
        ],
        compiler_params=params(),
        cost_estimate=pl.CostEstimate(
            flops=2 * lines * M * (total + 3 * HALF), transcendentals=0, bytes_accessed=1 << 24
        ),
        name="density",
    )(device, cells, tables[0], tables[1])


def place_rows(out, first, top, bottom, steps):
    count, rows = out.shape[0], out.shape[1]
    top = encode(top, steps)
    bottom = encode(bottom, steps)
    for inner in range(TILE // rows):
        here = slice(inner * rows, (inner + 1) * rows)
        out[first + inner] = top[here]
        out[count - 1 - first - inner] = bottom[here]


def spectrum_kernel(
    device,
    codes,
    ce_hi,
    ce_lo,
    co_hi,
    co_lo,
    ct_hi,
    ct_lo,
    out,
    dye_hi,
    dye_lo,
    dyo_hi,
    dyo_lo,
    energy,
    even_hi,
    even_lo,
    odd_hi,
    odd_lo,
    dxe_hi,
    dxe_lo,
    dxo_hi,
    dxo_lo,
    *,
    fwd_steps,
    back_steps,
):
    step = pl.program_id(0)
    count, rows = codes.shape[0], codes.shape[1]

    @pl.when(step == 0)
    def _():
        for block in range(count // 2):
            here = pl.ds(block * rows, rows)
            near = decode(codes[block], fwd_steps)
            mirrored = decode(codes[count - 1 - block], fwd_steps)
            even_hi[here, :], even_lo[here, :] = split(near + mirrored)
            odd_hi[here, :], odd_lo[here, :] = split(near - mirrored)
        energy[...] = jnp.zeros((8, 128), F32)

    @pl.when(step < PARTS)
    def _():
        unit = math.pi / M
        lane = lax.broadcasted_iota(jnp.int32, (1, codes.shape[2]), 1) & (rows - 1)
        odd = jnp.where(device[0] >= count // 2, 1, 0)
        q = (2 * (rows * (device[0] - odd * (count // 2)) + lane) + odd).astype(F32)
        first = lax.broadcasted_iota(jnp.int32, (TILE, 1), 0) + step * TILE
        here = pl.ds(pl.multiple_of(step * TILE, TILE), TILE)

        def solve(spectrum, p):
            squared = p * p + q * q
            inverse = jnp.where(squared == 0.0, 0.0, 1.0 / jnp.where(squared == 0.0, 1.0, squared))
            scaled = spectrum * inverse
            return scaled * (q * (1.0 / unit)), scaled * (p * (1.0 / unit)), spectrum * scaled

        spec = dot3(ce_hi[...], ce_lo[...], even_hi[...], even_lo[...])
        drive_x, drive_y, power = solve(spec, (2 * first).astype(F32))
        dxe_hi[here, :], dxe_lo[here, :] = split(drive_x)
        dye_hi[...], dye_lo[...] = split(drive_y)
        spec = dot3(co_hi[...], co_lo[...], odd_hi[...], odd_lo[...])
        drive_x, drive_y, more = solve(spec, (2 * first + 1).astype(F32))
        dxo_hi[here, :], dxo_lo[here, :] = split(drive_x)
        dyo_hi[...], dyo_lo[...] = split(drive_y)
        both = power + more
        if both.shape[1] % 128:
            both = jnp.concatenate(
                [both, jnp.zeros((TILE, 128 - both.shape[1] % 128), F32)], axis=1
            )
        energy[...] += fold_rows(both) * (1.0 / (unit * unit))

    @pl.when(step >= PARTS)
    def _():
        even = dot3(ct_hi[...], ct_lo[...], dxe_hi[...], dxe_lo[...])
        odd = dot3(co_hi[...], co_lo[...], dxo_hi[...], dxo_lo[...])
        first = (step - PARTS) * (TILE // rows)
        place_rows(out, first, even + odd, even - odd, back_steps)


def spectrum_call(device, codes, tables, fwd_steps, back_steps):
    fwd_hi, fwd_lo, _, _, ce_hi, ce_lo, _, _ = tables
    count, rows, cols = codes.shape
    early = lambda t: (jnp.minimum(t, PARTS - 1), 0)
    drive = jax.ShapeDtypeStruct((HALF, cols), BF)
    return pl.pallas_call(
        functools.partial(spectrum_kernel, fwd_steps=fwd_steps, back_steps=back_steps),
        grid=(2 * PARTS,),
        in_specs=[
            pl.BlockSpec(memory_space=pltpu.SMEM),
            pl.BlockSpec((count, rows, cols), lambda t: (0, 0, 0)),
        ]
        + [pl.BlockSpec((TILE, HALF), early)] * 2
        + [pl.BlockSpec((TILE, HALF), lambda t: (t % PARTS, 1))] * 2
        + [pl.BlockSpec((TILE, HALF), lambda t: (jnp.maximum(t - PARTS, 0), 0))] * 2,
        out_specs=[pl.BlockSpec((count, rows, cols), lambda t: (0, 0, 0))]
        + [pl.BlockSpec((TILE, cols), early)] * 4
        + [pl.BlockSpec((8, 128), lambda t: (0, 0))],
        out_shape=[jax.ShapeDtypeStruct((count, rows, cols), I16)]
        + [drive] * 4
        + [jax.ShapeDtypeStruct((8, 128), F32)],
        scratch_shapes=[pltpu.VMEM((HALF, cols), BF)] * 8,
        compiler_params=params(),
        cost_estimate=pl.CostEstimate(
            flops=24 * HALF * HALF * cols, transcendentals=0, bytes_accessed=1 << 24
        ),
        name="spectrum",
    )(device, codes, ce_hi, ce_lo, fwd_hi, fwd_lo, fwd_hi, fwd_lo)


def sine_kernel(
    dye_hi, dye_lo, dyo_hi, dyo_lo, se_hi, se_lo, so_hi, so_lo, out, *, back_steps
):
    even = dot3(se_hi[...], se_lo[...], dye_hi[...], dye_lo[...])
    odd = dot3(so_hi[...], so_lo[...], dyo_hi[...], dyo_lo[...])
    first = pl.program_id(0) * (TILE // out.shape[1])
    place_rows(out, first, odd + even, odd - even, back_steps)


def sine_call(drives, tables, count, rows, back_steps):
    sy_hi, sy_lo = tables[2], tables[3]
    cols = drives[0].shape[1]
    return pl.pallas_call(
        functools.partial(sine_kernel, back_steps=back_steps),
        grid=(PARTS,),
        in_specs=[pl.BlockSpec((HALF, cols), lambda t: (0, 0))] * 4
        + [pl.BlockSpec((TILE, HALF), lambda t: (t, 0))] * 2
        + [pl.BlockSpec((TILE, HALF), lambda t: (t, 1))] * 2,
        out_specs=pl.BlockSpec((count, rows, cols), lambda t: (0, 0, 0)),
        out_shape=jax.ShapeDtypeStruct((count, rows, cols), I16),
        compiler_params=params(),
        cost_estimate=pl.CostEstimate(
            flops=12 * HALF * HALF * cols, transcendentals=0, bytes_accessed=1 << 23
        ),
        name="sine_rows",
    )(*drives, sy_hi, sy_lo, sy_hi, sy_lo)


def field_kernel(
    device,
    codes,
    even_hi,
    even_lo,
    odd_hi,
    odd_lo,
    x_near,
    x_far,
    yt,
    earlier,
    field,
    force,
    part_hi,
    part_lo,
    acc,
    *,
    steps,
    rows,
    count,
    sine,
    by_half,
):
    step = pl.program_id(0)
    flipped = device[0] >= count // 2

    @pl.when(step == 0)
    def _():
        if by_half:
            sources, width = codes.shape[0], codes.shape[2]
            for source in range(sources):
                value = decode(codes[source, 0 : REGIONS * rows, :], steps)
                part = 2 * source // sources
                here = pl.ds((source % (sources // 2)) * width, width)
                part_hi[part, :, here], part_lo[part, :, here] = split(value)
        elif packable(rows):
            for pair in range(count // 2):
                near = decode(codes[2 * pair], steps)
                far = decode(codes[2 * pair + 1], steps)
                part = 2 * pair // (count // 2)
                here = pl.ds((pair % (count // 4)) * 128, 128)
                for half in range(2):
                    lanes = slice(half * 128, (half + 1) * 128)
                    for inner, value in enumerate(swap_halves((near[:, lanes], far[:, lanes]))):
                        lines = pl.ds((2 * half + inner) * rows, rows)
                        part_hi[part, lines, here], part_lo[part, lines, here] = split(value)
        else:
            for part in range(2):
                for block in range(PARTS):
                    here = pl.ds(block * TILE, TILE)
                    value = decode(codes[:, part * HALF + block * TILE :][:, :TILE], steps)
                    part_hi[part, :, here], part_lo[part, :, here] = split(value)

    even = dot3(part_hi[0], part_lo[0], even_hi[...], even_lo[...])
    odd = dot3(part_hi[1], part_lo[1], odd_hi[...], odd_lo[...])
    near = even + odd
    far = odd - even if sine else even - odd
    gathered = dot(near.astype(BF), x_near[...]) + dot(far.astype(BF), x_far[...])

    @pl.when(step == 0)
    def _():
        acc[...] = gathered

    @pl.when(step > 0)
    def _():
        acc[...] += gathered

    lane = 127 - lax.broadcasted_iota(jnp.int32, (8, 128), 1)
    sub = lax.broadcasted_iota(jnp.int32, (8, 128), 0)
    sub = jnp.where(flipped, 7 - sub, sub)
    for region in range(near.shape[0] // rows):
        for block in range(rows // 8):
            start = region * rows + 8 * block
            target = region * rows + jnp.where(flipped, rows - 8 - 8 * block, 8 * block)
            target = pl.multiple_of(target, 8)
            for tile in range(TILE // 128):
                piece = near[start : start + 8, tile * 128 : (tile + 1) * 128]
                piece = jnp.take_along_axis(piece, sub, axis=0)
                col = pl.multiple_of(step * TILE + tile * 128, 128)
                field[pl.ds(target, 8), pl.ds(col, 128)] = piece
                piece = far[start : start + 8, tile * 128 : (tile + 1) * 128]
                piece = jnp.take_along_axis(piece, sub, axis=0)
                piece = jnp.take_along_axis(piece, lane, axis=1)
                col = pl.multiple_of(M - 128 - step * TILE - tile * 128, 128)
                field[pl.ds(target, 8), pl.ds(col, 128)] = piece

    @pl.when(step == PARTS - 1)
    def _():
        latest = jnp.sum(yt[...].astype(F32) * acc[...], axis=0, keepdims=True)
        force[...] = jnp.concatenate([earlier[...], latest], axis=0)[1 - force.shape[0] + 1 :]


def field_call(device, codes, even, odd, xt, yt, steps, rows, count, sine, half=False, earlier=None):
    lines, total = yt.shape
    zeros = (0,) * codes.ndim
    found = 1 if earlier is None else 2
    if earlier is None:
        earlier = jnp.zeros((1, total), F32)
    return pl.pallas_call(
        functools.partial(field_kernel, steps=steps, rows=rows, count=count, sine=sine, by_half=half),
        grid=(PARTS,),
        in_specs=[
            pl.BlockSpec(memory_space=pltpu.SMEM),
            pl.BlockSpec(codes.shape, lambda t: zeros),
        ]
        + [pl.BlockSpec((HALF, TILE), lambda t: (0, t))] * 2
        + [pl.BlockSpec((HALF, TILE), lambda t: (0, PARTS + t))] * 2
        + [
            pl.BlockSpec((TILE, total), lambda t: (t, 0)),
            pl.BlockSpec((TILE, total), lambda t: (PARTS + t, 0)),
            pl.BlockSpec((lines, total), lambda t: (0, 0)),
            pl.BlockSpec((1, total), lambda t: (0, 0)),
        ],
        out_specs=[
            pl.BlockSpec((lines, M), lambda t: (0, 0)),
            pl.BlockSpec((found, total), lambda t: (0, 0)),
        ],
        out_shape=[
            jax.ShapeDtypeStruct((lines, M), F32),
            jax.ShapeDtypeStruct((found, total), F32),
        ],
        scratch_shapes=[
            pltpu.VMEM((2, lines, HALF), BF),
            pltpu.VMEM((2, lines, HALF), BF),
            pltpu.VMEM((lines, total), F32),
        ],
        compiler_params=params(),
        cost_estimate=pl.CostEstimate(
            flops=2 * lines * M * (total + 3 * HALF), transcendentals=0, bytes_accessed=1 << 24
        ),
        name="field_x" if sine else "field_y",
    )(device, codes, even[0], even[1], odd[0], odd[1], xt, xt, yt, earlier)


def profile(rel, low, extent):
    high = jnp.minimum(rel + 1.0, low + extent)
    return jnp.maximum(high - jnp.maximum(rel, low), 0.0)


def prepare_kernel(row, col, width, height, region, offset, out):
    first = row[...] + M * (region[...] + REGIONS * (height[...] - 1))
    second = col[...] + M * (width[...] - 1)
    block = jnp.concatenate([first.astype(F32), second.astype(F32), offset[...]], axis=0)
    for target in range(out.shape[0]):
        out[target] = block


def prepare_call(lists, offset, count):
    return pl.pallas_call(
        prepare_kernel,
        out_shape=jax.ShapeDtypeStruct((count, 4, offset.shape[1]), F32),
        name="prepare",
    )(*lists, offset)


def unpack(first, second):
    turn = M.bit_length() - 1
    first = first.astype(jnp.int32)
    second = second.astype(jnp.int32)
    row = (first & (M - 1)).astype(F32)
    region = (first >> turn) & (REGIONS - 1)
    height = ((first >> (turn + 2)) + 1).astype(F32)
    return row, region, height, second & (M - 1), ((second >> turn) + 1).astype(F32)


def local_kernel(device, everyone, xt, yt, sums, *, rows, count, cell_count):
    step = pl.program_id(0)
    chunk = everyone.shape[2]
    pieces = 2 * cell_count
    slab = device[0] >> (cell_count.bit_length() - 1)
    member = device[0] & (cell_count - 1)

    def source(piece):
        if piece < cell_count:
            return slab * cell_count + ((member + piece) & (cell_count - 1))
        return jnp.maximum(slab - 1, 0) * cell_count + piece - cell_count

    @pl.when(step == 0)
    def _():
        line = lax.broadcasted_iota(jnp.int32, (yt.shape[0], 1), 0)
        inside = line & (rows - 1)
        place = jnp.where(device[0] >= count // 2, rows - 1 - inside, inside) + device[0] * rows
        place = place.astype(F32)
        owner = line >> (rows.bit_length() - 1)
        reached = jnp.where((member == 0) & (slab > 0), 0, REGIONS)
        for piece in range(pieces):
            cell = everyone[source(piece)]
            row, region, height, _, _ = unpack(cell[0:1], cell[1:2])
            if piece >= cell_count:
                region = region + reached
            value = profile(place - row, cell[3:4], height)
            yt[:, pl.ds(piece * chunk, chunk)] = jnp.where(owner == region, value, 0.0).astype(BF)
        sums[...] = jnp.zeros((16, 128), F32)

    place = (step % BIG_PARTS) * BIG + lax.broadcasted_iota(jnp.int32, (BIG, 1), 0)
    place = jnp.where(step >= BIG_PARTS, M - 1 - place, place).astype(F32)
    acc = None
    for piece in range(pieces):
        here = pl.ds(piece * chunk, chunk)
        cell = everyone[source(piece)]
        _, _, _, col, width = unpack(cell[0:1], cell[1:2])
        value = profile(place - col.astype(F32), cell[2:3], width).astype(BF)
        xt[:, here] = value
        part = lax.dot_general(
            yt[:, here], value, (((1,), (1,)), ((), ())), preferred_element_type=F32
        )
        acc = part if acc is None else acc + part
    sums[0:8, :] += fold_rows(jnp.maximum(acc - 1.0, 0.0))
    sums[8:16, :] += fold_rows(acc)


def local_call(device, everyone, rows, count, cell_count):
    total = 2 * cell_count * everyone.shape[2]
    lines = REGIONS * rows
    whole = lambda t: (0, 0)
    return pl.pallas_call(
        functools.partial(local_kernel, rows=rows, count=count, cell_count=cell_count),
        grid=(2 * BIG_PARTS,),
        in_specs=[
            pl.BlockSpec(memory_space=pltpu.SMEM),
            pl.BlockSpec(everyone.shape, lambda t: (0, 0, 0)),
        ],
        out_specs=[
            pl.BlockSpec((BIG, total), lambda t: (t, 0)),
            pl.BlockSpec((lines, total), whole),
            pl.BlockSpec((16, 128), whole),
        ],
        out_shape=[
            jax.ShapeDtypeStruct((M, total), BF),
            jax.ShapeDtypeStruct((lines, total), BF),
            jax.ShapeDtypeStruct((16, 128), F32),
        ],
        compiler_params=params(),
        cost_estimate=pl.CostEstimate(
            flops=2 * lines * M * total, transcendentals=0, bytes_accessed=1 << 23
        ),
        name="local",
    )(device, everyone)


BATCH = 4
BIG = 512
BIG_PARTS = HALF // BIG
NEAR = 32
LOOK = 64
EXTRA = 16
DIGIT = 2048.0
SCALAR_STEPS = steps_of(2.0**36)


def spectral_kernel(
    device,
    cells,
    look_table,
    ce_hi,
    ce_lo,
    co_hi,
    co_lo,
    ct_hi,
    ct_lo,
    out,
    dye_hi,
    dye_lo,
    dyo_hi,
    dyo_lo,
    energy,
    dens,
    look,
    even_hi,
    even_lo,
    odd_hi,
    odd_lo,
    dxe_hi,
    dxe_lo,
    dxo_hi,
    dxo_lo,
    *,
    slab_count,
    count,
    batch,
    back_steps,
):
    step = pl.program_id(0)
    cell_steps = slab_count // batch
    slab_rows = M // slab_count
    group = count // 2
    rows = M // count
    width = M // group
    window = slab_rows + EXTRA
    upper = device[0] >= group
    member = jnp.where(upper, device[0] - group, device[0])
    sign = jnp.where(upper, -1.0, 1.0).astype(F32)

    @pl.when(step == 0)
    def _():
        dens[...] = jnp.zeros(dens.shape, F32)
        look[:, : 2 * LOOK], look[:, 2 * LOOK :] = split(look_table[...])
        energy[...] = jnp.zeros((8, 128), F32)

    def add_slab(slab, pieces):
        top = slab >= slab_count // 2
        line = lax.broadcasted_iota(jnp.int32, (window, 1), 0)
        line = jnp.where(top, window - 1 - line, line) + slab * slab_rows
        line = line.astype(F32)
        cell = jnp.concatenate([cells[piece] for piece in pieces], axis=1)
        row, region, height, col, width_x = unpack(cell[0:1], cell[1:2])
        low_x, low_y = cell[2:3], cell[3:4]
        value_y = profile(line - row, low_y, height).astype(BF)
        stacked = jnp.concatenate(
            [value_y * jnp.where(region == g, 1.0, 0.0).astype(BF) for g in range(REGIONS)],
            axis=0,
        )
        slot = lax.broadcasted_iota(jnp.int32, (NEAR + 16, 1), 0).astype(F32)
        inside = (col & (NEAR - 1)).astype(F32)
        feature = profile(slot - inside, low_x, width_x).astype(BF)
        feature = jnp.concatenate(
            [feature, jnp.zeros((LOOK - NEAR - 16, feature.shape[1]), BF)], axis=0
        )
        spot = lax.broadcasted_iota(jnp.int32, (LOOK, 1), 0)
        chosen = jnp.where(spot == (col >> (NEAR.bit_length() - 1)), 1.0, 0.0).astype(BF)
        found = dot(look[...], jnp.concatenate([feature, chosen, feature, chosen], axis=0))
        value = found[:width] * found[2 * width : 3 * width]
        value = value - found[width : 2 * width] * found[3 * width :]
        value = jnp.concatenate(split(value), axis=0)
        acc = lax.dot_general(
            stacked, value, (((1,), (1,)), ((), ())), preferred_element_type=F32
        )
        half = jnp.where(top, 1, 0)
        start = jnp.where(top, slab_count - 1 - slab, slab) * slab_rows
        here = pl.ds(pl.multiple_of(start, 8), window)
        for g in range(REGIONS):
            lines = slice(g * window, (g + 1) * window)
            lanes = pl.ds(g * width, width)
            dens[half, here, lanes] += acc[lines, :width] + acc[lines, width:]

    @pl.when(step < cell_steps)
    def _():
        share = count // slab_count
        for inner in range(batch):
            add_slab(step * batch + inner, range(inner * share, (inner + 1) * share))

    @pl.when(step == cell_steps)
    def _():
        sub = 7 - lax.broadcasted_iota(jnp.int32, (8, 128), 0)
        for tile in range(dens.shape[2] // 128):
            lanes = pl.ds(tile * 128, 128)
            spill = jnp.take_along_axis(dens[0, HALF : HALF + 8, lanes], sub, axis=0)
            dens[1, HALF + EXTRA - 8 : HALF + EXTRA, lanes] += spill
        for block in range(HALF // 128):
            here = pl.ds(block * 128, 128)
            near = dens[0, here, :]
            mirrored = dens[1, pl.ds(block * 128 + EXTRA, 128), :]
            even_hi[here, :], even_lo[here, :] = split(near + mirrored)
            odd_hi[here, :], odd_lo[here, :] = split(near - mirrored)

    @pl.when((step >= cell_steps) & (step < cell_steps + BIG_PARTS))
    def _():
        turn = step - cell_steps
        unit = math.pi / M
        lane = lax.broadcasted_iota(jnp.int32, (1, width), 1)
        odd = jnp.where(member >= group // 2, 1, 0)
        q = (2 * (width * (member - odd * (group // 2)) + lane) + odd).astype(F32)
        first = lax.broadcasted_iota(jnp.int32, (BIG, 1), 0) + turn * BIG
        here = pl.ds(pl.multiple_of(turn * BIG, BIG), BIG)
        spent = jnp.zeros((8, 128), F32)

        def solve(spectrum, p, x_hi, x_lo, y_hi, y_lo, sign_x, sign_y, spent):
            squared = p * p + q * q
            inverse = jnp.where(squared == 0.0, 0.0, 1.0 / jnp.where(squared == 0.0, 1.0, squared))
            factor_x = inverse * (q * (sign_x / unit))
            factor_y = inverse * (p * (sign_y / unit))
            for g in range(REGIONS):
                lanes = pl.ds(g * width, width)
                part = spectrum[:, g * width : (g + 1) * width]
                x_hi[here, lanes], x_lo[here, lanes] = split(part * factor_x)
                y_hi[:, lanes], y_lo[:, lanes] = split(part * factor_y)
                spent = spent + fold_rows(part * (part * inverse))
            return spent

        spec = dot3(ce_hi[...], ce_lo[...], even_hi[...], even_lo[...])
        spent = solve(
            spec, (2 * first).astype(F32), dxe_hi, dxe_lo, dye_hi, dye_lo, 1.0, sign, spent
        )
        spec = dot3(co_hi[...], co_lo[...], odd_hi[...], odd_lo[...])
        spent = solve(
            spec, (2 * first + 1).astype(F32), dxo_hi, dxo_lo, dyo_hi, dyo_lo, sign, 1.0, spent
        )
        energy[...] += spent * (1.0 / (unit * unit))

    @pl.when(step >= cell_steps + BIG_PARTS)
    def _():
        value = dot3(ct_hi[...], ct_lo[...], dxe_hi[...], dxe_lo[...])
        value = value + dot3(co_hi[...], co_lo[...], dxo_hi[...], dxo_lo[...])
        first = (step - cell_steps - BIG_PARTS) * (BIG // rows)
        send_rows(out, first, value, upper, rows, back_steps)


def send_rows(out, first, value, upper, rows, steps):
    count, width = out.shape[0], out.shape[2]
    code = encode(value, steps)
    for inner in range(value.shape[0] // rows):
        target = first + inner
        target = jnp.where(upper, count - 1 - target, target)
        for g in range(REGIONS):
            here = pl.ds(g * rows, rows)
            piece = code[inner * rows : (inner + 1) * rows, g * width : (g + 1) * width]
            out[target, here, :] = piece


def spectral_call(device, cells, look_table, tables, slab_count, back_steps):
    fwd_hi, fwd_lo, _, _, ce_hi, ce_lo, _, _ = tables
    count = cells.shape[0]
    group = count // 2
    rows = M // count
    width = M // group
    cols = REGIONS * width
    batch = math.gcd(slab_count, BATCH)
    cell_steps = slab_count // batch
    share = batch * count // slab_count
    phase = lambda t: jnp.clip(t - cell_steps, 0, BIG_PARTS - 1)
    last = lambda t: jnp.clip(t - cell_steps - BIG_PARTS, 0, BIG_PARTS - 1)
    both = lambda t: jnp.where(t < cell_steps, 0, (t - cell_steps) % BIG_PARTS)
    drive = jax.ShapeDtypeStruct((HALF, cols), BF)
    return pl.pallas_call(
        functools.partial(
            spectral_kernel,
            slab_count=slab_count,
            count=count,
            batch=batch,
            back_steps=back_steps,
        ),
        grid=(cell_steps + 2 * BIG_PARTS,),
        in_specs=[
            pl.BlockSpec(memory_space=pltpu.SMEM),
            pl.BlockSpec(
                (share,) + cells.shape[1:], lambda t: (jnp.minimum(t, cell_steps - 1), 0, 0)
            ),
            pl.BlockSpec(look_table.shape, lambda t: (0, 0)),
        ]
        + [pl.BlockSpec((BIG, HALF), lambda t: (phase(t), 0))] * 2
        + [pl.BlockSpec((BIG, HALF), lambda t: (both(t), 1))] * 2
        + [pl.BlockSpec((BIG, HALF), lambda t: (last(t), 0))] * 2,
        out_specs=[pl.BlockSpec((group, REGIONS * rows, width), lambda t: (0, 0, 0))]
        + [pl.BlockSpec((BIG, cols), lambda t: (phase(t), 0))] * 4
        + [pl.BlockSpec((8, 128), lambda t: (0, 0))],
        out_shape=[jax.ShapeDtypeStruct((group, REGIONS * rows, width), I16)]
        + [drive] * 4
        + [jax.ShapeDtypeStruct((8, 128), F32)],
        scratch_shapes=[
            pltpu.VMEM((2, HALF + EXTRA, cols), F32),
            pltpu.VMEM((4 * width, 4 * LOOK), BF),
        ]
        + [pltpu.VMEM((HALF, cols), BF)] * 8,
        compiler_params=params(),
        cost_estimate=pl.CostEstimate(
            flops=30 * HALF * HALF * cols, transcendentals=0, bytes_accessed=1 << 24
        ),
        name="spectral",
    )(device, cells, look_table, ce_hi, ce_lo, fwd_hi, fwd_lo, fwd_hi, fwd_lo)


def sine_half_kernel(
    device,
    sums,
    power,
    dye_hi,
    dye_lo,
    dyo_hi,
    dyo_lo,
    se_hi,
    se_lo,
    so_hi,
    so_lo,
    out,
    *,
    rows,
    back_steps,
):
    @pl.when(pl.program_id(0) == 0)
    def _():
        def digits(parts):
            total = jnp.sum(jnp.sum(parts, axis=1, keepdims=True), axis=0, keepdims=True)
            first = encode_wide(total, SCALAR_STEPS)
            rest = (total - decode(first.astype(jnp.int32), SCALAR_STEPS)) * DIGIT
            return [first, encode_wide(rest, SCALAR_STEPS)]

        shape = (EXTRA, out.shape[2])
        lane = lax.broadcasted_iota(jnp.int32, shape, 1)
        lane = jnp.where(lax.broadcasted_iota(jnp.int32, shape, 0) == 0, lane, -1)
        block = jnp.zeros(shape, F32)
        codes = digits(sums[0:8, :]) + digits(sums[8:16, :])
        codes = codes + digits(power[...] * (1.0 / (M * M)))
        for index, code in enumerate(codes):
            block = jnp.where(lane == index, code, block)
        block = block.astype(jnp.int32).astype(I16)
        for target in range(out.shape[0]):
            out[target, REGIONS * rows : REGIONS * rows + EXTRA, :] = block

    value = dot3(se_hi[...], se_lo[...], dye_hi[...], dye_lo[...])
    value = value + dot3(so_hi[...], so_lo[...], dyo_hi[...], dyo_lo[...])
    first = pl.program_id(0) * (TILE // rows)
    send_rows(out, first, value, device[0] >= out.shape[0], rows, back_steps)


def sine_half_call(device, sums, power, drives, tables, group, rows, back_steps):
    sy_hi, sy_lo = tables[2], tables[3]
    cols = drives[0].shape[1]
    shape = (group, REGIONS * rows + EXTRA, cols // REGIONS)
    return pl.pallas_call(
        functools.partial(sine_half_kernel, rows=rows, back_steps=back_steps),
        grid=(PARTS,),
        in_specs=[
            pl.BlockSpec(memory_space=pltpu.SMEM),
            pl.BlockSpec((16, 128), lambda t: (0, 0)),
            pl.BlockSpec((8, 128), lambda t: (0, 0)),
        ]
        + [pl.BlockSpec((HALF, cols), lambda t: (0, 0))] * 4
        + [pl.BlockSpec((TILE, HALF), lambda t: (t, 0))] * 2
        + [pl.BlockSpec((TILE, HALF), lambda t: (t, 1))] * 2,
        out_specs=pl.BlockSpec(shape, lambda t: (0, 0, 0)),
        out_shape=jax.ShapeDtypeStruct(shape, I16),
        compiler_params=params(),
        cost_estimate=pl.CostEstimate(
            flops=12 * HALF * HALF * cols, transcendentals=0, bytes_accessed=1 << 23
        ),
        name="sine_half",
    )(device, sums, power, *drives, sy_hi, sy_lo, sy_hi, sy_lo)


def cell_tables(first_q, width):
    line = lax.broadcasted_iota(jnp.int32, (2 * width, 2 * LOOK), 0)
    lane = lax.broadcasted_iota(jnp.int32, (2 * width, 2 * LOOK), 1)
    q = first_q + 2 * (line & (width - 1))
    near = lane < LOOK
    moment = jnp.where(near, 2 * lane + 1, 2 * NEAR * (lane - LOOK))
    phase = (q * moment + jnp.where(line < width, 0, 3 * M)) & (4 * M - 1)
    weight = jnp.where(q == 0, math.sqrt(1.0 / M), math.sqrt(2.0 / M)).astype(F32)
    value = jnp.cos(phase.astype(F32) * (math.pi / (2.0 * M)))
    return jnp.concatenate(
        [jnp.where(near, value * weight, 0.0), jnp.where(near, 0.0, value)], axis=0
    )


def exchange(blocks, groups=None):
    return lax.all_to_all(
        blocks, AXES, split_axis=0, concat_axis=0, tiled=True, axis_index_groups=groups
    )


def full_work(cell_row, cell_col, cell_width, cell_height, cell_region, cell_offset):
    slab_count = lax.axis_size("slab")
    cell_count = lax.axis_size("cell")
    count = slab_count * cell_count
    device = lax.axis_index("slab") * cell_count + lax.axis_index("cell")
    rows = M // count
    own = cell_row.shape[0]
    lines = REGIONS * rows
    gain = math.sqrt(2.0 / M)
    fwd_steps = steps_of(2.1 * own * cell_count * WMAX * gain)
    back_steps = steps_of(gain**3 * own * count * WMAX * HMAX * 1.1 * M / math.pi * 8.5)

    ints = [cell_row, cell_col, cell_width, cell_height, cell_region]
    mine = jnp.concatenate(
        [jnp.stack(ints).astype(F32), cell_offset, jnp.zeros((1, own), F32)], axis=0
    )
    pieces = [mine]
    back_moves = []
    for turn in range(1, cell_count):
        pairs = [
            (slab * cell_count + c, slab * cell_count + (c + turn) % cell_count)
            for slab in range(slab_count)
            for c in range(cell_count)
        ]
        pieces.append(lax.ppermute(mine, AXES, pairs))
        back_moves.append([(b, a) for a, b in pairs])
    for c in range(cell_count):
        pairs = [
            (slab * cell_count + c, (slab + 1) * cell_count) for slab in range(slab_count - 1)
        ]
        pieces.append(lax.ppermute(mine, AXES, pairs))
        back_moves.append([(b, a) for a, b in pairs])
    tables = make_tables(jnp.zeros((1,), jnp.int32), 128)[:8]
    cells = jnp.concatenate(pieces, axis=1)

    device = device.astype(jnp.int32).reshape(1)
    xt, yt, codes, sums = density_call(device, cells, tables, rows, count, fwd_steps)
    if not packable(rows):
        codes = jnp.transpose(codes.reshape(REGIONS, rows, count, rows), (2, 1, 0, 3))
        codes = codes.reshape(count, rows, lines)
    arrived = exchange(codes)
    drive = spectrum_call(device, arrived, tables, fwd_steps, back_steps)
    along_x = exchange(drive[0])
    sine_part = sine_call(drive[1:5], tables, count, rows, back_steps)
    along_y = exchange(sine_part)

    sums = jnp.concatenate([sums, drive[5]], axis=0)
    reach = 1
    while reach < count:
        sums = sums + lax.ppermute(sums, AXES, [(i, i ^ reach) for i in range(count)])
        reach *= 2
    sums = jnp.sum(sums.reshape(3, 8 * 128), axis=1)

    def lines_of(blocks):
        if packable(rows):
            return blocks
        shaped = blocks.reshape(count, rows, REGIONS, rows)
        return jnp.transpose(shaped, (2, 1, 0, 3)).reshape(lines, M)

    fwd, sy, ce, se = tables[0:2], tables[2:4], tables[4:6], tables[6:8]
    field_x, force_x = field_call(
        device, lines_of(along_x), se, sy, xt, yt, back_steps, rows, count, True
    )
    field_y, force_y = field_call(
        device, lines_of(along_y), ce, fwd, xt, yt, back_steps, rows, count, False
    )
    partial = jnp.concatenate([force_x, force_y], axis=0)
    cell_force = partial[:, :own]
    for index, pairs in enumerate(back_moves):
        piece = partial[:, (index + 1) * own : (index + 2) * own]
        cell_force = cell_force + lax.ppermute(piece, AXES, pairs)
    energy = sums[2] / (M * M)
    overflow = sums[0] / sums[1]
    shape = (REGIONS, rows, M)
    return (field_x.reshape(shape), field_y.reshape(shape), cell_force, energy, overflow)


def half_work(cell_row, cell_col, cell_width, cell_height, cell_region, cell_offset):
    slab_count = lax.axis_size("slab")
    cell_count = lax.axis_size("cell")
    count = slab_count * cell_count
    group = count // 2
    slab = lax.axis_index("slab")
    member = lax.axis_index("cell")
    device = slab * cell_count + member
    rows = M // count
    width = M // group
    lines = REGIONS * rows
    own = cell_row.shape[0]
    gain = math.sqrt(2.0 / M)
    back_steps = steps_of(gain**3 * own * count * WMAX * HMAX * 1.1 * M / math.pi * 8.5)
    groups = [list(range(group)), list(range(group, count))]

    lists = [cell_row, cell_col, cell_width, cell_height, cell_region]
    mine = prepare_call([item.reshape(1, own) for item in lists], cell_offset, count)
    everyone = exchange(mine)
    within = device % group
    odd = within // (group // 2)
    first_q = 2 * width * (within - odd * (group // 2)) + odd
    tables = make_tables(first_q.astype(jnp.int32).reshape(1), width)
    scalar = device.astype(jnp.int32).reshape(1)

    drive = spectral_call(scalar, everyone, tables[8], tables[:8], slab_count, back_steps)
    along_x = exchange(drive[0], groups)
    xt, yt, sums = local_call(scalar, everyone, rows, count, cell_count)
    sine_part = sine_half_call(scalar, sums, drive[5], drive[1:5], tables, group, rows, back_steps)
    along_y = exchange(sine_part, groups)
    scalars = jnp.sum(decode(along_y[:, lines : lines + 8, :], SCALAR_STEPS), axis=0)
    other = lax.ppermute(scalars, AXES, [(i, (i + group) % count) for i in range(count)])
    joint = scalars[0] + other[0]

    fwd, sy, ce, se = tables[0:2], tables[2:4], tables[4:6], tables[6:8]
    field_x, force_x = field_call(
        scalar, along_x, se, sy, xt, yt, back_steps, rows, count, True, True
    )
    field_y, partial = field_call(
        scalar, along_y, ce, fwd, xt, yt, back_steps, rows, count, False, True, force_x
    )
    cell_force = partial[:, :own]
    for turn in range(1, cell_count):
        piece = partial[:, turn * own : (turn + 1) * own]
        pairs = [
            (s * cell_count + c, s * cell_count + (c + turn) % cell_count)
            for s in range(slab_count)
            for c in range(cell_count)
        ]
        cell_force = cell_force + lax.ppermute(piece, AXES, pairs)
    for c in range(cell_count):
        pairs = [(s * cell_count, (s - 1) * cell_count + c) for s in range(1, slab_count)]
        cell_force = cell_force + lax.ppermute(
            partial[:, (cell_count + c) * own : (cell_count + c + 1) * own], AXES, pairs
        )
    energy = scalars[0, 4] + scalars[0, 5] * (1.0 / DIGIT)
    overflow = (joint[0] + joint[1] * (1.0 / DIGIT)) / (joint[2] + joint[3] * (1.0 / DIGIT))
    shape = (REGIONS, rows, M)
    return (field_x.reshape(shape), field_y.reshape(shape), cell_force, energy, overflow)


def work(*args):
    count = lax.axis_size("slab") * lax.axis_size("cell")
    if packable(M // count):
        return half_work(*args)
    return full_work(*args)


def solution(mesh):
    return jax.shard_map(
        work,
        mesh=mesh,
        in_specs=(
            P(("slab", "cell")),
            P(("slab", "cell")),
            P(("slab", "cell")),
            P(("slab", "cell")),
            P(("slab", "cell")),
            P(None, ("slab", "cell")),
        ),
        out_specs=(
            P(None, ("slab", "cell"), None),
            P(None, ("slab", "cell"), None),
            P(None, ("slab", "cell")),
            P(),
            P(),
        ),
        check_vma=False,
    )
```
